32 devices in a mesh: dp: 2 (over x), tp: 4 (over z), cp: 4 (over y, core).
Axes of the slice: x: 2, y: 2, z: 4, core: 2. Of those that a mesh axis runs over, the one named last changes fastest.
Arguments:
- hidden: bfloat16 [16, 64, 2560], P('dp'), parts along dimension 0
- prefix_len: int32 [16], P('dp'), parts along dimension 0
- k_cache: bfloat16 [16, 16384, 8, 128], P('dp', 'cp', 'tp'), parts along dimension 0
- v_cache: bfloat16 [16, 16384, 8, 128], P('dp', 'cp', 'tp'), parts along dimension 0
- attn_norm: bfloat16 [2560], replicated
- w_q: bfloat16 [2560, 4096], P(None, 'tp')
- w_k: bfloat16 [2560, 1024], P(None, 'tp')
- w_v: bfloat16 [2560, 1024], P(None, 'tp')
- w_o: bfloat16 [4096, 2560], P('tp')
- q_norm: bfloat16 [128], replicated
- k_norm: bfloat16 [128], replicated
Outputs:
- output 1: bfloat16 [16, 64, 2560], P('dp'), parts along dimension 0
- output 2: bfloat16 [16, 64, 8, 128], P('dp', None, 'tp'), parts along dimension 0
- output 3: bfloat16 [16, 64, 8, 128], P('dp', None, 'tp'), parts along dimension 0
There are 2 independent parts. The reference program is written for one: setup_inputs(seed, part) draws one part's arguments, and reference() takes and returns one part's arrays. A program takes and returns all parts, laid end to end along the dimension named above; an argument that names none is the same for every part.
All inputs are finite; a program needn't handle non-finite values.
Results may differ from the reference program's by a relative error of at most 0.00827889.
Values sent between devices are 32-bit elements.
A program may use at most 1 GiB of HBM per device.

```python
import jax
import jax.numpy as jnp
from jax import lax

NUM_SEQ = 8
NEW_TOKENS = 64
CACHE_LEN = 16384
D_MODEL = 2560
N_HEADS = 32
KV_HEADS = 8
HEAD_DIM = 128


def rms_scale(tensor, norm_gain):
    mean_sq = jnp.mean(jnp.square(tensor), axis=-1, keepdims=True)
    return tensor * lax.rsqrt(mean_sq + 1e-6) * norm_gain


def rope_apply(tensor, positions):
    half_dim = HEAD_DIM // 2
    inv_freq = 1.0 / (1000000.0 ** (jnp.arange(half_dim, dtype=jnp.float32) * 2.0 / HEAD_DIM))
    angles = positions.astype(jnp.float32)[..., None] * inv_freq
    cos_t = jnp.cos(angles)[..., None, :]
    sin_t = jnp.sin(angles)[..., None, :]
    lead_half = tensor[..., :half_dim]
    tail_half = tensor[..., half_dim:]
    return jnp.concatenate([lead_half * cos_t - tail_half * sin_t, tail_half * cos_t + lead_half * sin_t], axis=-1)


def smooth_field(key, amplitude):
    n_freq = 4
    coords = (jnp.arange(CACHE_LEN, dtype=jnp.float32) + 0.5) / CACHE_LEN
    angles = jnp.pi * coords[:, None] * jnp.arange(1, n_freq + 1, dtype=jnp.float32)[None, :]
    cos_basis = jnp.concatenate([jnp.cos(angles), jnp.sin(angles)], axis=1)
    coeffs = jax.random.normal(key, (NUM_SEQ, 2 * n_freq, KV_HEADS, HEAD_DIM), jnp.float32) * (amplitude / n_freq ** 0.5)
    return jnp.einsum('pf,bfke->bpke', cos_basis, coeffs)


def setup_inputs(seed: int = 0, part: int = 0) -> dict:
    shared = jax.random.split(jax.random.key(seed), 8)
    part_keys = jax.random.split(jax.random.fold_in(jax.random.key(seed + 1), part), 8)
    cache_shape = (NUM_SEQ, CACHE_LEN, KV_HEADS, HEAD_DIM)
    len_draw = jax.random.randint(part_keys[1], (NUM_SEQ,), 0, CACHE_LEN + 1)
    full_at = jax.random.randint(part_keys[2], (), 0, NUM_SEQ)
    prefix_len = jnp.where(jnp.arange(NUM_SEQ) == full_at, CACHE_LEN, len_draw).astype(jnp.int32)
    k_cache = smooth_field(part_keys[3], 2.0) + 0.5 * jax.random.normal(part_keys[4], cache_shape, jnp.float32)
    v_cache = smooth_field(part_keys[5], 1.0) + 0.5 * jax.random.normal(part_keys[6], cache_shape, jnp.float32)
    q_width = N_HEADS * HEAD_DIM
    kv_width = KV_HEADS * HEAD_DIM
    return {
        'hidden': jax.random.normal(part_keys[0], (NUM_SEQ, NEW_TOKENS, D_MODEL), jnp.float32).astype(jnp.bfloat16),
        'prefix_len': prefix_len,
        'k_cache': k_cache.astype(jnp.bfloat16),
        'v_cache': v_cache.astype(jnp.bfloat16),
        'attn_norm': (1.0 + 0.4 * jax.random.normal(shared[0], (D_MODEL,), jnp.float32)).astype(jnp.bfloat16),
        'w_q': (jax.random.normal(shared[1], (D_MODEL, q_width), jnp.float32) * D_MODEL ** -0.5).astype(jnp.bfloat16),
        'w_k': (jax.random.normal(shared[2], (D_MODEL, kv_width), jnp.float32) * D_MODEL ** -0.5).astype(jnp.bfloat16),
        'w_v': (jax.random.normal(shared[3], (D_MODEL, kv_width), jnp.float32) * D_MODEL ** -0.5).astype(jnp.bfloat16),
        'w_o': (jax.random.normal(shared[4], (q_width, D_MODEL), jnp.float32) * q_width ** -0.5).astype(jnp.bfloat16),
        'q_norm': (1.0 + 0.4 * jax.random.normal(shared[5], (HEAD_DIM,), jnp.float32)).astype(jnp.bfloat16),
        'k_norm': (1.0 + 0.4 * jax.random.normal(shared[6], (HEAD_DIM,), jnp.float32)).astype(jnp.bfloat16),
    }


def reference(hidden, prefix_len, k_cache, v_cache, attn_norm, w_q, w_k, w_v, w_o, q_norm, k_norm):
    group_size = N_HEADS // KV_HEADS
    flat_rows = hidden.reshape(NUM_SEQ * NEW_TOKENS, D_MODEL)
    normed = rms_scale(flat_rows.astype(jnp.float32), attn_norm.astype(jnp.float32)).astype(jnp.bfloat16)
    q_lin = jnp.dot(normed, w_q, preferred_element_type=jnp.float32).astype(jnp.bfloat16)
    k_lin = jnp.dot(normed, w_k, preferred_element_type=jnp.float32).astype(jnp.bfloat16)
    v_lin = jnp.dot(normed, w_v, preferred_element_type=jnp.float32).astype(jnp.bfloat16)
    positions = prefix_len[:, None] + jnp.arange(NEW_TOKENS, dtype=jnp.int32)[None, :]
    q_heads = q_lin.reshape(NUM_SEQ, NEW_TOKENS, N_HEADS, HEAD_DIM).astype(jnp.float32)
    k_heads = k_lin.reshape(NUM_SEQ, NEW_TOKENS, KV_HEADS, HEAD_DIM).astype(jnp.float32)
    q_rot = rope_apply(rms_scale(q_heads, q_norm.astype(jnp.float32)), positions).astype(jnp.bfloat16)
    k_new = rope_apply(rms_scale(k_heads, k_norm.astype(jnp.float32)), positions).astype(jnp.bfloat16)
    v_new = v_lin.reshape(NUM_SEQ, NEW_TOKENS, KV_HEADS, HEAD_DIM)
    causal = jnp.arange(NEW_TOKENS)[:, None] >= jnp.arange(NEW_TOKENS)[None, :]
    score_scale = HEAD_DIM ** -0.5

    def one_sequence(operands):
        q_seq, k_seq, v_seq, kc_seq, vc_seq, seq_len = operands
        cache_ok = jnp.arange(CACHE_LEN) < seq_len
        key_mask = jnp.concatenate([jnp.broadcast_to(cache_ok[None, :], (NEW_TOKENS, CACHE_LEN)), causal], axis=1)

        def one_head_group(group_ops):
            q_grp, key_all, val_all = group_ops
            scores = jnp.einsum('cgd,kd->gck', q_grp.astype(jnp.float32), key_all.astype(jnp.float32)) * score_scale
            scores = jnp.where(key_mask[None], scores, -jnp.inf)
            prob_mat = jax.nn.softmax(scores, axis=-1)
            return jnp.einsum('gck,kd->cgd', prob_mat, val_all.astype(jnp.float32))

        key_all = jnp.concatenate([kc_seq, k_seq], axis=0).transpose(1, 0, 2)
        val_all = jnp.concatenate([vc_seq, v_seq], axis=0).transpose(1, 0, 2)
        q_grp = q_seq.reshape(NEW_TOKENS, KV_HEADS, group_size, HEAD_DIM).transpose(1, 0, 2, 3)
        out_grp = lax.map(one_head_group, (q_grp, key_all, val_all))
        return out_grp.transpose(1, 0, 2, 3).reshape(NEW_TOKENS, N_HEADS * HEAD_DIM)

    attn_seq = lax.map(one_sequence, (q_rot, k_new, v_new, k_cache, v_cache, prefix_len))
    attn_rows = attn_seq.reshape(NUM_SEQ * NEW_TOKENS, N_HEADS * HEAD_DIM).astype(jnp.bfloat16)
    block_out = flat_rows.astype(jnp.float32) + jnp.dot(attn_rows, w_o, preferred_element_type=jnp.float32)
    return block_out.astype(jnp.bfloat16).reshape(NUM_SEQ, NEW_TOKENS, D_MODEL), k_new, v_new
```

```python
import functools

import jax
import jax.numpy as jnp
import numpy as np
from jax import lax
from jax.experimental import pallas as pl
from jax.experimental.pallas import tpu as pltpu
from jax.sharding import PartitionSpec as P

HEAD_DIM = 128
MASKED = -1e30
EPS = 1e-6
LOG2_SCALE = float(HEAD_DIM ** -0.5 / np.log(2.0))
MESH = pl.DeviceIdType.MESH
NT = (((1,), (1,)), ((), ()))
TN = (((0,), (0,)), ((), ()))
F32 = jnp.float32
BF16 = jnp.bfloat16


def project_kernel(prefix_ref, x_ref, an_ref, wq_hbm, wk_hbm, wv_hbm, qn_ref, kn_ref, freq_ref,
                   q_ref, k_ref, v_ref, wq, wk, wv, normed, cos_ref, sin_ref, sems):
    n_seq, n_new = k_ref.shape[0], k_ref.shape[2]
    rows = n_seq * n_new
    copies = [pltpu.make_async_copy(wq_hbm.at[:, pl.ds(256 * j, 256)], wq.at[j], sems.at[j]) for j in range(4)]
    copies.append(pltpu.make_async_copy(wk_hbm, wk, sems.at[4]))
    copies.append(pltpu.make_async_copy(wv_hbm, wv, sems.at[5]))
    for c in copies:
        c.start()
    for r in range(0, rows, 64):
        x = x_ref[r:r + 64, :].astype(F32)
        scale = lax.rsqrt(jnp.mean(x * x, axis=-1, keepdims=True) + EPS)
        normed[r:r + 64, :] = (x * scale * an_ref[...].astype(F32)).astype(BF16)
    lane = lax.broadcasted_iota(jnp.int32, (n_new, HEAD_DIM), 1)
    step = lax.broadcasted_iota(jnp.int32, (n_new, HEAD_DIM), 0)
    for b in range(n_seq):
        angle = (prefix_ref[b] + step).astype(F32) * freq_ref[...]
        cos_ref[b * n_new:(b + 1) * n_new, :] = jnp.cos(angle)
        sin_t = jnp.sin(angle)
        sin_ref[b * n_new:(b + 1) * n_new, :] = jnp.where(lane < HEAD_DIM // 2, -sin_t, sin_t)

    def norm_rope(y, gain_ref):
        y = y.astype(BF16).astype(F32)
        y = y * lax.rsqrt(jnp.mean(y * y, axis=-1, keepdims=True) + EPS) * gain_ref[...].astype(F32)
        return (y * cos_ref[...] + pltpu.roll(y, HEAD_DIM // 2, 1) * sin_ref[...]).astype(BF16)

    for j in range(4):
        copies[j].wait()
        y = jnp.dot(normed[...], wq[j], preferred_element_type=F32)
        for i in range(2):
            h, g = j // 2, 2 * (j % 2) + i
            head = norm_rope(y[:, i * HEAD_DIM:(i + 1) * HEAD_DIM], qn_ref)
            for b in range(n_seq):
                for c in range(2):
                    q_ref[b, c * 128 + g * 32:c * 128 + g * 32 + 32, h * 128:(h + 1) * 128] = (
                        head[b * 64 + c * 32:b * 64 + c * 32 + 32])
    copies[4].wait()
    y = jnp.dot(normed[...], wk[...], preferred_element_type=F32)
    for h in range(2):
        head = norm_rope(y[:, h * HEAD_DIM:(h + 1) * HEAD_DIM], kn_ref)
        for b in range(n_seq):
            k_ref[b, h] = head[b * 64:(b + 1) * 64]
    copies[5].wait()
    y = jnp.dot(normed[...], wv[...], preferred_element_type=F32).astype(BF16)
    for h in range(2):
        for b in range(n_seq):
            v_ref[b, h] = y[b * 64:(b + 1) * 64, h * HEAD_DIM:(h + 1) * HEAD_DIM]


def project(hidden, prefix_len, attn_norm, w_q, w_k, w_v, q_norm, k_norm):
    n_seq, n_new, d_model = hidden.shape
    freq = 1.0 / (1000000.0 ** (np.arange(HEAD_DIM // 2, dtype=np.float64) * 2.0 / HEAD_DIM))
    freq = jnp.asarray(np.concatenate([freq, freq])[None].astype(np.float32))
    vmem = pl.BlockSpec(memory_space=pltpu.VMEM)
    hbm = pl.BlockSpec(memory_space=pl.ANY)
    rows = n_seq * n_new
    return pl.pallas_call(
        project_kernel,
        out_shape=(jax.ShapeDtypeStruct((n_seq, 256, 256), BF16),
                   jax.ShapeDtypeStruct((n_seq, 2, n_new, HEAD_DIM), BF16),
                   jax.ShapeDtypeStruct((n_seq, 2, n_new, HEAD_DIM), BF16)),
        in_specs=[pl.BlockSpec(memory_space=pltpu.SMEM), vmem, vmem, hbm, hbm, hbm, vmem, vmem, vmem],
        out_specs=(vmem, vmem, vmem),
        scratch_shapes=[pltpu.VMEM((4, d_model, 256), BF16), pltpu.VMEM((d_model, 256), BF16),
                        pltpu.VMEM((d_model, 256), BF16), pltpu.VMEM((rows, d_model), BF16),
                        pltpu.VMEM((rows, HEAD_DIM), F32), pltpu.VMEM((rows, HEAD_DIM), F32),
                        pltpu.SemaphoreType.DMA((6,))],
        compiler_params=pltpu.CompilerParams(vmem_limit_bytes=48 << 20),
        cost_estimate=pl.CostEstimate(flops=2 * rows * d_model * 1536, bytes_accessed=12 << 20, transcendentals=0),
        name="project",
    )(prefix_len, hidden.reshape(rows, d_model), attn_norm[None], w_q, w_k, w_v, q_norm[None], k_norm[None], freq)


def pair_reduce(op, x):
    x = op(x, pltpu.roll(x, 2, 0))
    return op(x, pltpu.roll(x, 4, 0))


def own_keys(q, k_own_ref, v_own_ref, first):
    n_new = k_own_ref.shape[-2]
    key = lax.broadcasted_iota(jnp.int32, (n_new, 256), 0)
    col = lax.broadcasted_iota(jnp.int32, (n_new, 256), 1)
    token = (col // 128) * 32 + col % 32
    keep = jnp.logical_and(key <= token, first)
    maxes, sums, accs = [], [], []
    for h in range(2):
        s = lax.dot_general(k_own_ref[h], q[:, h * 128:(h + 1) * 128], NT, preferred_element_type=F32)
        s = jnp.where(keep, s * LOG2_SCALE, MASKED)
        m = jnp.max(s, axis=0, keepdims=True)
        p = jnp.exp2(s - m)
        maxes.append(m)
        sums.append(jnp.sum(p, axis=0, keepdims=True))
        accs.append(lax.dot_general(v_own_ref[h], p.astype(BF16), TN, preferred_element_type=F32))
    even = lax.broadcasted_iota(jnp.int32, (8, 256), 0) % 2 == 0
    return (jnp.where(even, maxes[0], maxes[1]), jnp.where(even, sums[0], sums[1]), accs)


def block_scores(q, k_ref, s_ref, row0, limit, step=512):
    rows = k_ref.shape[0]
    even = (lax.broadcasted_iota(jnp.int32, (step, HEAD_DIM), 0) % 2 == 0)
    even_f = even.astype(F32).astype(BF16)
    odd_f = (1.0 - even.astype(F32)).astype(BF16)
    row = lax.broadcasted_iota(jnp.int32, (step, 256), 0)
    block_max = jnp.full((8, 256), MASKED, F32)
    for r in range(0, rows, step):
        k = k_ref[r:r + step, :]
        both = jnp.concatenate([k * even_f, k * odd_f], axis=1)
        s = lax.dot_general(both, q, NT, preferred_element_type=F32)
        s = jnp.where(row < limit - (row0 + r), s, MASKED)
        s_ref[r:r + step, :] = s
        block_max = jnp.maximum(block_max, jnp.max(s.reshape(step // 8, 8, 256), axis=0))
    return pair_reduce(jnp.maximum, block_max)


def block_values(v_ref, s_ref, m8, step=1024):
    rows = v_ref.shape[0]
    even = (lax.broadcasted_iota(jnp.int32, (HEAD_DIM, step), 1) % 2 == 0)
    even_f = even.astype(F32).astype(BF16)
    odd_f = (1.0 - even.astype(F32)).astype(BF16)
    l8 = jnp.zeros((8, 256), F32)
    acc = None
    for r in range(0, rows, step):
        p = jnp.exp2(s_ref[r:r + step, :].reshape(step // 8, 8, 256) * LOG2_SCALE - m8[None])
        l8 = l8 + jnp.sum(p, axis=0)
        vt = v_ref[r:r + step, :].T
        both = jnp.concatenate([vt * even_f, vt * odd_f], axis=0)
        part = jnp.dot(both, p.reshape(step, 256).astype(BF16), preferred_element_type=F32)
        acc = part if acc is None else acc + part
    return pair_reduce(jnp.add, l8), acc


def attend_kernel(prefix_ref, q_ref, k_ref, v_ref, k_own, v_own, o_ref, s_ref, m_ref, l_ref, acc_ref):
    b, j = pl.program_id(0), pl.program_id(1)
    rows = k_ref.shape[1]
    cp = lax.axis_index("cp")
    limit = 2 * prefix_ref[b] - cp * (rows * pl.num_programs(1))
    q = q_ref[0]

    @pl.when(j == 0)
    def _():
        m8, l8, accs = own_keys(q, k_own.at[0], v_own.at[0], cp == 0)
        m_ref[...] = m8
        l_ref[...] = l8
        for h in range(2):
            acc_ref[h * 128:(h + 1) * 128, :] = accs[h]

    @pl.when(j * rows < limit)
    def _():
        block_max = block_scores(q, k_ref.at[0], s_ref, j * rows, limit)
        m8 = jnp.maximum(m_ref[...], block_max * LOG2_SCALE)
        alpha = jnp.exp2(m_ref[...] - m8)
        l8, acc = block_values(v_ref.at[0], s_ref, m8)
        m_ref[...] = m8
        l_ref[...] = l_ref[...] * alpha + l8
        for h in range(2):
            part = slice(h * 128, (h + 1) * 128)
            acc_ref[part, :] = acc_ref[part, :] * alpha[h:h + 1] + acc[part]

    @pl.when(j == pl.num_programs(1) - 1)
    def _():
        sub = lax.broadcasted_iota(jnp.int32, (8, 256), 0)
        stats = jnp.where(sub < 2, m_ref[...], l_ref[...])
        for c in range(2):
            o_ref[0, c, 0:256, :] = acc_ref[:, c * 128:(c + 1) * 128]
            o_ref[0, c, 256:264, :] = stats[:, c * 128:(c + 1) * 128]


def attend(prefix_len, q, k_cache, v_cache, k_own, v_own):
    n_seq, slots = k_cache.shape[0], k_cache.shape[1]
    rows = 4096
    n_new = k_own.shape[2]
    k_rows = k_cache.reshape(n_seq, slots * 2, HEAD_DIM)
    v_rows = v_cache.reshape(n_seq, slots * 2, HEAD_DIM)
    blocks = slots * 2 // rows
    cache_spec = pl.BlockSpec((1, rows, HEAD_DIM), lambda b, j: (b, j, 0))
    own_spec = pl.BlockSpec((1, 2, n_new, HEAD_DIM), lambda b, j: (b, 0, 0, 0))
    return pl.pallas_call(
        attend_kernel,
        grid=(n_seq, blocks),
        out_shape=jax.ShapeDtypeStruct((n_seq, 2, 264, 128), F32),
        in_specs=[pl.BlockSpec(memory_space=pltpu.SMEM), pl.BlockSpec((1, 256, 256), lambda b, j: (b, 0, 0)),
                  cache_spec, cache_spec, own_spec, own_spec],
        out_specs=pl.BlockSpec((1, 2, 264, 128), lambda b, j: (b, 0, 0, 0)),
        scratch_shapes=[pltpu.VMEM((rows, 256), F32), pltpu.VMEM((8, 256), F32), pltpu.VMEM((8, 256), F32),
                        pltpu.VMEM((256, 256), F32)],
        compiler_params=pltpu.CompilerParams(vmem_limit_bytes=40 << 20),
        cost_estimate=pl.CostEstimate(flops=17 << 30, bytes_accessed=36 << 20, transcendentals=17 << 20),
        name="attend",
    )(prefix_len, q, k_rows, v_rows, k_own, v_own)


def merge(parts):
    sub = lax.broadcasted_iota(jnp.int32, (8, 128), 0)
    stats = [p[256:264, :] for p in parts]
    maxes = [jnp.where(sub % 4 < 2, s, pltpu.roll(s, 2, 0)) for s in stats]
    top = functools.reduce(jnp.maximum, maxes)
    weights = [jnp.exp2(m - top) for m in maxes]
    total = sum(w * s for w, s in zip(weights, stats))
    stats_out = jnp.where(sub < 2, top, total)
    accs = [sum(w[h:h + 1] * p[h * 128:(h + 1) * 128, :] for w, p in zip(weights, parts)) for h in range(2)]
    return accs, stats_out


def combine_kernel(part_ref, x_hbm, wo_hbm, out_ref, x_buf, wo, ra1, sa2, ra2, proj, rs_o, rs_i, fwd, og,
                   loc_sem, a1_s, a1_r, a2_s, a2_r, rs_s, rso_r, rsi_r, og_s, og_r):
    n_seq = part_ref.shape[0]
    units = n_seq // 2
    half_cols = proj.shape[-1]
    cp, z = lax.axis_index("cp"), lax.axis_index("tp")
    y, c = cp // 2, cp % 2
    is_mid = jnp.logical_and(z >= 1, z <= 2)
    is_end = jnp.logical_not(is_mid)
    near, far = z // 2, 1 - z // 2
    outer = jnp.where(z == 1, 0, 3)
    inner = jnp.where(z == 1, 2, 1)
    mid = jnp.where(z == 0, 1, 2)
    core_peer = {"cp": y * 2 + 1 - c}
    y_peer = {"cp": (1 - y) * 2 + c}
    me, yq = y * 2 + c, (1 - y) * 2 + c

    def remote(src, dst, send_sem, recv_sem, peer):
        return pltpu.make_async_remote_copy(src_ref=src, dst_ref=dst, send_sem=send_sem, recv_sem=recv_sem,
                                            device_id=peer, device_id_type=MESH)

    wo_copy = pltpu.make_async_copy(wo_hbm, wo, loc_sem.at[0])
    wo_copy.start()
    x_copies = [pltpu.make_async_copy(x_hbm.at[2 * u + y, pl.ds(32 * c, 32), :], x_buf.at[u], loc_sem.at[1 + u])
                for u in range(units)]
    for x_copy in x_copies:
        x_copy.start()

    barrier = pltpu.get_barrier_semaphore()
    pl.semaphore_signal(barrier, inc=1, device_id=core_peer, device_id_type=MESH)
    pl.semaphore_signal(barrier, inc=1, device_id=y_peer, device_id_type=MESH)

    @pl.when(is_mid)
    def _():
        pl.semaphore_signal(barrier, inc=1, device_id={"tp": outer}, device_id_type=MESH)
        pl.semaphore_signal(barrier, inc=1, device_id={"tp": inner}, device_id_type=MESH)
        pl.semaphore_wait(barrier, 4)

    @pl.when(is_end)
    def _():
        pl.semaphore_signal(barrier, inc=1, device_id={"tp": mid}, device_id_type=MESH)
        pl.semaphore_wait(barrier, 3)

    def a1(b):
        return remote(part_ref.at[b, 1 - c], ra1.at[b], a1_s.at[b], a1_r.at[b], core_peer)

    def a2(u):
        return remote(sa2.at[u], ra2.at[u], a2_s.at[u], a2_r.at[u], y_peer)

    def rs_out(u, half):
        return remote(proj.at[u, half], rs_o.at[u, half], rs_s.at[u, half], rso_r.at[u, half], {"tp": mid})

    def rs_in(u):
        return remote(fwd.at[u], rs_i.at[u], rs_s.at[u, 0], rsi_r.at[u], {"tp": inner})

    def gather(q, u, half, lane, peer):
        return remote(og.at[q, u, half], og.at[q, u, half], og_s.at[lane, u, half], og_r.at[q, u, half], peer)

    for b in range(n_seq):
        a1(b).start()

    def s1(u):
        b = 2 * u + 1 - y
        a1(b).wait_recv()
        accs, stats = merge([part_ref[b, c], ra1[b]])
        for h in range(2):
            sa2[u, h * 128:(h + 1) * 128, :] = accs[h]
        sa2[u, 256:264, :] = stats
        a2(u).start()

    def s2(u):
        b = 2 * u + y
        a1(b).wait_recv()
        a2(u).wait_recv()
        accs, stats = merge([part_ref[b, c], ra1[b], ra2[u]])
        heads = []
        for h in range(2):
            o = (accs[h] / stats[2 + h:3 + h]).T.astype(BF16)
            heads += [o[g * 32:(g + 1) * 32] for g in range(4)]
        o = jnp.concatenate(heads, axis=1)
        for half in range(2):
            proj[u, half] = jnp.dot(o, wo[:, half * half_cols:(half + 1) * half_cols], preferred_element_type=F32)

        @pl.when(is_end)
        def _():
            rs_out(u, far).start()
            rs_out(u, near).start()

    def s3(u):
        @pl.when(is_mid)
        def _():
            rs_out(u, far).wait_recv()
            fwd[u] = proj[u, far] + rs_o[u, far]
            rs_in(u).start()

    def x_half(u):
        lo = x_buf[u, :, 0:half_cols].astype(F32)
        hi = x_buf[u, :, half_cols:2 * half_cols].astype(F32)
        return jnp.where(near == 0, lo, hi)

    def s4(u):
        @pl.when(is_mid)
        def _():
            rs_out(u, near).wait_recv()
            rs_in(u).wait_recv()
            total = (proj[u, near] + rs_o[u, near]) + rs_i[u]
            og[me, u, near] = (x_half(u) + total).astype(BF16).astype(F32)
            gather(me, u, near, 2, {"tp": inner}).start()
            gather(me, u, near, 3, {"tp": outer}).start()

        @pl.when(is_end)
        def _():
            gather(me, u, near, 2, {"tp": mid}).wait_recv()

        gather(me, u, near, 1, y_peer).start()
        gather(me, u, near, 0, core_peer).start()

    def s5(u):
        gather(me, u, far, 2, {"tp": inner}).wait_recv()

        @pl.when(is_mid)
        def _():
            gather(me, u, far, 3, {"tp": outer}).start()

        gather(me, u, far, 1, y_peer).start()
        gather(me, u, far, 0, core_peer).start()

    def s6(u):
        for half in (near, far):
            gather(yq, u, half, 1, y_peer).wait_recv()
            gather(yq, u, half, 4, core_peer).start()

    def s7(u):
        for q in (y * 2 + 1 - c, (1 - y) * 2 + 1 - c):
            for half in range(2):
                gather(q, u, half, 0, core_peer).wait_recv()
        for q in range(4):
            for half in range(2):
                out_ref[2 * u + q // 2, 32 * (q % 2):32 * (q % 2) + 32, half * half_cols:(half + 1) * half_cols] = (
                    og[q, u, half].astype(BF16))

    wo_copy.wait()
    for x_copy in x_copies:
        x_copy.wait()
    stages = (s1, s2, s3, s4, s5, s6, s7)

    def slot(t, carry):
        for i, stage in enumerate(stages):
            @pl.when(jnp.logical_and(t >= i, t < units + i))
            def _(stage=stage, i=i):
                stage(t - i)
        return carry

    lax.fori_loop(0, units + len(stages) - 1, slot, 0)

    for b in range(n_seq):
        a1(b).wait_send()
    for u in range(units):
        a2(u).wait_send()
        for half in (near, far):
            gather(me, u, half, 0, core_peer).wait_send()
            gather(me, u, half, 1, y_peer).wait_send()
            gather(yq, u, half, 4, core_peer).wait_send()

    @pl.when(is_end)
    def _():
        for u in range(units):
            for half in (near, far):
                rs_out(u, half).wait_send()

    @pl.when(is_mid)
    def _():
        for u in range(units):
            rs_in(u).wait_send()
            gather(me, u, near, 2, {"tp": inner}).wait_send()
            for half in (near, far):
                gather(me, u, half, 3, {"tp": outer}).wait_send()


def combine(parts, hidden, w_o):
    n_seq, n_new, d_model = hidden.shape
    units, half = n_seq // 2, d_model // 2
    vmem = pl.BlockSpec(memory_space=pltpu.VMEM)
    hbm = pl.BlockSpec(memory_space=pl.ANY)
    dma = pltpu.SemaphoreType.DMA
    return pl.pallas_call(
        combine_kernel,
        out_shape=jax.ShapeDtypeStruct((n_seq, n_new, d_model), BF16),
        in_specs=[vmem, hbm, hbm],
        out_specs=vmem,
        scratch_shapes=[
            pltpu.VMEM((units, 32, d_model), BF16), pltpu.VMEM(w_o.shape, BF16),
            pltpu.VMEM((n_seq, 264, 128), F32), pltpu.VMEM((units, 264, 128), F32),
            pltpu.VMEM((units, 264, 128), F32), pltpu.VMEM((units, 2, 32, half), F32),
            pltpu.VMEM((units, 2, 32, half), F32), pltpu.VMEM((units, 32, half), F32),
            pltpu.VMEM((units, 32, half), F32), pltpu.VMEM((4, units, 2, 32, half), F32),
            dma((1 + units,)), dma((n_seq,)), dma((n_seq,)), dma((units,)), dma((units,)), dma((units, 2)),
            dma((units, 2)), dma((units,)), dma((5, units, 2)), dma((4, units, 2))],
        compiler_params=pltpu.CompilerParams(collective_id=0, has_side_effects=True, vmem_limit_bytes=48 << 20),
        cost_estimate=pl.CostEstimate(flops=2 << 30, bytes_accessed=10 << 20, transcendentals=0),
        name="combine",
    )(parts, hidden, w_o)


def solution(mesh):
    def per_device(hidden, prefix_len, k_cache, v_cache, attn_norm, w_q, w_k, w_v, w_o, q_norm, k_norm):
        q, k_own, v_own = project(hidden, prefix_len, attn_norm, w_q, w_k, w_v, q_norm, k_norm)
        parts = attend(prefix_len, q, k_cache, v_cache, k_own, v_own)
        block_out = combine(parts, hidden, w_o)
        return block_out, k_own.transpose(0, 2, 1, 3), v_own.transpose(0, 2, 1, 3)

    cache_spec = P('dp', 'cp', 'tp', None)
    arg_specs = (P('dp', None, None), P('dp'), cache_spec, cache_spec, P(None), P(None, 'tp'), P(None, 'tp'), P(None, 'tp'), P('tp', None), P(None), P(None))
    out_specs = (P('dp', None, None), P('dp', None, 'tp', None), P('dp', None, 'tp', None))
    return jax.shard_map(per_device, mesh=mesh, in_specs=arg_specs, out_specs=out_specs, check_vma=False)
```

```python
import functools

import jax
import jax.numpy as jnp
import numpy as np
from jax import lax
from jax.experimental import pallas as pl
from jax.experimental.pallas import tpu as pltpu
from jax.sharding import PartitionSpec as P

HEAD_DIM = 128
MASKED = -1e30
EPS = 1e-6
LOG2_SCALE = float(HEAD_DIM ** -0.5 / np.log(2.0))
MESH = pl.DeviceIdType.MESH
NT = (((1,), (1,)), ((), ()))
TN = (((0,), (0,)), ((), ()))
F32 = jnp.float32
BF16 = jnp.bfloat16
VMEM_LIMIT = 67043328


def cos_or_sin(x, want_cos):
    quarter = jnp.floor(x * F32(2.0 / np.pi) + F32(0.5))
    r = ((x - quarter * F32(1.5703125)) - quarter * F32(4.8351287841796875e-4)) - quarter * F32(3.13855707645416259765625e-7)
    r = r - quarter * F32(6.077100628276710381e-11)
    n = quarter.astype(jnp.int32) + want_cos.astype(jnp.int32)
    r2 = r * r
    sin_r = r + r * r2 * (F32(-1.6666654611e-1) + r2 * (F32(8.3321608736e-3) + r2 * F32(-1.9515295891e-4)))
    cos_r = 1.0 - 0.5 * r2 + r2 * r2 * (F32(4.166664568298827e-2) + r2 * (F32(-1.388731625493765e-3) + r2 * F32(2.443315711809948e-5)))
    y = jnp.where(n % 2 == 0, sin_r, cos_r)
    return jnp.where(n % 4 >= 2, -y, y)


def project_kernel(prefix_ref, x_ref, an_ref, wq_hbm, wk_hbm, wv_hbm, qn_ref, kn_ref, freq_ref,
                   q_ref, k_ref, v_ref, wq, wk, wv, normed, cos_ref, sin_ref, sems):
    n_seq, n_new = k_ref.shape[0], k_ref.shape[2]
    rows = n_seq * n_new
    copies = [pltpu.make_async_copy(wq_hbm.at[:, pl.ds(256 * j, 256)], wq.at[j], sems.at[j]) for j in range(4)]
    copies.append(pltpu.make_async_copy(wk_hbm, wk, sems.at[4]))
    copies.append(pltpu.make_async_copy(wv_hbm, wv, sems.at[5]))
    for c in copies:
        c.start()
    for r in range(0, rows, 64):
        x = x_ref[r:r + 64, :].astype(F32)
        scale = lax.rsqrt(jnp.mean(x * x, axis=-1, keepdims=True) + EPS)
        normed[r:r + 64, :] = (x * scale * an_ref[...].astype(F32)).astype(BF16)
    low = lax.broadcasted_iota(jnp.int32, (n_new, HEAD_DIM), 1) < HEAD_DIM // 2
    step = lax.broadcasted_iota(jnp.int32, (n_new, HEAD_DIM), 0)
    for b in range(n_seq):
        angle = (prefix_ref[b] + step).astype(F32) * freq_ref[...]
        trig = cos_or_sin(angle, low)
        turned = pltpu.roll(trig, HEAD_DIM // 2, 1)
        cos_ref[b * n_new:(b + 1) * n_new, :] = jnp.where(low, trig, turned)
        sin_ref[b * n_new:(b + 1) * n_new, :] = jnp.where(low, -turned, trig)

    def norm_rope(y, gain_ref):
        y = y.astype(BF16).astype(F32)
        y = y * lax.rsqrt(jnp.mean(y * y, axis=-1, keepdims=True) + EPS) * gain_ref[...].astype(F32)
        return (y * cos_ref[...] + pltpu.roll(y, HEAD_DIM // 2, 1) * sin_ref[...]).astype(BF16)

    for j in range(4):
        copies[j].wait()
        y = jnp.dot(normed[...], wq[j], preferred_element_type=F32)
        for i in range(2):
            h, g = j // 2, 2 * (j % 2) + i
            head = norm_rope(y[:, i * HEAD_DIM:(i + 1) * HEAD_DIM], qn_ref)
            for b in range(n_seq):
                for c in range(2):
                    q_ref[b, c * 128 + g * 32:c * 128 + g * 32 + 32, h * 128:(h + 1) * 128] = (
                        head[b * 64 + c * 32:b * 64 + c * 32 + 32])
    copies[4].wait()
    y = jnp.dot(normed[...], wk[...], preferred_element_type=F32)
    for h in range(2):
        head = norm_rope(y[:, h * HEAD_DIM:(h + 1) * HEAD_DIM], kn_ref)
        for b in range(n_seq):
            k_ref[b, h] = head[b * 64:(b + 1) * 64]
    copies[5].wait()
    y = jnp.dot(normed[...], wv[...], preferred_element_type=F32).astype(BF16)
    for h in range(2):
        for b in range(n_seq):
            v_ref[b, h] = y[b * 64:(b + 1) * 64, h * HEAD_DIM:(h + 1) * HEAD_DIM]


def project(hidden, prefix_len, attn_norm, w_q, w_k, w_v, q_norm, k_norm):
    n_seq, n_new, d_model = hidden.shape
    freq = 1.0 / (1000000.0 ** (np.arange(HEAD_DIM // 2, dtype=np.float64) * 2.0 / HEAD_DIM))
    freq = jnp.asarray(np.concatenate([freq, freq])[None].astype(np.float32))
    vmem = pl.BlockSpec(memory_space=pltpu.VMEM)
    hbm = pl.BlockSpec(memory_space=pl.ANY)
    rows = n_seq * n_new
    return pl.pallas_call(
        project_kernel,
        out_shape=(jax.ShapeDtypeStruct((n_seq, 256, 256), BF16),
                   jax.ShapeDtypeStruct((n_seq, 2, n_new, HEAD_DIM), BF16),
                   jax.ShapeDtypeStruct((n_seq, 2, n_new, HEAD_DIM), BF16)),
        in_specs=[pl.BlockSpec(memory_space=pltpu.SMEM), vmem, vmem, hbm, hbm, hbm, vmem, vmem, vmem],
        out_specs=(vmem, vmem, vmem),
        scratch_shapes=[pltpu.VMEM((4, d_model, 256), BF16), pltpu.VMEM((d_model, 256), BF16),
                        pltpu.VMEM((d_model, 256), BF16), pltpu.VMEM((rows, d_model), BF16),
                        pltpu.VMEM((rows, HEAD_DIM), F32), pltpu.VMEM((rows, HEAD_DIM), F32),
                        pltpu.SemaphoreType.DMA((6,))],
        compiler_params=pltpu.CompilerParams(vmem_limit_bytes=VMEM_LIMIT),
        cost_estimate=pl.CostEstimate(flops=2 * rows * d_model * 1536, bytes_accessed=12 << 20, transcendentals=0),
        name="project",
    )(prefix_len, hidden.reshape(rows, d_model), attn_norm[None], w_q, w_k, w_v, q_norm[None], k_norm[None], freq)


CHUNK = 2048
SLOTS = 4


def pair_reduce(op, x):
    x = op(x, pltpu.roll(x, 2, 0))
    return op(x, pltpu.roll(x, 4, 0))


def split_heads(x, par_ref):
    return jnp.concatenate([x * par_ref[h] for h in range(2)], axis=1)


def own_keys(q, k_own_ref, v_own_ref):
    n_new = k_own_ref.shape[-2]
    key = lax.broadcasted_iota(jnp.int32, (n_new, 256), 0)
    col = lax.broadcasted_iota(jnp.int32, (n_new, 256), 1)
    keep = key <= (col // 128) * 32 + col % 32
    maxes, sums, accs = [], [], []
    for h in range(2):
        s = lax.dot_general(k_own_ref[h], q[:, h * 128:(h + 1) * 128], NT, preferred_element_type=F32)
        s = jnp.where(keep, s * LOG2_SCALE, MASKED)
        m = jnp.max(s, axis=0, keepdims=True)
        p = jnp.exp2(s - m)
        maxes.append(m)
        sums.append(jnp.sum(p, axis=0, keepdims=True))
        accs.append(lax.dot_general(v_own_ref[h], p.astype(BF16), TN, preferred_element_type=F32))
    even = lax.broadcasted_iota(jnp.int32, (8, 256), 0) % 2 == 0
    return (jnp.where(even, maxes[0], maxes[1]), jnp.where(even, sums[0], sums[1]), accs)


def attend_step(it, n_seq, per_seq, limit_of, q_all, k_ref, v_ref, k_own, v_own, par_ref, emit,
                s_a, s_b, m_ref, l_ref, acc_ref, m_own, l_own, acc_own):
    cp = lax.axis_index("cp")
    s_refs = (s_a, s_b)

    @pl.when(it == 0)
    def _():
        even = (lax.broadcasted_iota(jnp.int32, (CHUNK, HEAD_DIM), 0) % 2 == 0).astype(F32)
        par_ref[0] = even.astype(BF16)
        par_ref[1] = (1.0 - even).astype(BF16)
        acc_ref[...] = jnp.zeros_like(acc_ref)
        l_ref[...] = jnp.zeros_like(l_ref)

        @pl.when(cp == 0)
        def _():
            for b in range(n_seq):
                m8, l8, accs = own_keys(q_all[b], k_own.at[b], v_own.at[b])
                m_own[b] = m8
                l_own[b] = l8
                for h in range(2):
                    acc_own[b, h * 128:(h + 1) * 128, :] = accs[h]

        @pl.when(cp != 0)
        def _():
            m_own[...] = jnp.full_like(m_own, MASKED)
            l_own[...] = jnp.zeros_like(l_own)
            acc_own[...] = jnp.zeros_like(acc_own)

    b_new, i = it // per_seq, it % per_seq
    b_old = b_new - 1
    rows = pl.ds(pl.multiple_of(i * CHUNK, CHUNK), CHUNK)

    def score_dot():
        both = split_heads(k_ref[...], par_ref)
        return lax.dot_general(both, q_all[b_new], NT, preferred_element_type=F32)

    def score_post(s, par):
        keep = lax.broadcasted_iota(jnp.int32, (CHUNK, 128), 0) < limit_of(b_new) - i * CHUNK
        s = jnp.concatenate([jnp.where(keep, s[:, 0:128], MASKED), jnp.where(keep, s[:, 128:256], MASKED)], axis=1)
        s_refs[par][rows, :] = s
        top = pair_reduce(jnp.maximum, jnp.max(s.reshape(CHUNK // 8, 8, 256), axis=0)) * LOG2_SCALE
        m_ref[par] = jnp.maximum(jnp.where(i == 0, m_own[b_new], m_ref[par]), top)

    def expo(par):
        s = s_refs[par][rows, :]
        p = jnp.exp2(s.reshape(CHUNK // 8, 8, 256) * LOG2_SCALE - m_ref[par][None])
        l_ref[par] = jnp.where(i == 0, 0.0, l_ref[par]) + jnp.sum(p, axis=0)
        return p.reshape(CHUNK, 256).astype(BF16)

    def value(p):
        both = split_heads(v_ref[...], par_ref)
        part = lax.dot_general(both, p, TN, preferred_element_type=F32)
        acc_ref[...] = jnp.where(i == 0, 0.0, acc_ref[...]) + part

    total = n_seq * per_seq
    scoring, adding = it < total, jnp.logical_and(it >= per_seq, it < total + per_seq)
    for par in range(2):
        @pl.when(b_new % 2 == par)
        def _(par=par):
            main = jnp.logical_and(scoring, adding)

            @pl.when(main)
            def _():
                s = score_dot()
                p = expo(1 - par)
                value(p)
                score_post(s, par)

            @pl.when(jnp.logical_and(scoring, jnp.logical_not(adding)))
            def _():
                score_post(score_dot(), par)

            @pl.when(jnp.logical_and(adding, jnp.logical_not(scoring)))
            def _():
                value(expo(1 - par))

    @pl.when(jnp.logical_and(adding, i == per_seq - 1))
    def _():
        b = b_old
        m8 = m_ref[b % 2]
        w = jnp.exp2(m_own[b] - m8)
        l8 = pair_reduce(jnp.add, l_ref[b % 2]) + w * l_own[b]
        sub = lax.broadcasted_iota(jnp.int32, (8, 256), 0)
        stats = jnp.where(sub < 2, m8, l8)
        accs = [acc_ref[h * 128:(h + 1) * 128, :] + w[h:h + 1] * acc_own[b, h * 128:(h + 1) * 128, :] for h in range(2)]
        emit(b, accs, stats)


def attend_kernel(prefix_ref, q_ref, k_hbm, v_hbm, k_own, v_own, o_ref, par_ref, k_buf, v_buf, k_sem, v_sem, *scratch):
    n_seq = q_ref.shape[0]
    per_seq = pl.num_programs(0) // (n_seq + 1)
    it = pl.program_id(0)
    cp = lax.axis_index("cp")
    fetch(it, n_seq * per_seq, per_seq, k_hbm, v_hbm, k_buf, v_buf, k_sem, v_sem)

    def emit(b, accs, stats):
        for c in range(2):
            for h in range(2):
                o_ref[b, c, h * 128:(h + 1) * 128, :] = accs[h][:, c * 128:(c + 1) * 128]
            o_ref[b, c, 256:264, :] = stats[:, c * 128:(c + 1) * 128]

    attend_step(it, n_seq, per_seq, lambda b: 2 * prefix_ref[b] - cp * (per_seq * CHUNK), q_ref, k_buf.at[it % SLOTS],
                v_buf.at[it % SLOTS], k_own, v_own, par_ref, emit, *scratch)


def fetch(it, total, per_seq, k_hbm, v_hbm, k_buf, v_buf, k_sem, v_sem):
    def copy(hbm, buf, sem, lag, step):
        j = step - lag
        src = hbm.at[j // per_seq, pl.ds(pl.multiple_of((j % per_seq) * CHUNK, CHUNK), CHUNK), :]
        return pltpu.make_async_copy(src, buf.at[step % SLOTS], sem.at[step % SLOTS])

    for hbm, buf, sem, lag in ((k_hbm, k_buf, k_sem, 0), (v_hbm, v_buf, v_sem, per_seq)):
        if lag == 0:
            @pl.when(it == 0)
            def _():
                for step in range(SLOTS - 1):
                    copy(hbm, buf, sem, lag, step).start()
        ahead = it + SLOTS - 1

        @pl.when(jnp.logical_and(ahead >= lag, ahead < total + lag))
        def _():
            copy(hbm, buf, sem, lag, ahead).start()

        @pl.when(jnp.logical_and(it >= lag, it < total + lag))
        def _():
            copy(hbm, buf, sem, lag, it).wait()


def attend(prefix_len, q, k_cache, v_cache, k_own, v_own):
    n_seq, slots = k_cache.shape[0], k_cache.shape[1]
    k_rows = k_cache.reshape(n_seq, slots * 2, HEAD_DIM)
    v_rows = v_cache.reshape(n_seq, slots * 2, HEAD_DIM)
    per_seq = slots * 2 // CHUNK
    total = n_seq * per_seq

    vmem = pl.BlockSpec(memory_space=pltpu.VMEM)
    return pl.pallas_call(
        attend_kernel,
        grid=(total + per_seq,),
        out_shape=jax.ShapeDtypeStruct((n_seq, 2, 264, 128), F32),
        in_specs=[pl.BlockSpec(memory_space=pltpu.SMEM), vmem,
                  pl.BlockSpec(memory_space=pl.ANY), pl.BlockSpec(memory_space=pl.ANY), vmem, vmem],
        out_specs=vmem,
        scratch_shapes=[pltpu.VMEM((2, CHUNK, HEAD_DIM), BF16), pltpu.VMEM((SLOTS, CHUNK, HEAD_DIM), BF16), pltpu.VMEM((SLOTS, CHUNK, HEAD_DIM), BF16),
                        pltpu.SemaphoreType.DMA((SLOTS,)), pltpu.SemaphoreType.DMA((SLOTS,)),
                        pltpu.VMEM((slots * 2, 256), F32), pltpu.VMEM((slots * 2, 256), F32),
                        pltpu.VMEM((2, 8, 256), F32), pltpu.VMEM((2, 8, 256), F32), pltpu.VMEM((256, 256), F32),
                        pltpu.VMEM((n_seq, 8, 256), F32), pltpu.VMEM((n_seq, 8, 256), F32),
                        pltpu.VMEM((n_seq, 256, 256), F32)],
        compiler_params=pltpu.CompilerParams(vmem_limit_bytes=VMEM_LIMIT),
        cost_estimate=pl.CostEstimate(flops=17 << 30, bytes_accessed=36 << 20, transcendentals=17 << 20),
        name="attend",
    )(prefix_len, q, k_rows, v_rows, k_own, v_own)


def merge(parts):
    sub = lax.broadcasted_iota(jnp.int32, (8, 128), 0)
    stats = [p[256:264, :] for p in parts]
    maxes = [jnp.where(sub % 4 < 2, s, pltpu.roll(s, 2, 0)) for s in stats]
    top = functools.reduce(jnp.maximum, maxes)
    weights = [jnp.exp2(m - top) for m in maxes]
    total = sum(w * s for w, s in zip(weights, stats))
    stats_out = jnp.where(sub < 2, top, total)
    accs = [sum(w[h:h + 1] * p[h * 128:(h + 1) * 128, :] for w, p in zip(weights, parts)) for h in range(2)]
    return accs, stats_out


def combine_kernel(part_ref, x_hbm, wo_hbm, out_ref, x_buf, wo, ra1, sa2, ra2, proj, rs_o, rs_i, fwd, og,
                   loc_sem, a1_s, a1_r, a2_s, a2_r, rs_s, rso_r, rsi_r, og_s, og_r):
    n_seq = part_ref.shape[0]
    units = n_seq // 2
    half_cols = proj.shape[-1]
    cp, z = lax.axis_index("cp"), lax.axis_index("tp")
    y, c = cp // 2, cp % 2
    is_mid = jnp.logical_and(z >= 1, z <= 2)
    is_end = jnp.logical_not(is_mid)
    near, far = z // 2, 1 - z // 2
    outer = jnp.where(z == 1, 0, 3)
    inner = jnp.where(z == 1, 2, 1)
    mid = jnp.where(z == 0, 1, 2)
    core_peer = {"cp": y * 2 + 1 - c}
    y_peer = {"cp": (1 - y) * 2 + c}
    me, yq = y * 2 + c, (1 - y) * 2 + c

    def remote(src, dst, send_sem, recv_sem, peer):
        return pltpu.make_async_remote_copy(src_ref=src, dst_ref=dst, send_sem=send_sem, recv_sem=recv_sem,
                                            device_id=peer, device_id_type=MESH)

    wo_copy = pltpu.make_async_copy(wo_hbm, wo, loc_sem.at[0])
    wo_copy.start()
    x_copies = [pltpu.make_async_copy(x_hbm.at[2 * u + y, pl.ds(32 * c, 32), :], x_buf.at[u], loc_sem.at[1 + u])
                for u in range(units)]
    for x_copy in x_copies:
        x_copy.start()

    barrier = pltpu.get_barrier_semaphore()
    pl.semaphore_signal(barrier, inc=1, device_id=core_peer, device_id_type=MESH)
    pl.semaphore_signal(barrier, inc=1, device_id=y_peer, device_id_type=MESH)

    @pl.when(is_mid)
    def _():
        pl.semaphore_signal(barrier, inc=1, device_id={"tp": outer}, device_id_type=MESH)
        pl.semaphore_signal(barrier, inc=1, device_id={"tp": inner}, device_id_type=MESH)
        pl.semaphore_wait(barrier, 4)

    @pl.when(is_end)
    def _():
        pl.semaphore_signal(barrier, inc=1, device_id={"tp": mid}, device_id_type=MESH)
        pl.semaphore_wait(barrier, 3)

    def a1(b):
        return remote(part_ref.at[b, 1 - c], ra1.at[b], a1_s.at[b], a1_r.at[b], core_peer)

    def a2(u):
        return remote(sa2.at[u], ra2.at[u], a2_s.at[u], a2_r.at[u], y_peer)

    def rs_out(u, half):
        return remote(proj.at[u, half], rs_o.at[u, half], rs_s.at[u, half], rso_r.at[u, half], {"tp": mid})

    def rs_in(u):
        return remote(fwd.at[u], rs_i.at[u], rs_s.at[u, 0], rsi_r.at[u], {"tp": inner})

    def gather(q, u, half, lane, peer):
        return remote(og.at[q, u, half], og.at[q, u, half], og_s.at[lane, u, half], og_r.at[q, u, half], peer)

    for b in range(n_seq):
        a1(b).start()

    def s1(u):
        b = 2 * u + 1 - y
        a1(b).wait_recv()
        accs, stats = merge([part_ref[b, c], ra1[b]])
        for h in range(2):
            sa2[u, h * 128:(h + 1) * 128, :] = accs[h]
        sa2[u, 256:264, :] = stats
        a2(u).start()

    def s2(u):
        b = 2 * u + y
        a1(b).wait_recv()
        a2(u).wait_recv()
        accs, stats = merge([part_ref[b, c], ra1[b], ra2[u]])
        heads = []
        for h in range(2):
            o = (accs[h] / stats[2 + h:3 + h]).T.astype(BF16)
            heads += [o[g * 32:(g + 1) * 32] for g in range(4)]
        o = jnp.concatenate(heads, axis=1)
        for half in range(2):
            proj[u, half] = jnp.dot(o, wo[:, half * half_cols:(half + 1) * half_cols], preferred_element_type=F32)

        @pl.when(is_end)
        def _():
            rs_out(u, far).start()
            rs_out(u, near).start()

    def s3(u):
        @pl.when(is_mid)
        def _():
            rs_out(u, far).wait_recv()
            fwd[u] = proj[u, far] + rs_o[u, far]
            rs_in(u).start()

    def x_half(u):
        lo = x_buf[u, :, 0:half_cols].astype(F32)
        hi = x_buf[u, :, half_cols:2 * half_cols].astype(F32)
        return jnp.where(near == 0, lo, hi)

    def s4(u):
        @pl.when(is_mid)
        def _():
            rs_out(u, near).wait_recv()
            rs_in(u).wait_recv()
            total = (proj[u, near] + rs_o[u, near]) + rs_i[u]
            og[me, u, near] = (x_half(u) + total).astype(BF16).astype(F32)
            gather(me, u, near, 2, {"tp": inner}).start()
            gather(me, u, near, 3, {"tp": outer}).start()

        @pl.when(is_end)
        def _():
            gather(me, u, near, 2, {"tp": mid}).wait_recv()

        gather(me, u, near, 1, y_peer).start()
        gather(me, u, near, 0, core_peer).start()

    def s5(u):
        gather(me, u, far, 2, {"tp": inner}).wait_recv()

        @pl.when(is_mid)
        def _():
            gather(me, u, far, 3, {"tp": outer}).start()

        gather(me, u, far, 1, y_peer).start()
        gather(me, u, far, 0, core_peer).start()

    def s6(u):
        for half in (near, far):
            gather(yq, u, half, 1, y_peer).wait_recv()
            gather(yq, u, half, 4, core_peer).start()

    def s7(u):
        for q in (y * 2 + 1 - c, (1 - y) * 2 + 1 - c):
            for half in range(2):
                gather(q, u, half, 0, core_peer).wait_recv()
        for q in range(4):
            for half in range(2):
                out_ref[2 * u + q // 2, 32 * (q % 2):32 * (q % 2) + 32, half * half_cols:(half + 1) * half_cols] = (
                    og[q, u, half].astype(BF16))

    wo_copy.wait()
    for x_copy in x_copies:
        x_copy.wait()
    stages = (s1, s2, s3, s4, s5, s6, s7)

    def slot(t, carry):
        for i, stage in enumerate(stages):
            @pl.when(jnp.logical_and(t >= i, t < units + i))
            def _(stage=stage, i=i):
                stage(t - i)
        return carry

    lax.fori_loop(0, units + len(stages) - 1, slot, 0)

    for b in range(n_seq):
        a1(b).wait_send()
    for u in range(units):
        a2(u).wait_send()
        for half in (near, far):
            gather(me, u, half, 0, core_peer).wait_send()
            gather(me, u, half, 1, y_peer).wait_send()
            gather(yq, u, half, 4, core_peer).wait_send()

    @pl.when(is_end)
    def _():
        for u in range(units):
            for half in (near, far):
                rs_out(u, half).wait_send()

    @pl.when(is_mid)
    def _():
        for u in range(units):
            rs_in(u).wait_send()
            gather(me, u, near, 2, {"tp": inner}).wait_send()
            for half in (near, far):
                gather(me, u, half, 3, {"tp": outer}).wait_send()


def combine(parts, hidden, w_o):
    n_seq, n_new, d_model = hidden.shape
    units, half = n_seq // 2, d_model // 2
    vmem = pl.BlockSpec(memory_space=pltpu.VMEM)
    hbm = pl.BlockSpec(memory_space=pl.ANY)
    dma = pltpu.SemaphoreType.DMA
    return pl.pallas_call(
        combine_kernel,
        out_shape=jax.ShapeDtypeStruct((n_seq, n_new, d_model), BF16),
        in_specs=[vmem, hbm, hbm],
        out_specs=vmem,
        scratch_shapes=[
            pltpu.VMEM((units, 32, d_model), BF16), pltpu.VMEM(w_o.shape, BF16),
            pltpu.VMEM((n_seq, 264, 128), F32), pltpu.VMEM((units, 264, 128), F32),
            pltpu.VMEM((units, 264, 128), F32), pltpu.VMEM((units, 2, 32, half), F32),
            pltpu.VMEM((units, 2, 32, half), F32), pltpu.VMEM((units, 32, half), F32),
            pltpu.VMEM((units, 32, half), F32), pltpu.VMEM((4, units, 2, 32, half), F32),
            dma((1 + units,)), dma((n_seq,)), dma((n_seq,)), dma((units,)), dma((units,)), dma((units, 2)),
            dma((units, 2)), dma((units,)), dma((5, units, 2)), dma((4, units, 2))],
        compiler_params=pltpu.CompilerParams(collective_id=0, has_side_effects=True, vmem_limit_bytes=VMEM_LIMIT),
        cost_estimate=pl.CostEstimate(flops=2 << 30, bytes_accessed=10 << 20, transcendentals=0),
        name="combine",
    )(parts, hidden, w_o)


def solution(mesh):
    def per_device(hidden, prefix_len, k_cache, v_cache, attn_norm, w_q, w_k, w_v, w_o, q_norm, k_norm):
        q, k_own, v_own = project(hidden, prefix_len, attn_norm, w_q, w_k, w_v, q_norm, k_norm)
        parts = attend(prefix_len, q, k_cache, v_cache, k_own, v_own)
        block_out = combine(parts, hidden, w_o)
        return block_out, k_own.transpose(0, 2, 1, 3), v_own.transpose(0, 2, 1, 3)

    cache_spec = P('dp', 'cp', 'tp', None)
    arg_specs = (P('dp', None, None), P('dp'), cache_spec, cache_spec, P(None), P(None, 'tp'), P(None, 'tp'), P(None, 'tp'), P('tp', None), P(None), P(None))
    out_specs = (P('dp', None, None), P('dp', None, 'tp', None), P('dp', None, 'tp', None))
    return jax.shard_map(per_device, mesh=mesh, in_specs=arg_specs, out_specs=out_specs, check_vma=False)
```

```python
import functools

import jax
import jax.numpy as jnp
import numpy as np
from jax import lax
from jax.experimental import pallas as pl
from jax.experimental.pallas import tpu as pltpu
from jax.sharding import PartitionSpec as P

HEAD_DIM = 128
MASKED = -1e30
EPS = 1e-6
LOG2_SCALE = float(HEAD_DIM ** -0.5 / np.log(2.0))
MESH = pl.DeviceIdType.MESH
NT = (((1,), (1,)), ((), ()))
TN = (((0,), (0,)), ((), ()))
F32 = jnp.float32
BF16 = jnp.bfloat16
VMEM_LIMIT = 67043328


def cos_or_sin(x, want_cos):
    quarter = jnp.floor(x * F32(2.0 / np.pi) + F32(0.5))
    r = ((x - quarter * F32(1.5703125)) - quarter * F32(4.8351287841796875e-4)) - quarter * F32(3.13855707645416259765625e-7)
    r = r - quarter * F32(6.077100628276710381e-11)
    n = quarter.astype(jnp.int32) + want_cos.astype(jnp.int32)
    r2 = r * r
    sin_r = r + r * r2 * (F32(-1.6666654611e-1) + r2 * (F32(8.3321608736e-3) + r2 * F32(-1.9515295891e-4)))
    cos_r = 1.0 - 0.5 * r2 + r2 * r2 * (F32(4.166664568298827e-2) + r2 * (F32(-1.388731625493765e-3) + r2 * F32(2.443315711809948e-5)))
    y = jnp.where(n % 2 == 0, sin_r, cos_r)
    return jnp.where(n % 4 >= 2, -y, y)


def project_kernel(prefix_ref, x_ref, an_ref, wq_hbm, wk_hbm, wv_hbm, qn_ref, kn_ref, freq_ref,
                   q_ref, k_ref, v_ref, wq, wk, wv, normed, cos_ref, sin_ref, sems):
    n_seq, n_new = k_ref.shape[0], k_ref.shape[2]
    rows = n_seq * n_new
    copies = [pltpu.make_async_copy(wq_hbm.at[:, pl.ds(256 * j, 256)], wq.at[j], sems.at[j]) for j in range(4)]
    copies.append(pltpu.make_async_copy(wk_hbm, wk, sems.at[4]))
    copies.append(pltpu.make_async_copy(wv_hbm, wv, sems.at[5]))
    for c in copies:
        c.start()
    for r in range(0, rows, 64):
        x = x_ref[r:r + 64, :].astype(F32)
        scale = lax.rsqrt(jnp.mean(x * x, axis=-1, keepdims=True) + EPS)
        normed[r:r + 64, :] = (x * scale * an_ref[...].astype(F32)).astype(BF16)
    low = lax.broadcasted_iota(jnp.int32, (n_new, HEAD_DIM), 1) < HEAD_DIM // 2
    step = lax.broadcasted_iota(jnp.int32, (n_new, HEAD_DIM), 0)
    for b in range(n_seq):
        angle = (prefix_ref[b] + step).astype(F32) * freq_ref[...]
        trig = cos_or_sin(angle, low)
        turned = pltpu.roll(trig, HEAD_DIM // 2, 1)
        cos_ref[b * n_new:(b + 1) * n_new, :] = jnp.where(low, trig, turned)
        sin_ref[b * n_new:(b + 1) * n_new, :] = jnp.where(low, -turned, trig)

    def norm_rope(y, gain_ref):
        y = y.astype(BF16).astype(F32)
        y = y * lax.rsqrt(jnp.mean(y * y, axis=-1, keepdims=True) + EPS) * gain_ref[...].astype(F32)
        return (y * cos_ref[...] + pltpu.roll(y, HEAD_DIM // 2, 1) * sin_ref[...]).astype(BF16)

    for j in range(4):
        copies[j].wait()
        y = jnp.dot(normed[...], wq[j], preferred_element_type=F32)
        for i in range(2):
            h, g = j // 2, 2 * (j % 2) + i
            head = norm_rope(y[:, i * HEAD_DIM:(i + 1) * HEAD_DIM], qn_ref)
            for b in range(n_seq):
                for c in range(2):
                    q_ref[b, c * 128 + g * 32:c * 128 + g * 32 + 32, h * 128:(h + 1) * 128] = (
                        head[b * 64 + c * 32:b * 64 + c * 32 + 32])
    copies[4].wait()
    y = jnp.dot(normed[...], wk[...], preferred_element_type=F32)
    for h in range(2):
        head = norm_rope(y[:, h * HEAD_DIM:(h + 1) * HEAD_DIM], kn_ref)
        for b in range(n_seq):
            k_ref[b, h] = head[b * 64:(b + 1) * 64]
    copies[5].wait()
    y = jnp.dot(normed[...], wv[...], preferred_element_type=F32).astype(BF16)
    for h in range(2):
        for b in range(n_seq):
            v_ref[b, h] = y[b * 64:(b + 1) * 64, h * HEAD_DIM:(h + 1) * HEAD_DIM]


def project(hidden, prefix_len, attn_norm, w_q, w_k, w_v, q_norm, k_norm):
    n_seq, n_new, d_model = hidden.shape
    freq = 1.0 / (1000000.0 ** (np.arange(HEAD_DIM // 2, dtype=np.float64) * 2.0 / HEAD_DIM))
    freq = jnp.asarray(np.concatenate([freq, freq])[None].astype(np.float32))
    vmem = pl.BlockSpec(memory_space=pltpu.VMEM)
    hbm = pl.BlockSpec(memory_space=pl.ANY)
    rows = n_seq * n_new
    return pl.pallas_call(
        project_kernel,
        out_shape=(jax.ShapeDtypeStruct((n_seq, 256, 256), BF16),
                   jax.ShapeDtypeStruct((n_seq, 2, n_new, HEAD_DIM), BF16),
                   jax.ShapeDtypeStruct((n_seq, 2, n_new, HEAD_DIM), BF16)),
        in_specs=[pl.BlockSpec(memory_space=pltpu.SMEM), vmem, vmem, hbm, hbm, hbm, vmem, vmem, vmem],
        out_specs=(vmem, vmem, vmem),
        scratch_shapes=[pltpu.VMEM((4, d_model, 256), BF16), pltpu.VMEM((d_model, 256), BF16),
                        pltpu.VMEM((d_model, 256), BF16), pltpu.VMEM((rows, d_model), BF16),
                        pltpu.VMEM((rows, HEAD_DIM), F32), pltpu.VMEM((rows, HEAD_DIM), F32),
                        pltpu.SemaphoreType.DMA((6,))],
        compiler_params=pltpu.CompilerParams(vmem_limit_bytes=VMEM_LIMIT),
        cost_estimate=pl.CostEstimate(flops=2 * rows * d_model * 1536, bytes_accessed=12 << 20, transcendentals=0),
        name="project",
    )(prefix_len, hidden.reshape(rows, d_model), attn_norm[None], w_q, w_k, w_v, q_norm[None], k_norm[None], freq)


CHUNK = 2048
SLOTS = 4


def pair_reduce(op, x):
    x = op(x, pltpu.roll(x, 2, 0))
    return op(x, pltpu.roll(x, 4, 0))


def split_heads(x, par_ref):
    return jnp.concatenate([x * par_ref[h] for h in range(2)], axis=1)


def own_keys(q, k_own_ref, v_own_ref):
    n_new = k_own_ref.shape[-2]
    key = lax.broadcasted_iota(jnp.int32, (n_new, 256), 0)
    col = lax.broadcasted_iota(jnp.int32, (n_new, 256), 1)
    keep = key <= (col // 128) * 32 + col % 32
    maxes, sums, accs = [], [], []
    for h in range(2):
        s = lax.dot_general(k_own_ref[h], q[:, h * 128:(h + 1) * 128], NT, preferred_element_type=F32)
        s = jnp.where(keep, s * LOG2_SCALE, MASKED)
        m = jnp.max(s, axis=0, keepdims=True)
        p = jnp.exp2(s - m)
        maxes.append(m)
        sums.append(jnp.sum(p, axis=0, keepdims=True))
        accs.append(lax.dot_general(v_own_ref[h], p.astype(BF16), TN, preferred_element_type=F32))
    even = lax.broadcasted_iota(jnp.int32, (8, 256), 0) % 2 == 0
    return (jnp.where(even, maxes[0], maxes[1]), jnp.where(even, sums[0], sums[1]), accs)


def attend_step(it, n_seq, per_seq, limit_of, q_all, k_ref, v_ref, k_own, v_own, par_ref, emit,
                s_a, s_b, m_ref, l_ref, acc_ref, m_own, l_own, acc_own):
    cp = lax.axis_index("cp")
    s_refs = (s_a, s_b)

    @pl.when(it == 0)
    def _():
        even = (lax.broadcasted_iota(jnp.int32, (CHUNK, HEAD_DIM), 0) % 2 == 0).astype(F32)
        par_ref[0] = even.astype(BF16)
        par_ref[1] = (1.0 - even).astype(BF16)
        acc_ref[...] = jnp.zeros_like(acc_ref)
        l_ref[...] = jnp.zeros_like(l_ref)

        @pl.when(cp == 0)
        def _():
            for b in range(n_seq):
                m8, l8, accs = own_keys(q_all[b], k_own.at[b], v_own.at[b])
                m_own[b] = m8
                l_own[b] = l8
                for h in range(2):
                    acc_own[b, h * 128:(h + 1) * 128, :] = accs[h]

        @pl.when(cp != 0)
        def _():
            m_own[...] = jnp.full_like(m_own, MASKED)
            l_own[...] = jnp.zeros_like(l_own)
            acc_own[...] = jnp.zeros_like(acc_own)

    b_new, i = it // per_seq, it % per_seq
    b_old = b_new - 1
    rows = pl.ds(pl.multiple_of(i * CHUNK, CHUNK), CHUNK)

    def score_dot():
        both = split_heads(k_ref[...], par_ref)
        return lax.dot_general(both, q_all[b_new], NT, preferred_element_type=F32)

    def score_post(s, par):
        keep = lax.broadcasted_iota(jnp.int32, (CHUNK, 128), 0) < limit_of(b_new) - i * CHUNK
        s = jnp.concatenate([jnp.where(keep, s[:, 0:128], MASKED), jnp.where(keep, s[:, 128:256], MASKED)], axis=1)
        s_refs[par][rows, :] = s
        top = pair_reduce(jnp.maximum, jnp.max(s.reshape(CHUNK // 8, 8, 256), axis=0)) * LOG2_SCALE
        m_ref[par] = jnp.maximum(jnp.where(i == 0, m_own[b_new], m_ref[par]), top)

    def expo(par):
        s = s_refs[par][rows, :]
        p = jnp.exp2(s.reshape(CHUNK // 8, 8, 256) * LOG2_SCALE - m_ref[par][None])
        l_ref[par] = jnp.where(i == 0, 0.0, l_ref[par]) + jnp.sum(p, axis=0)
        return p.reshape(CHUNK, 256).astype(BF16)

    def value(p):
        both = split_heads(v_ref[...], par_ref)
        part = lax.dot_general(both, p, TN, preferred_element_type=F32)
        acc_ref[...] = jnp.where(i == 0, 0.0, acc_ref[...]) + part

    total = n_seq * per_seq
    scoring, adding = it < total, jnp.logical_and(it >= per_seq, it < total + per_seq)
    for par in range(2):
        @pl.when(b_new % 2 == par)
        def _(par=par):
            main = jnp.logical_and(scoring, adding)

            @pl.when(main)
            def _():
                s = score_dot()
                p = expo(1 - par)
                value(p)
                score_post(s, par)

            @pl.when(jnp.logical_and(scoring, jnp.logical_not(adding)))
            def _():
                score_post(score_dot(), par)

            @pl.when(jnp.logical_and(adding, jnp.logical_not(scoring)))
            def _():
                value(expo(1 - par))

    @pl.when(jnp.logical_and(adding, i == per_seq - 1))
    def _():
        b = b_old
        m8 = m_ref[b % 2]
        w = jnp.exp2(m_own[b] - m8)
        l8 = pair_reduce(jnp.add, l_ref[b % 2]) + w * l_own[b]
        sub = lax.broadcasted_iota(jnp.int32, (8, 256), 0)
        stats = jnp.where(sub < 2, m8, l8)
        accs = [acc_ref[h * 128:(h + 1) * 128, :] + w[h:h + 1] * acc_own[b, h * 128:(h + 1) * 128, :] for h in range(2)]
        emit(b, accs, stats)


def fetch(it, total, per_seq, k_hbm, v_hbm, k_buf, v_buf, k_sem, v_sem):
    def copy(hbm, buf, sem, lag, step):
        j = step - lag
        src = hbm.at[j // per_seq, pl.ds(pl.multiple_of((j % per_seq) * CHUNK, CHUNK), CHUNK), :]
        return pltpu.make_async_copy(src, buf.at[step % SLOTS], sem.at[step % SLOTS])

    for hbm, buf, sem, lag in ((k_hbm, k_buf, k_sem, 0), (v_hbm, v_buf, v_sem, per_seq)):
        if lag == 0:
            @pl.when(it == 0)
            def _():
                for step in range(SLOTS - 1):
                    copy(hbm, buf, sem, lag, step).start()
        ahead = it + SLOTS - 1

        @pl.when(jnp.logical_and(ahead >= lag, ahead < total + lag))
        def _():
            copy(hbm, buf, sem, lag, ahead).start()

        @pl.when(jnp.logical_and(it >= lag, it < total + lag))
        def _():
            copy(hbm, buf, sem, lag, it).wait()


def merge(parts):
    sub = lax.broadcasted_iota(jnp.int32, (8, 128), 0)
    stats = [p[256:264, :] for p in parts]
    maxes = [jnp.where(sub % 4 < 2, s, pltpu.roll(s, 2, 0)) for s in stats]
    top = functools.reduce(jnp.maximum, maxes)
    weights = [jnp.exp2(m - top) for m in maxes]
    total = sum(w * s for w, s in zip(weights, stats))
    stats_out = jnp.where(sub < 2, top, total)
    accs = [sum(w[h:h + 1] * p[h * 128:(h + 1) * 128, :] for w, p in zip(weights, parts)) for h in range(2)]
    return accs, stats_out


STAGES = 7
LAGS = (3, 7, 12, 16, 20, 24, 28)


def fused_kernel(prefix_ref, q_ref, k_hbm, v_hbm, k_own, v_own, x_hbm, wo_hbm, out_ref,
                 par_ref, k_buf, v_buf, k_sem, v_sem, s_a, s_b, m_ref, l_ref, acc_ref, m_own, l_own, acc_own,
                 part_ref, x_buf, wo, ra1, sa2, ra2, proj, rs_o, rs_i, fwd, og,
                 loc_sem, a1_s, a1_r, a2_s, a2_r, rs_s, rso_r, rsi_r, og_s, og_r):
    it = pl.program_id(0)
    steps = pl.num_programs(0)
    per_seq = steps // (q_ref.shape[0] + 1)
    n_seq = q_ref.shape[0]
    units = n_seq // 2
    half_cols = proj.shape[-1]
    cp, z = lax.axis_index("cp"), lax.axis_index("tp")
    y, c = cp // 2, cp % 2
    is_mid = jnp.logical_and(z >= 1, z <= 2)
    is_end = jnp.logical_not(is_mid)
    near, far = z // 2, 1 - z // 2
    outer = jnp.where(z == 1, 0, 3)
    inner = jnp.where(z == 1, 2, 1)
    mid = jnp.where(z == 0, 1, 2)
    core_peer = {"cp": y * 2 + 1 - c}
    y_peer = {"cp": (1 - y) * 2 + c}
    me, yq = y * 2 + c, (1 - y) * 2 + c

    def remote(src, dst, send_sem, recv_sem, peer):
        return pltpu.make_async_remote_copy(src_ref=src, dst_ref=dst, send_sem=send_sem, recv_sem=recv_sem,
                                            device_id=peer, device_id_type=MESH)

    wo_copy = pltpu.make_async_copy(wo_hbm, wo, loc_sem.at[0])
    x_copies = [pltpu.make_async_copy(x_hbm.at[2 * u + y, pl.ds(32 * c, 32), :], x_buf.at[u], loc_sem.at[1 + u])
                for u in range(units)]

    @pl.when(it == 0)
    def _():
        barrier = pltpu.get_barrier_semaphore()
        pl.semaphore_signal(barrier, inc=1, device_id=core_peer, device_id_type=MESH)
        pl.semaphore_signal(barrier, inc=1, device_id=y_peer, device_id_type=MESH)

        @pl.when(is_mid)
        def _():
            pl.semaphore_signal(barrier, inc=1, device_id={"tp": outer}, device_id_type=MESH)
            pl.semaphore_signal(barrier, inc=1, device_id={"tp": inner}, device_id_type=MESH)
            pl.semaphore_wait(barrier, 4)

        @pl.when(is_end)
        def _():
            pl.semaphore_signal(barrier, inc=1, device_id={"tp": mid}, device_id_type=MESH)
            pl.semaphore_wait(barrier, 3)

    fetch(it, n_seq * per_seq, per_seq, k_hbm, v_hbm, k_buf, v_buf, k_sem, v_sem)

    @pl.when(it == 1)
    def _():
        wo_copy.start()
        for x_copy in x_copies:
            x_copy.start()

    @pl.when(it == 2 * per_seq)
    def _():
        wo_copy.wait()
        for x_copy in x_copies:
            x_copy.wait()

    def a1(b):
        return remote(part_ref.at[b, 1 - c], ra1.at[b], a1_s.at[b], a1_r.at[b], core_peer)

    def a2(u):
        return remote(sa2.at[u], ra2.at[u], a2_s.at[u], a2_r.at[u], y_peer)

    def rs_out(u, half):
        return remote(proj.at[u, half], rs_o.at[u, half], rs_s.at[u, half], rso_r.at[u, half], {"tp": mid})

    def rs_in(u):
        return remote(fwd.at[u], rs_i.at[u], rs_s.at[u, 0], rsi_r.at[u], {"tp": inner})

    def gather(q, u, half, lane, peer):
        return remote(og.at[q, u, half], og.at[q, u, half], og_s.at[lane, u, half], og_r.at[q, u, half], peer)

    def emit(b, accs, stats):
        for core in range(2):
            for h in range(2):
                part_ref[b, core, h * 128:(h + 1) * 128, :] = accs[h][:, core * 128:(core + 1) * 128]
            part_ref[b, core, 256:264, :] = stats[:, core * 128:(core + 1) * 128]
        a1(b).start()

    attend_step(it, n_seq, per_seq, lambda b: 2 * prefix_ref[b] - cp * (per_seq * CHUNK), q_ref, k_buf.at[it % SLOTS],
                v_buf.at[it % SLOTS], k_own, v_own, par_ref, emit,
                s_a, s_b, m_ref, l_ref, acc_ref, m_own, l_own, acc_own)

    def s1(u):
        b = 2 * u + 1 - y
        a1(b).wait_recv()
        accs, stats = merge([part_ref[b, c], ra1[b]])
        for h in range(2):
            sa2[u, h * 128:(h + 1) * 128, :] = accs[h]
        sa2[u, 256:264, :] = stats
        a2(u).start()

    def s2(u):
        b = 2 * u + y
        a1(b).wait_recv()
        a2(u).wait_recv()
        accs, stats = merge([part_ref[b, c], ra1[b], ra2[u]])
        heads = []
        for h in range(2):
            o = (accs[h] / stats[2 + h:3 + h]).T.astype(BF16)
            heads += [o[g * 32:(g + 1) * 32] for g in range(4)]
        o = jnp.concatenate(heads, axis=1)
        for half in range(2):
            proj[u, half] = jnp.dot(o, wo[:, half * half_cols:(half + 1) * half_cols], preferred_element_type=F32)

        @pl.when(is_end)
        def _():
            rs_out(u, far).start()
            rs_out(u, near).start()

    def s3(u):
        @pl.when(is_mid)
        def _():
            rs_out(u, far).wait_recv()
            fwd[u] = proj[u, far] + rs_o[u, far]
            rs_in(u).start()

    def x_half(u):
        lo = x_buf[u, :, 0:half_cols].astype(F32)
        hi = x_buf[u, :, half_cols:2 * half_cols].astype(F32)
        return jnp.where(near == 0, lo, hi)

    def s4(u):
        @pl.when(is_mid)
        def _():
            rs_out(u, near).wait_recv()
            rs_in(u).wait_recv()
            total = (proj[u, near] + rs_o[u, near]) + rs_i[u]
            og[me, u, near] = (x_half(u) + total).astype(BF16).astype(F32)
            gather(me, u, near, 2, {"tp": inner}).start()
            gather(me, u, near, 3, {"tp": outer}).start()

        @pl.when(is_end)
        def _():
            gather(me, u, near, 2, {"tp": mid}).wait_recv()

        gather(me, u, near, 1, y_peer).start()
        gather(me, u, near, 0, core_peer).start()

    def s5(u):
        gather(me, u, far, 2, {"tp": inner}).wait_recv()

        @pl.when(is_mid)
        def _():
            gather(me, u, far, 3, {"tp": outer}).start()

        gather(me, u, far, 1, y_peer).start()
        gather(me, u, far, 0, core_peer).start()

    def s6(u):
        for half in (near, far):
            gather(yq, u, half, 1, y_peer).wait_recv()
            gather(yq, u, half, 4, core_peer).start()

    def s7(u):
        for q in (y * 2 + 1 - c, (1 - y) * 2 + 1 - c):
            for half in range(2):
                gather(q, u, half, 0, core_peer).wait_recv()
        for q in range(4):
            for half in range(2):
                out_ref[2 * u + q // 2, 32 * (q % 2):32 * (q % 2) + 32, half * half_cols:(half + 1) * half_cols] = (
                    og[q, u, half].astype(BF16))

    stages = (s1, s2, s3, s4, s5, s6, s7)

    def slot(t, carry):
        for stage, lag in zip(stages, LAGS):
            since = t - (3 * per_seq - 1) - lag
            @pl.when(jnp.logical_and(since >= 0, jnp.logical_and(since < 2 * per_seq * units, since % (2 * per_seq) == 0)))
            def _(stage=stage, since=since):
                stage(since // (2 * per_seq))
        return carry

    last = (2 * units + 1) * per_seq - 1 + LAGS[-1]
    lax.fori_loop(it, jnp.where(it == steps - 1, last + 1, it + 1), slot, 0)

    @pl.when(it == steps - 1)
    def _():
        for b in range(n_seq):
            a1(b).wait_send()
        for u in range(units):
            a2(u).wait_send()
            for half in (near, far):
                gather(me, u, half, 0, core_peer).wait_send()
                gather(me, u, half, 1, y_peer).wait_send()
                gather(yq, u, half, 4, core_peer).wait_send()

        @pl.when(is_end)
        def _():
            for u in range(units):
                for half in (near, far):
                    rs_out(u, half).wait_send()

        @pl.when(is_mid)
        def _():
            for u in range(units):
                rs_in(u).wait_send()
                gather(me, u, near, 2, {"tp": inner}).wait_send()
                for half in (near, far):
                    gather(me, u, half, 3, {"tp": outer}).wait_send()


def attend_and_combine(prefix_len, q, k_cache, v_cache, k_own, v_own, hidden, w_o):
    n_seq, n_new, d_model = hidden.shape
    slots = k_cache.shape[1]
    k_rows = k_cache.reshape(n_seq, slots * 2, HEAD_DIM)
    v_rows = v_cache.reshape(n_seq, slots * 2, HEAD_DIM)
    per_seq = slots * 2 // CHUNK
    units, half = n_seq // 2, d_model // 2
    vmem = pl.BlockSpec(memory_space=pltpu.VMEM)
    hbm = pl.BlockSpec(memory_space=pl.ANY)
    dma = pltpu.SemaphoreType.DMA
    return pl.pallas_call(
        fused_kernel,
        grid=((n_seq + 1) * per_seq,),
        out_shape=jax.ShapeDtypeStruct((n_seq, n_new, d_model), BF16),
        in_specs=[pl.BlockSpec(memory_space=pltpu.SMEM), vmem, hbm, hbm, vmem, vmem, hbm, hbm],
        out_specs=vmem,
        scratch_shapes=[
            pltpu.VMEM((2, CHUNK, HEAD_DIM), BF16), pltpu.VMEM((SLOTS, CHUNK, HEAD_DIM), BF16),
            pltpu.VMEM((SLOTS, CHUNK, HEAD_DIM), BF16), dma((SLOTS,)), dma((SLOTS,)),
            pltpu.VMEM((slots * 2, 256), F32), pltpu.VMEM((slots * 2, 256), F32),
            pltpu.VMEM((2, 8, 256), F32), pltpu.VMEM((2, 8, 256), F32), pltpu.VMEM((256, 256), F32),
            pltpu.VMEM((n_seq, 8, 256), F32), pltpu.VMEM((n_seq, 8, 256), F32), pltpu.VMEM((n_seq, 256, 256), F32),
            pltpu.VMEM((n_seq, 2, 264, 128), F32),
            pltpu.VMEM((units, 32, d_model), BF16), pltpu.VMEM(w_o.shape, BF16),
            pltpu.VMEM((n_seq, 264, 128), F32), pltpu.VMEM((units, 264, 128), F32),
            pltpu.VMEM((units, 264, 128), F32), pltpu.VMEM((units, 2, 32, half), F32),
            pltpu.VMEM((units, 2, 32, half), F32), pltpu.VMEM((units, 32, half), F32),
            pltpu.VMEM((units, 32, half), F32), pltpu.VMEM((4, units, 2, 32, half), F32),
            dma((1 + units,)), dma((n_seq,)), dma((n_seq,)), dma((units,)), dma((units,)), dma((units, 2)),
            dma((units, 2)), dma((units,)), dma((5, units, 2)), dma((4, units, 2))],
        compiler_params=pltpu.CompilerParams(collective_id=0, has_side_effects=True, vmem_limit_bytes=56 << 20),
        cost_estimate=pl.CostEstimate(flops=19 << 30, bytes_accessed=46 << 20, transcendentals=17 << 20),
        name="attend_and_combine",
    )(prefix_len, q, k_rows, v_rows, k_own, v_own, hidden, w_o)


def solution(mesh):
    def per_device(hidden, prefix_len, k_cache, v_cache, attn_norm, w_q, w_k, w_v, w_o, q_norm, k_norm):
        q, k_own, v_own = project(hidden, prefix_len, attn_norm, w_q, w_k, w_v, q_norm, k_norm)
        block_out = attend_and_combine(prefix_len, q, k_cache, v_cache, k_own, v_own, hidden, w_o)
        return block_out, k_own.transpose(0, 2, 1, 3), v_own.transpose(0, 2, 1, 3)

    cache_spec = P('dp', 'cp', 'tp', None)
    arg_specs = (P('dp', None, None), P('dp'), cache_spec, cache_spec, P(None), P(None, 'tp'), P(None, 'tp'), P(None, 'tp'), P('tp', None), P(None), P(None))
    out_specs = (P('dp', None, None), P('dp', None, 'tp', None), P('dp', None, 'tp', None))
    return jax.shard_map(per_device, mesh=mesh, in_specs=arg_specs, out_specs=out_specs, check_vma=False)
```

```python
import functools

import jax
import jax.numpy as jnp
import numpy as np
from jax import lax
from jax.experimental import pallas as pl
from jax.experimental.pallas import tpu as pltpu
from jax.sharding import PartitionSpec as P

HEAD_DIM = 128
MASKED = -1e30
EPS = 1e-6
LOG2_SCALE = float(HEAD_DIM ** -0.5 / np.log(2.0))
MESH = pl.DeviceIdType.MESH
NT = (((1,), (1,)), ((), ()))
TN = (((0,), (0,)), ((), ()))
F32 = jnp.float32
BF16 = jnp.bfloat16
VMEM_LIMIT = 67043328


def cos_or_sin(x, want_cos):
    quarter = jnp.floor(x * F32(2.0 / np.pi) + F32(0.5))
    r = ((x - quarter * F32(1.5703125)) - quarter * F32(4.8351287841796875e-4)) - quarter * F32(3.13855707645416259765625e-7)
    r = r - quarter * F32(6.077100628276710381e-11)
    n = quarter.astype(jnp.int32) + want_cos.astype(jnp.int32)
    r2 = r * r
    sin_r = r + r * r2 * (F32(-1.6666654611e-1) + r2 * (F32(8.3321608736e-3) + r2 * F32(-1.9515295891e-4)))
    cos_r = 1.0 - 0.5 * r2 + r2 * r2 * (F32(4.166664568298827e-2) + r2 * (F32(-1.388731625493765e-3) + r2 * F32(2.443315711809948e-5)))
    y = jnp.where(n % 2 == 0, sin_r, cos_r)
    return jnp.where(n % 4 >= 2, -y, y)


def project_kernel(prefix_ref, x_ref, an_ref, wq_hbm, wk_hbm, wv_hbm, qn_ref, kn_ref, freq_ref,
                   q_ref, k_ref, v_ref, kn_out, vn_out, wq, wk, wv, normed, cos_ref, sin_ref, sems):
    n_seq, n_new = k_ref.shape[0], k_ref.shape[2]
    rows = n_seq * n_new
    copies = [pltpu.make_async_copy(wq_hbm.at[:, pl.ds(256 * j, 256)], wq.at[j], sems.at[j]) for j in range(4)]
    copies.append(pltpu.make_async_copy(wk_hbm, wk, sems.at[4]))
    copies.append(pltpu.make_async_copy(wv_hbm, wv, sems.at[5]))
    for c in copies:
        c.start()
    for r in range(0, rows, 64):
        x = x_ref[r:r + 64, :].astype(F32)
        scale = lax.rsqrt(jnp.mean(x * x, axis=-1, keepdims=True) + EPS)
        normed[r:r + 64, :] = (x * scale * an_ref[...].astype(F32)).astype(BF16)
    low = lax.broadcasted_iota(jnp.int32, (n_new, HEAD_DIM), 1) < HEAD_DIM // 2
    step = lax.broadcasted_iota(jnp.int32, (n_new, HEAD_DIM), 0)
    for b in range(n_seq):
        angle = (prefix_ref[b] + step).astype(F32) * freq_ref[...]
        trig = cos_or_sin(angle, low)
        turned = pltpu.roll(trig, HEAD_DIM // 2, 1)
        cos_ref[b * n_new:(b + 1) * n_new, :] = jnp.where(low, trig, turned)
        sin_ref[b * n_new:(b + 1) * n_new, :] = jnp.where(low, -turned, trig)

    def norm_rope(y, gain_ref):
        y = y.astype(BF16).astype(F32)
        y = y * lax.rsqrt(jnp.mean(y * y, axis=-1, keepdims=True) + EPS) * gain_ref[...].astype(F32)
        return (y * cos_ref[...] + pltpu.roll(y, HEAD_DIM // 2, 1) * sin_ref[...]).astype(BF16)

    for j in range(4):
        copies[j].wait()
        y = jnp.dot(normed[...], wq[j], preferred_element_type=F32)
        for i in range(2):
            h, g = j // 2, 2 * (j % 2) + i
            head = norm_rope(y[:, i * HEAD_DIM:(i + 1) * HEAD_DIM], qn_ref)
            for b in range(n_seq):
                for c in range(2):
                    q_ref[b, c * 128 + g * 32:c * 128 + g * 32 + 32, h * 128:(h + 1) * 128] = (
                        head[b * 64 + c * 32:b * 64 + c * 32 + 32])
    dst = lax.broadcasted_iota(jnp.int32, (2 * n_new, 2 * n_new), 0)
    src = lax.broadcasted_iota(jnp.int32, (2 * n_new, 2 * n_new), 1)
    perm = (src == (dst % 2) * n_new + dst // 2).astype(F32).astype(BF16)

    def put(heads, own_ref, new_ref):
        for b in range(n_seq):
            both = jnp.concatenate([head[b * n_new:(b + 1) * n_new] for head in heads], axis=0)
            for h in range(2):
                own_ref[b, h] = both[h * n_new:(h + 1) * n_new]
            new_ref[b] = jnp.dot(perm, both, preferred_element_type=F32).astype(BF16)

    copies[4].wait()
    y = jnp.dot(normed[...], wk[...], preferred_element_type=F32)
    put([norm_rope(y[:, h * HEAD_DIM:(h + 1) * HEAD_DIM], kn_ref) for h in range(2)], k_ref, kn_out)
    copies[5].wait()
    y = jnp.dot(normed[...], wv[...], preferred_element_type=F32).astype(BF16)
    put([y[:, h * HEAD_DIM:(h + 1) * HEAD_DIM] for h in range(2)], v_ref, vn_out)


def project(hidden, prefix_len, attn_norm, w_q, w_k, w_v, q_norm, k_norm):
    n_seq, n_new, d_model = hidden.shape
    freq = 1.0 / (1000000.0 ** (np.arange(HEAD_DIM // 2, dtype=np.float64) * 2.0 / HEAD_DIM))
    freq = jnp.asarray(np.concatenate([freq, freq])[None].astype(np.float32))
    vmem = pl.BlockSpec(memory_space=pltpu.VMEM)
    hbm = pl.BlockSpec(memory_space=pl.ANY)
    rows = n_seq * n_new
    return pl.pallas_call(
        project_kernel,
        out_shape=(jax.ShapeDtypeStruct((n_seq, 256, 256), BF16),
                   jax.ShapeDtypeStruct((n_seq, 2, n_new, HEAD_DIM), BF16),
                   jax.ShapeDtypeStruct((n_seq, 2, n_new, HEAD_DIM), BF16),
                   jax.ShapeDtypeStruct((n_seq, 2 * n_new, HEAD_DIM), BF16),
                   jax.ShapeDtypeStruct((n_seq, 2 * n_new, HEAD_DIM), BF16)),
        in_specs=[pl.BlockSpec(memory_space=pltpu.SMEM), vmem, vmem, hbm, hbm, hbm, vmem, vmem, vmem],
        out_specs=(vmem,) * 5,
        scratch_shapes=[pltpu.VMEM((4, d_model, 256), BF16), pltpu.VMEM((d_model, 256), BF16),
                        pltpu.VMEM((d_model, 256), BF16), pltpu.VMEM((rows, d_model), BF16),
                        pltpu.VMEM((rows, HEAD_DIM), F32), pltpu.VMEM((rows, HEAD_DIM), F32),
                        pltpu.SemaphoreType.DMA((6,))],
        compiler_params=pltpu.CompilerParams(vmem_limit_bytes=VMEM_LIMIT),
        cost_estimate=pl.CostEstimate(flops=2 * rows * d_model * 1536, bytes_accessed=12 << 20, transcendentals=0),
        name="project",
    )(prefix_len, hidden.reshape(rows, d_model), attn_norm[None], w_q, w_k, w_v, q_norm[None], k_norm[None], freq)


CHUNK = 2048
SLOTS = 4


def pair_reduce(op, x):
    x = op(x, pltpu.roll(x, 2, 0))
    return op(x, pltpu.roll(x, 4, 0))


def split_heads(x, par_ref):
    return jnp.concatenate([x * par_ref[h] for h in range(2)], axis=1)


def own_keys(q, k_own_ref, v_own_ref):
    n_new = k_own_ref.shape[-2]
    key = lax.broadcasted_iota(jnp.int32, (n_new, 256), 0)
    col = lax.broadcasted_iota(jnp.int32, (n_new, 256), 1)
    keep = key <= (col // 128) * 32 + col % 32
    maxes, sums, accs = [], [], []
    for h in range(2):
        s = lax.dot_general(k_own_ref[h], q[:, h * 128:(h + 1) * 128], NT, preferred_element_type=F32)
        s = jnp.where(keep, s * LOG2_SCALE, MASKED)
        m = jnp.max(s, axis=0, keepdims=True)
        p = jnp.exp2(s - m)
        maxes.append(m)
        sums.append(jnp.sum(p, axis=0, keepdims=True))
        accs.append(lax.dot_general(v_own_ref[h], p.astype(BF16), TN, preferred_element_type=F32))
    even = lax.broadcasted_iota(jnp.int32, (8, 256), 0) % 2 == 0
    return (jnp.where(even, maxes[0], maxes[1]), jnp.where(even, sums[0], sums[1]), accs)


def attend_step(it, n_seq, per_seq, limit_of, q_all, k_ref, v_ref, k_own, v_own, par_ref, emit,
                s_a, s_b, m_ref, l_ref, acc_ref, m_own, l_own, acc_own):
    cp = lax.axis_index("cp")
    s_refs = (s_a, s_b)

    @pl.when(it == 0)
    def _():
        even = (lax.broadcasted_iota(jnp.int32, (CHUNK, HEAD_DIM), 0) % 2 == 0).astype(F32)
        par_ref[0] = even.astype(BF16)
        par_ref[1] = (1.0 - even).astype(BF16)
        acc_ref[...] = jnp.zeros_like(acc_ref)
        l_ref[...] = jnp.zeros_like(l_ref)

        @pl.when(cp == 0)
        def _():
            for b in range(n_seq):
                m8, l8, accs = own_keys(q_all[b], k_own.at[b], v_own.at[b])
                m_own[b] = m8
                l_own[b] = l8
                for h in range(2):
                    acc_own[b, h * 128:(h + 1) * 128, :] = accs[h]

        @pl.when(cp != 0)
        def _():
            m_own[...] = jnp.full_like(m_own, MASKED)
            l_own[...] = jnp.zeros_like(l_own)
            acc_own[...] = jnp.zeros_like(acc_own)

    b_new, i = it // per_seq, it % per_seq
    b_old = b_new - 1
    rows = pl.ds(pl.multiple_of(i * CHUNK, CHUNK), CHUNK)

    def score_dot():
        both = split_heads(k_ref[...], par_ref)
        return lax.dot_general(both, q_all[b_new], NT, preferred_element_type=F32)

    def score_post(s, par):
        left = limit_of(b_new) - i * CHUNK - lax.broadcasted_iota(jnp.int32, (8, 128), 0)
        keep = (lax.broadcasted_iota(jnp.int32, (CHUNK // 8, 8, 128), 0) * 8 < left[None]).reshape(CHUNK, 128)
        s = jnp.concatenate([jnp.where(keep, s[:, 0:128], MASKED), jnp.where(keep, s[:, 128:256], MASKED)], axis=1)
        s_refs[par][rows, :] = s
        top = pair_reduce(jnp.maximum, jnp.max(s.reshape(CHUNK // 8, 8, 256), axis=0)) * LOG2_SCALE
        m_ref[par] = jnp.maximum(jnp.where(i == 0, m_own[b_new], m_ref[par]), top)

    def expo(par):
        s = s_refs[par][rows, :]
        p = jnp.exp2(s.reshape(CHUNK // 8, 8, 256) * LOG2_SCALE - m_ref[par][None])
        l_ref[par] = jnp.where(i == 0, 0.0, l_ref[par]) + jnp.sum(p, axis=0)
        return p.reshape(CHUNK, 256).astype(BF16)

    def value(p):
        both = split_heads(v_ref[...], par_ref)
        part = lax.dot_general(both, p, TN, preferred_element_type=F32)
        acc_ref[...] = jnp.where(i == 0, 0.0, acc_ref[...]) + part

    total = n_seq * per_seq
    scoring, adding = it < total, jnp.logical_and(it >= per_seq, it < total + per_seq)
    for par in range(2):
        @pl.when(b_new % 2 == par)
        def _(par=par):
            main = jnp.logical_and(scoring, adding)

            @pl.when(main)
            def _():
                s = score_dot()
                p = expo(1 - par)
                value(p)
                score_post(s, par)

            @pl.when(jnp.logical_and(scoring, jnp.logical_not(adding)))
            def _():
                score_post(score_dot(), par)

            @pl.when(jnp.logical_and(adding, jnp.logical_not(scoring)))
            def _():
                value(expo(1 - par))

    @pl.when(jnp.logical_and(adding, i == per_seq - 1))
    def _():
        b = b_old
        m8 = m_ref[b % 2]
        w = jnp.exp2(m_own[b] - m8)
        l8 = pair_reduce(jnp.add, l_ref[b % 2]) + w * l_own[b]
        sub = lax.broadcasted_iota(jnp.int32, (8, 256), 0)
        stats = jnp.where(sub < 2, m8, l8)
        accs = [acc_ref[h * 128:(h + 1) * 128, :] + w[h:h + 1] * acc_own[b, h * 128:(h + 1) * 128, :] for h in range(2)]
        emit(b, accs, stats)


def fetch(it, total, per_seq, k_hbm, v_hbm, k_buf, v_buf, k_sem, v_sem):
    def copy(hbm, buf, sem, lag, step):
        j = step - lag
        src = hbm.at[j // per_seq, pl.ds(pl.multiple_of((j % per_seq) * CHUNK, CHUNK), CHUNK), :]
        return pltpu.make_async_copy(src, buf.at[step % SLOTS], sem.at[step % SLOTS])

    for hbm, buf, sem, lag in ((k_hbm, k_buf, k_sem, 0), (v_hbm, v_buf, v_sem, per_seq)):
        if lag == 0:
            @pl.when(it == 0)
            def _():
                for step in range(SLOTS - 1):
                    copy(hbm, buf, sem, lag, step).start()
        ahead = it + SLOTS - 1

        @pl.when(jnp.logical_and(ahead >= lag, ahead < total + lag))
        def _():
            copy(hbm, buf, sem, lag, ahead).start()

        @pl.when(jnp.logical_and(it >= lag, it < total + lag))
        def _():
            copy(hbm, buf, sem, lag, it).wait()


def merge(parts):
    sub = lax.broadcasted_iota(jnp.int32, (8, 128), 0)
    stats = [p[256:264, :] for p in parts]
    maxes = [jnp.where(sub % 4 < 2, s, pltpu.roll(s, 2, 0)) for s in stats]
    top = functools.reduce(jnp.maximum, maxes)
    weights = [jnp.exp2(m - top) for m in maxes]
    total = sum(w * s for w, s in zip(weights, stats))
    stats_out = jnp.where(sub < 2, top, total)
    accs = [sum(w[h:h + 1] * p[h * 128:(h + 1) * 128, :] for w, p in zip(weights, parts)) for h in range(2)]
    return accs, stats_out


STAGES = 7
PIECES = 5
LAGS = (3, 7, 11, 15, 18, 22, 24)


def fused_kernel(prefix_ref, q_ref, k_hbm, v_hbm, k_own, v_own, x_hbm, wo_hbm, out_ref,
                 par_ref, k_buf, v_buf, k_sem, v_sem, s_a, s_b, m_ref, l_ref, acc_ref, m_own, l_own, acc_own,
                 part_ref, x_buf, wo, ra1, sa2, ra2, proj, rs_o, rs_i, fwd, og,
                 loc_sem, a1_s, a1_r, a2_s, a2_r, rs_s, rso_r, rsi_r, og_s, og_r):
    it = pl.program_id(0)
    steps = pl.num_programs(0)
    per_seq = steps // (q_ref.shape[0] + 1)
    n_seq = q_ref.shape[0]
    units = n_seq // 2
    pieces, width = proj.shape[2], proj.shape[-1]
    cp, z = lax.axis_index("cp"), lax.axis_index("tp")
    y, c = cp // 2, cp % 2
    is_mid = jnp.logical_and(z >= 1, z <= 2)
    is_end = jnp.logical_not(is_mid)
    near, far = z // 2, 1 - z // 2
    outer = jnp.where(z == 1, 0, 3)
    inner = jnp.where(z == 1, 2, 1)
    mid = jnp.where(z == 0, 1, 2)
    core_peer = {"cp": y * 2 + 1 - c}
    y_peer = {"cp": (1 - y) * 2 + c}
    me, yq = y * 2 + c, (1 - y) * 2 + c

    def remote(src, dst, send_sem, recv_sem, peer):
        return pltpu.make_async_remote_copy(src_ref=src, dst_ref=dst, send_sem=send_sem, recv_sem=recv_sem,
                                            device_id=peer, device_id_type=MESH)

    wo_copy = pltpu.make_async_copy(wo_hbm, wo, loc_sem.at[0])
    x_copies = [pltpu.make_async_copy(x_hbm.at[2 * u + y, pl.ds(32 * c, 32), :], x_buf.at[u], loc_sem.at[1 + u])
                for u in range(units)]

    @pl.when(it == 0)
    def _():
        barrier = pltpu.get_barrier_semaphore()
        pl.semaphore_signal(barrier, inc=1, device_id=core_peer, device_id_type=MESH)
        pl.semaphore_signal(barrier, inc=1, device_id=y_peer, device_id_type=MESH)

        @pl.when(is_mid)
        def _():
            pl.semaphore_signal(barrier, inc=1, device_id={"tp": outer}, device_id_type=MESH)
            pl.semaphore_signal(barrier, inc=1, device_id={"tp": inner}, device_id_type=MESH)
            pl.semaphore_wait(barrier, 4)

        @pl.when(is_end)
        def _():
            pl.semaphore_signal(barrier, inc=1, device_id={"tp": mid}, device_id_type=MESH)
            pl.semaphore_wait(barrier, 3)

    fetch(it, n_seq * per_seq, per_seq, k_hbm, v_hbm, k_buf, v_buf, k_sem, v_sem)

    @pl.when(it == 1)
    def _():
        wo_copy.start()
        for x_copy in x_copies:
            x_copy.start()

    @pl.when(it == 2 * per_seq)
    def _():
        wo_copy.wait()
        for x_copy in x_copies:
            x_copy.wait()

    def a1(b):
        return remote(part_ref.at[b, 1 - c], ra1.at[b], a1_s.at[b], a1_r.at[b], core_peer)

    def a2(u):
        return remote(sa2.at[u], ra2.at[u], a2_s.at[u], a2_r.at[u], y_peer)

    def rs_out(u, half, p):
        return remote(proj.at[u, half, p], rs_o.at[u, half, p], rs_s.at[u, half, p], rso_r.at[u, half, p], {"tp": mid})

    def rs_in(u, p):
        return remote(fwd.at[u, p], rs_i.at[u, p], rs_s.at[u, 0, p], rsi_r.at[u, p], {"tp": inner})

    def gather(q, u, half, p, lane, peer):
        return remote(og.at[q, u, half, p], og.at[q, u, half, p], og_s.at[lane, u, half, p], og_r.at[q, u, half, p], peer)

    def emit(b, accs, stats):
        for core in range(2):
            for h in range(2):
                part_ref[b, core, h * 128:(h + 1) * 128, :] = accs[h][:, core * 128:(core + 1) * 128]
            part_ref[b, core, 256:264, :] = stats[:, core * 128:(core + 1) * 128]
        a1(b).start()

    attend_step(it, n_seq, per_seq, lambda b: 2 * prefix_ref[b] - cp * (per_seq * CHUNK), q_ref, k_buf.at[it % SLOTS],
                v_buf.at[it % SLOTS], k_own, v_own, par_ref, emit,
                s_a, s_b, m_ref, l_ref, acc_ref, m_own, l_own, acc_own)

    def s1(u):
        b = 2 * u + 1 - y
        a1(b).wait_recv()
        accs, stats = merge([part_ref[b, c], ra1[b]])
        for h in range(2):
            sa2[u, h * 128:(h + 1) * 128, :] = accs[h]
        sa2[u, 256:264, :] = stats
        a2(u).start()

    def s2(u):
        b = 2 * u + y
        a1(b).wait_recv()
        a2(u).wait_recv()
        accs, stats = merge([part_ref[b, c], ra1[b], ra2[u]])
        heads = []
        for h in range(2):
            o = (accs[h] / stats[2 + h:3 + h]).T.astype(BF16)
            heads += [o[g * 32:(g + 1) * 32] for g in range(4)]
        o = jnp.concatenate(heads, axis=1)
        for half in (far, near):
            for p in range(pieces):
                cols = pl.ds(pl.multiple_of((half * pieces + p) * width, width), width)
                proj[u, half, p] = jnp.dot(o, wo[:, cols], preferred_element_type=F32)

                @pl.when(is_end)
                def _(half=half, p=p):
                    rs_out(u, half, p).start()

    def s3(u):
        @pl.when(is_mid)
        def _():
            for p in range(pieces):
                rs_out(u, far, p).wait_recv()
                fwd[u, p] = proj[u, far, p] + rs_o[u, far, p]
                rs_in(u, p).start()

    def s4(u):
        for p in range(pieces):
            @pl.when(is_mid)
            def _(p=p):
                rs_out(u, near, p).wait_recv()
                rs_in(u, p).wait_recv()
                total = (proj[u, near, p] + rs_o[u, near, p]) + rs_i[u, p]
                x = x_buf[u, :, pl.ds(pl.multiple_of((near * pieces + p) * width, width), width)].astype(F32)
                og[me, u, near, p] = (x + total).astype(BF16).astype(F32)
                gather(me, u, near, p, 2, {"tp": inner}).start()
                gather(me, u, near, p, 3, {"tp": outer}).start()

            @pl.when(is_end)
            def _(p=p):
                gather(me, u, near, p, 2, {"tp": mid}).wait_recv()

            gather(me, u, near, p, 1, y_peer).start()
            gather(me, u, near, p, 0, core_peer).start()

    def s5(u):
        for p in range(pieces):
            gather(me, u, far, p, 2, {"tp": inner}).wait_recv()

            @pl.when(is_mid)
            def _(p=p):
                gather(me, u, far, p, 3, {"tp": outer}).start()

            gather(me, u, far, p, 1, y_peer).start()
            gather(me, u, far, p, 0, core_peer).start()

    def s6(u):
        for half in (near, far):
            for p in range(pieces):
                gather(yq, u, half, p, 1, y_peer).wait_recv()
                gather(yq, u, half, p, 4, core_peer).start()

    def put(q, u, half, p):
        cols = pl.ds(pl.multiple_of((half * pieces + p) * width, width), width)
        out_ref[2 * u + q // 2, pl.ds(pl.multiple_of(32 * (q % 2), 32), 32), cols] = og[q, u, half, p].astype(BF16)

    def s7(u):
        for half in (near, far):
            for p in range(pieces):
                put(me, u, half, p)
                put(yq, u, half, p)
        for q in (y * 2 + 1 - c, (1 - y) * 2 + 1 - c):
            for half in (near, far):
                for p in range(pieces):
                    gather(q, u, half, p, 0, core_peer).wait_recv()
                    put(q, u, half, p)

    stages = (s1, s2, s3, s4, s5, s6, s7)

    def slot(t, carry):
        for stage, lag in zip(stages, LAGS):
            since = t - (3 * per_seq - 1) - lag
            @pl.when(jnp.logical_and(since >= 0, jnp.logical_and(since < 2 * per_seq * units, since % (2 * per_seq) == 0)))
            def _(stage=stage, since=since):
                stage(since // (2 * per_seq))
        return carry

    last = (2 * units + 1) * per_seq - 1 + LAGS[-1]
    lax.fori_loop(it, jnp.where(it == steps - 1, last + 1, it + 1), slot, 0)

    @pl.when(it == steps - 1)
    def _():
        for b in range(n_seq):
            a1(b).wait_send()
        for u in range(units):
            a2(u).wait_send()
            for half in (near, far):
                for p in range(pieces):
                    gather(me, u, half, p, 0, core_peer).wait_send()
                    gather(me, u, half, p, 1, y_peer).wait_send()
                    gather(yq, u, half, p, 4, core_peer).wait_send()

        @pl.when(is_end)
        def _():
            for u in range(units):
                for half in (near, far):
                    for p in range(pieces):
                        rs_out(u, half, p).wait_send()

        @pl.when(is_mid)
        def _():
            for u in range(units):
                for p in range(pieces):
                    rs_in(u, p).wait_send()
                    gather(me, u, near, p, 2, {"tp": inner}).wait_send()
                    for half in (near, far):
                        gather(me, u, half, p, 3, {"tp": outer}).wait_send()


def attend_and_combine(prefix_len, q, k_cache, v_cache, k_own, v_own, hidden, w_o):
    n_seq, n_new, d_model = hidden.shape
    slots = k_cache.shape[1]
    k_rows = k_cache.reshape(n_seq, slots * 2, HEAD_DIM)
    v_rows = v_cache.reshape(n_seq, slots * 2, HEAD_DIM)
    per_seq = slots * 2 // CHUNK
    units, width = n_seq // 2, d_model // (2 * PIECES)
    vmem = pl.BlockSpec(memory_space=pltpu.VMEM)
    hbm = pl.BlockSpec(memory_space=pl.ANY)
    dma = pltpu.SemaphoreType.DMA
    return pl.pallas_call(
        fused_kernel,
        grid=((n_seq + 1) * per_seq,),
        out_shape=jax.ShapeDtypeStruct((n_seq, n_new, d_model), BF16),
        in_specs=[pl.BlockSpec(memory_space=pltpu.SMEM), vmem, hbm, hbm, vmem, vmem, hbm, hbm],
        out_specs=vmem,
        scratch_shapes=[
            pltpu.VMEM((2, CHUNK, HEAD_DIM), BF16), pltpu.VMEM((SLOTS, CHUNK, HEAD_DIM), BF16),
            pltpu.VMEM((SLOTS, CHUNK, HEAD_DIM), BF16), dma((SLOTS,)), dma((SLOTS,)),
            pltpu.VMEM((slots * 2, 256), F32), pltpu.VMEM((slots * 2, 256), F32),
            pltpu.VMEM((2, 8, 256), F32), pltpu.VMEM((2, 8, 256), F32), pltpu.VMEM((256, 256), F32),
            pltpu.VMEM((n_seq, 8, 256), F32), pltpu.VMEM((n_seq, 8, 256), F32), pltpu.VMEM((n_seq, 256, 256), F32),
            pltpu.VMEM((n_seq, 2, 264, 128), F32),
            pltpu.VMEM((units, 32, d_model), BF16), pltpu.VMEM(w_o.shape, BF16),
            pltpu.VMEM((n_seq, 264, 128), F32), pltpu.VMEM((units, 264, 128), F32),
            pltpu.VMEM((units, 264, 128), F32), pltpu.VMEM((units, 2, PIECES, 32, width), F32),
            pltpu.VMEM((units, 2, PIECES, 32, width), F32), pltpu.VMEM((units, PIECES, 32, width), F32),
            pltpu.VMEM((units, PIECES, 32, width), F32), pltpu.VMEM((4, units, 2, PIECES, 32, width), F32),
            dma((1 + units,)), dma((n_seq,)), dma((n_seq,)), dma((units,)), dma((units,)), dma((units, 2, PIECES)),
            dma((units, 2, PIECES)), dma((units, PIECES)), dma((5, units, 2, PIECES)), dma((4, units, 2, PIECES))],
        compiler_params=pltpu.CompilerParams(collective_id=0, has_side_effects=True, vmem_limit_bytes=56 << 20),
        cost_estimate=pl.CostEstimate(flops=19 << 30, bytes_accessed=46 << 20, transcendentals=17 << 20),
        name="attend_and_combine",
    )(prefix_len, q, k_rows, v_rows, k_own, v_own, hidden, w_o)


def solution(mesh):
    def per_device(hidden, prefix_len, k_cache, v_cache, attn_norm, w_q, w_k, w_v, w_o, q_norm, k_norm):
        q, k_own, v_own, k_new, v_new = project(hidden, prefix_len, attn_norm, w_q, w_k, w_v, q_norm, k_norm)
        block_out = attend_and_combine(prefix_len, q, k_cache, v_cache, k_own, v_own, hidden, w_o)
        shape = (hidden.shape[0], hidden.shape[1], 2, HEAD_DIM)
        return block_out, k_new.reshape(shape), v_new.reshape(shape)

    cache_spec = P('dp', 'cp', 'tp', None)
    arg_specs = (P('dp', None, None), P('dp'), cache_spec, cache_spec, P(None), P(None, 'tp'), P(None, 'tp'), P(None, 'tp'), P('tp', None), P(None), P(None))
    out_specs = (P('dp', None, None), P('dp', None, 'tp', None), P('dp', None, 'tp', None))
    return jax.shard_map(per_device, mesh=mesh, in_specs=arg_specs, out_specs=out_specs, check_vma=False)
```

```python
import functools

import jax
import jax.numpy as jnp
import numpy as np
from jax import lax
from jax.experimental import pallas as pl
from jax.experimental.pallas import tpu as pltpu
from jax.sharding import PartitionSpec as P

HEAD_DIM = 128
MASKED = -1e30
EPS = 1e-6
LOG2_SCALE = float(HEAD_DIM ** -0.5 / np.log(2.0))
MESH = pl.DeviceIdType.MESH
NT = (((1,), (1,)), ((), ()))
TN = (((0,), (0,)), ((), ()))
F32 = jnp.float32
BF16 = jnp.bfloat16
VMEM_LIMIT = 67043328


def cos_or_sin(x, want_cos):
    quarter = jnp.floor(x * F32(2.0 / np.pi) + F32(0.5))
    r = ((x - quarter * F32(1.5703125)) - quarter * F32(4.8351287841796875e-4)) - quarter * F32(3.13855707645416259765625e-7)
    r = r - quarter * F32(6.077100628276710381e-11)
    n = quarter.astype(jnp.int32) + want_cos.astype(jnp.int32)
    r2 = r * r
    sin_r = r + r * r2 * (F32(-1.6666654611e-1) + r2 * (F32(8.3321608736e-3) + r2 * F32(-1.9515295891e-4)))
    cos_r = 1.0 - 0.5 * r2 + r2 * r2 * (F32(4.166664568298827e-2) + r2 * (F32(-1.388731625493765e-3) + r2 * F32(2.443315711809948e-5)))
    y = jnp.where(n % 2 == 0, sin_r, cos_r)
    return jnp.where(n % 4 >= 2, -y, y)


def project_kernel(prefix_ref, x_ref, an_ref, wq_hbm, wk_hbm, wv_hbm, qn_ref, kn_ref, freq_ref,
                   q_ref, k_ref, v_ref, kn_out, vn_out, wq, wk, wv, normed, cos_ref, sin_ref, sems):
    n_seq, n_new = k_ref.shape[0], k_ref.shape[2]
    rows = n_seq * n_new
    depth = wq.shape[0] // 4
    copies = [pltpu.make_async_copy(wq_hbm.at[pl.ds(depth * j, depth)], wq.at[pl.ds(depth * j, depth)], sems.at[j])
              for j in range(4)]
    copies.append(pltpu.make_async_copy(wk_hbm, wk, sems.at[4]))
    copies.append(pltpu.make_async_copy(wv_hbm, wv, sems.at[5]))
    for c in copies:
        c.start()
    for r in range(0, rows, 64):
        x = x_ref[r:r + 64, :].astype(F32)
        scale = lax.rsqrt(jnp.mean(x * x, axis=-1, keepdims=True) + EPS)
        for j in range(x.shape[1] // 128):
            cols = slice(128 * j, 128 * j + 128)
            normed[r:r + 64, cols] = (x[:, cols] * scale * an_ref[j:j + 1, :].astype(F32)).astype(BF16)
    low = lax.broadcasted_iota(jnp.int32, (n_new, HEAD_DIM), 1) < HEAD_DIM // 2
    step = lax.broadcasted_iota(jnp.int32, (n_new, HEAD_DIM), 0)
    for b in range(n_seq):
        angle = (prefix_ref[b] + step).astype(F32) * freq_ref[...]
        trig = cos_or_sin(angle, low)
        turned = pltpu.roll(trig, HEAD_DIM // 2, 1)
        cos_ref[b * n_new:(b + 1) * n_new, :] = jnp.where(low, trig, turned)
        sin_ref[b * n_new:(b + 1) * n_new, :] = jnp.where(low, -turned, trig)

    def norm_rope(y, gain_ref):
        y = y.astype(BF16).astype(F32)
        y = y * lax.rsqrt(jnp.mean(y * y, axis=-1, keepdims=True) + EPS) * gain_ref[...].astype(F32)
        return (y * cos_ref[...] + pltpu.roll(y, HEAD_DIM // 2, 1) * sin_ref[...]).astype(BF16)

    for j in range(4):
        copies[j].wait()
    for j in range(4):
        y = jnp.dot(normed[...], wq[:, 256 * j:256 * j + 256], preferred_element_type=F32)
        for i in range(2):
            h, g = j // 2, 2 * (j % 2) + i
            head = norm_rope(y[:, i * HEAD_DIM:(i + 1) * HEAD_DIM], qn_ref)
            for b in range(n_seq):
                for c in range(2):
                    q_ref[b, c * 128 + g * 32:c * 128 + g * 32 + 32, h * 128:(h + 1) * 128] = (
                        head[b * 64 + c * 32:b * 64 + c * 32 + 32])
    dst = lax.broadcasted_iota(jnp.int32, (2 * n_new, 2 * n_new), 0)
    src = lax.broadcasted_iota(jnp.int32, (2 * n_new, 2 * n_new), 1)
    perm = (src == (dst % 2) * n_new + dst // 2).astype(F32).astype(BF16)

    def put(heads, own_ref, new_ref):
        for b in range(n_seq):
            both = jnp.concatenate([head[b * n_new:(b + 1) * n_new] for head in heads], axis=0)
            for h in range(2):
                own_ref[b, h] = both[h * n_new:(h + 1) * n_new]
            new_ref[b] = jnp.dot(perm, both, preferred_element_type=F32).astype(BF16)

    copies[4].wait()
    y = jnp.dot(normed[...], wk[...], preferred_element_type=F32)
    put([norm_rope(y[:, h * HEAD_DIM:(h + 1) * HEAD_DIM], kn_ref) for h in range(2)], k_ref, kn_out)
    copies[5].wait()
    y = jnp.dot(normed[...], wv[...], preferred_element_type=F32).astype(BF16)
    put([y[:, h * HEAD_DIM:(h + 1) * HEAD_DIM] for h in range(2)], v_ref, vn_out)


def project(hidden, prefix_len, attn_norm, w_q, w_k, w_v, q_norm, k_norm):
    n_seq, n_new, d_model = hidden.shape
    freq = 1.0 / (1000000.0 ** (np.arange(HEAD_DIM // 2, dtype=np.float64) * 2.0 / HEAD_DIM))
    freq = jnp.asarray(np.concatenate([freq, freq])[None].astype(np.float32))
    vmem = pl.BlockSpec(memory_space=pltpu.VMEM)
    hbm = pl.BlockSpec(memory_space=pl.ANY)
    rows = n_seq * n_new
    return pl.pallas_call(
        project_kernel,
        out_shape=(jax.ShapeDtypeStruct((n_seq, 256, 256), BF16),
                   jax.ShapeDtypeStruct((n_seq, 2, n_new, HEAD_DIM), BF16),
                   jax.ShapeDtypeStruct((n_seq, 2, n_new, HEAD_DIM), BF16),
                   jax.ShapeDtypeStruct((n_seq, 2 * n_new, HEAD_DIM), BF16),
                   jax.ShapeDtypeStruct((n_seq, 2 * n_new, HEAD_DIM), BF16)),
        in_specs=[pl.BlockSpec(memory_space=pltpu.SMEM), vmem, vmem, hbm, hbm, hbm, vmem, vmem, vmem],
        out_specs=(vmem,) * 5,
        scratch_shapes=[pltpu.VMEM(w_q.shape, BF16), pltpu.VMEM((d_model, 256), BF16),
                        pltpu.VMEM((d_model, 256), BF16), pltpu.VMEM((rows, d_model), BF16),
                        pltpu.VMEM((rows, HEAD_DIM), F32), pltpu.VMEM((rows, HEAD_DIM), F32),
                        pltpu.SemaphoreType.DMA((6,))],
        compiler_params=pltpu.CompilerParams(vmem_limit_bytes=VMEM_LIMIT),
        cost_estimate=pl.CostEstimate(flops=2 * rows * d_model * 1536, bytes_accessed=12 << 20, transcendentals=0),
        name="project",
    )(prefix_len, hidden.reshape(rows, d_model), attn_norm.reshape(d_model // 128, 128), w_q, w_k, w_v, q_norm[None], k_norm[None], freq)


CHUNK = 4096
SLOTS = 3


def pair_reduce(op, x):
    x = op(x, pltpu.roll(x, 2, 0))
    return op(x, pltpu.roll(x, 4, 0))


def split_heads(x):
    even = (lax.broadcasted_iota(jnp.int32, (16, HEAD_DIM), 0) % 2 == 0).astype(F32)
    gains = [even.astype(BF16), (1.0 - even).astype(BF16)]
    return jnp.concatenate([x * jnp.concatenate([g] * (x.shape[0] // 16), axis=0) for g in gains], axis=1)


def own_keys(q, k_own_ref, v_own_ref):
    n_new = k_own_ref.shape[-2]
    key = lax.broadcasted_iota(jnp.int32, (n_new, 256), 0)
    col = lax.broadcasted_iota(jnp.int32, (n_new, 256), 1)
    keep = key <= (col // 128) * 32 + col % 32
    maxes, sums, accs = [], [], []
    for h in range(2):
        s = lax.dot_general(k_own_ref[h], q[:, h * 128:(h + 1) * 128], NT, preferred_element_type=F32)
        s = jnp.where(keep, s * LOG2_SCALE, MASKED)
        m = jnp.max(s, axis=0, keepdims=True)
        p = jnp.exp2(s - m)
        maxes.append(m)
        sums.append(jnp.sum(p, axis=0, keepdims=True))
        accs.append(lax.dot_general(v_own_ref[h], p.astype(BF16), TN, preferred_element_type=F32))
    even = lax.broadcasted_iota(jnp.int32, (8, 256), 0) % 2 == 0
    return (jnp.where(even, maxes[0], maxes[1]), jnp.where(even, sums[0], sums[1]), accs)


def attend_step(it, n_seq, per_seq, limit_of, q_all, k_ref, v_ref, k_own, v_own, emit,
                s_a, s_b, m_ref, l_ref, acc_ref, m_own, l_own, acc_own):
    cp = lax.axis_index("cp")
    s_refs = (s_a, s_b)

    @pl.when(it == 0)
    def _():
        acc_ref[...] = jnp.zeros_like(acc_ref)
        l_ref[...] = jnp.zeros_like(l_ref)

        @pl.when(cp == 0)
        def _():
            for b in range(n_seq):
                m8, l8, accs = own_keys(q_all[b], k_own.at[b], v_own.at[b])
                m_own[b] = m8
                l_own[b] = l8
                for h in range(2):
                    acc_own[b, h * 128:(h + 1) * 128, :] = accs[h]

        @pl.when(cp != 0)
        def _():
            m_own[...] = jnp.full_like(m_own, MASKED)
            l_own[...] = jnp.zeros_like(l_own)
            acc_own[...] = jnp.zeros_like(acc_own)

    b_new, i = it // per_seq, it % per_seq
    b_old = b_new - 1
    rows = pl.ds(pl.multiple_of(i * CHUNK, CHUNK), CHUNK)

    def score_dot():
        both = split_heads(k_ref[...])
        return lax.dot_general(both, q_all[b_new], NT, preferred_element_type=F32)

    def score_post(s, par):
        left = limit_of(b_new) - i * CHUNK - lax.broadcasted_iota(jnp.int32, (8, 128), 0)
        keep = (lax.broadcasted_iota(jnp.int32, (CHUNK // 8, 8, 128), 0) * 8 < left[None]).reshape(CHUNK, 128)
        s = jnp.concatenate([jnp.where(keep, s[:, 0:128], MASKED), jnp.where(keep, s[:, 128:256], MASKED)], axis=1)
        s_refs[par][rows, :] = s
        top = pair_reduce(jnp.maximum, jnp.max(s.reshape(CHUNK // 8, 8, 256), axis=0)) * LOG2_SCALE
        m_ref[par] = jnp.maximum(jnp.where(i == 0, m_own[b_new], m_ref[par]), top)

    def expo(par):
        s = s_refs[par][rows, :]
        p = jnp.exp2(s.reshape(CHUNK // 8, 8, 256) * LOG2_SCALE - m_ref[par][None])
        l_ref[par] = jnp.where(i == 0, 0.0, l_ref[par]) + jnp.sum(p, axis=0)
        return p.reshape(CHUNK, 256).astype(BF16)

    def value(p):
        both = split_heads(v_ref[...])
        part = lax.dot_general(both, p, TN, preferred_element_type=F32)
        acc_ref[...] = jnp.where(i == 0, 0.0, acc_ref[...]) + part

    total = n_seq * per_seq
    scoring, adding = it < total, jnp.logical_and(it >= per_seq, it < total + per_seq)
    for par in range(2):
        @pl.when(b_new % 2 == par)
        def _(par=par):
            main = jnp.logical_and(scoring, adding)

            @pl.when(main)
            def _():
                s = score_dot()
                p = expo(1 - par)
                value(p)
                score_post(s, par)

            @pl.when(jnp.logical_and(scoring, jnp.logical_not(adding)))
            def _():
                score_post(score_dot(), par)

            @pl.when(jnp.logical_and(adding, jnp.logical_not(scoring)))
            def _():
                value(expo(1 - par))

    @pl.when(jnp.logical_and(adding, i == per_seq - 1))
    def _():
        b = b_old
        m8 = m_ref[b % 2]
        w = jnp.exp2(m_own[b] - m8)
        l8 = pair_reduce(jnp.add, l_ref[b % 2]) + w * l_own[b]
        sub = lax.broadcasted_iota(jnp.int32, (8, 256), 0)
        stats = jnp.where(sub < 2, m8, l8)
        accs = [acc_ref[h * 128:(h + 1) * 128, :] + w[h:h + 1] * acc_own[b, h * 128:(h + 1) * 128, :] for h in range(2)]
        emit(b, accs, stats)


def fetch(it, total, per_seq, k_hbm, v_hbm, k_buf, v_buf, k_sem, v_sem):
    def copy(hbm, buf, sem, lag, step):
        j = step - lag
        src = hbm.at[j // per_seq, pl.ds(pl.multiple_of((j % per_seq) * CHUNK, CHUNK), CHUNK), :]
        return pltpu.make_async_copy(src, buf.at[step % SLOTS], sem.at[step % SLOTS])

    for hbm, buf, sem, lag in ((k_hbm, k_buf, k_sem, 0), (v_hbm, v_buf, v_sem, per_seq)):
        if lag == 0:
            @pl.when(it == 0)
            def _():
                for step in range(SLOTS - 1):
                    copy(hbm, buf, sem, lag, step).start()
        ahead = it + SLOTS - 1

        @pl.when(jnp.logical_and(ahead >= lag, ahead < total + lag))
        def _():
            copy(hbm, buf, sem, lag, ahead).start()

        @pl.when(jnp.logical_and(it >= lag, it < total + lag))
        def _():
            copy(hbm, buf, sem, lag, it).wait()


def merge(parts):
    sub = lax.broadcasted_iota(jnp.int32, (8, 128), 0)
    stats = [p[256:264, :] for p in parts]
    maxes = [jnp.where(sub % 4 < 2, s, pltpu.roll(s, 2, 0)) for s in stats]
    top = functools.reduce(jnp.maximum, maxes)
    weights = [jnp.exp2(m - top) for m in maxes]
    total = sum(w * s for w, s in zip(weights, stats))
    stats_out = jnp.where(sub < 2, top, total)
    accs = [sum(w[h:h + 1] * p[h * 128:(h + 1) * 128, :] for w, p in zip(weights, parts)) for h in range(2)]
    return accs, stats_out


STAGES = 7
PIECES = 2
LAGS = (2, 4, 6, 8, 9, 11, 12)


def fused_kernel(prefix_ref, q_ref, k_hbm, v_hbm, k_own, v_own, x_hbm, wo_hbm, out_ref,
                 k_buf, v_buf, k_sem, v_sem, s_a, s_b, m_ref, l_ref, acc_ref, m_own, l_own, acc_own,
                 part_ref, x_buf, wo, ra1, sa2, ra2, proj, rs_o, rs_i, fwd, og,
                 loc_sem, a1_s, a1_r, a2_s, a2_r, rs_s, rso_r, rsi_r, og_s, og_r):
    it = pl.program_id(0)
    steps = pl.num_programs(0)
    per_seq = steps // (q_ref.shape[0] + 1)
    n_seq = q_ref.shape[0]
    units = n_seq // 2
    pieces, width = proj.shape[2], proj.shape[-1]
    cp, z = lax.axis_index("cp"), lax.axis_index("tp")
    y, c = cp // 2, cp % 2
    is_mid = jnp.logical_and(z >= 1, z <= 2)
    is_end = jnp.logical_not(is_mid)
    near, far = z // 2, 1 - z // 2
    outer = jnp.where(z == 1, 0, 3)
    inner = jnp.where(z == 1, 2, 1)
    mid = jnp.where(z == 0, 1, 2)
    core_peer = {"cp": y * 2 + 1 - c}
    y_peer = {"cp": (1 - y) * 2 + c}
    me, yq = y * 2 + c, (1 - y) * 2 + c

    def remote(src, dst, send_sem, recv_sem, peer):
        return pltpu.make_async_remote_copy(src_ref=src, dst_ref=dst, send_sem=send_sem, recv_sem=recv_sem,
                                            device_id=peer, device_id_type=MESH)

    wo_copy = pltpu.make_async_copy(wo_hbm, wo, loc_sem.at[0])
    x_copies = [pltpu.make_async_copy(x_hbm.at[2 * u + y, pl.ds(32 * c, 32), :], x_buf.at[u], loc_sem.at[1 + u])
                for u in range(units)]

    @pl.when(it == 0)
    def _():
        barrier = pltpu.get_barrier_semaphore()
        pl.semaphore_signal(barrier, inc=1, device_id=core_peer, device_id_type=MESH)
        pl.semaphore_signal(barrier, inc=1, device_id=y_peer, device_id_type=MESH)

        @pl.when(is_mid)
        def _():
            pl.semaphore_signal(barrier, inc=1, device_id={"tp": outer}, device_id_type=MESH)
            pl.semaphore_signal(barrier, inc=1, device_id={"tp": inner}, device_id_type=MESH)
            pl.semaphore_wait(barrier, 4)

        @pl.when(is_end)
        def _():
            pl.semaphore_signal(barrier, inc=1, device_id={"tp": mid}, device_id_type=MESH)
            pl.semaphore_wait(barrier, 3)

    fetch(it, n_seq * per_seq, per_seq, k_hbm, v_hbm, k_buf, v_buf, k_sem, v_sem)

    @pl.when(it == 1)
    def _():
        wo_copy.start()
        for x_copy in x_copies:
            x_copy.start()

    @pl.when(it == 2 * per_seq)
    def _():
        wo_copy.wait()
        for x_copy in x_copies:
            x_copy.wait()

    def a1(b):
        return remote(part_ref.at[b, 1 - c], ra1.at[b], a1_s.at[b], a1_r.at[b], core_peer)

    def a2(u):
        return remote(sa2.at[u], ra2.at[u], a2_s.at[u], a2_r.at[u], y_peer)

    def rs_out(u, half, p):
        return remote(proj.at[u, half, p], rs_o.at[u, half, p], rs_s.at[u, half, p], rso_r.at[u, half, p], {"tp": mid})

    def rs_in(u, p):
        return remote(fwd.at[u, p], rs_i.at[u, p], rs_s.at[u, 0, p], rsi_r.at[u, p], {"tp": inner})

    def gather(q, u, half, p, lane, peer):
        return remote(og.at[q, u, half, p], og.at[q, u, half, p], og_s.at[lane, u, half, p], og_r.at[q, u, half, p], peer)

    def emit(b, accs, stats):
        for core in range(2):
            for h in range(2):
                part_ref[b, core, h * 128:(h + 1) * 128, :] = accs[h][:, core * 128:(core + 1) * 128]
            part_ref[b, core, 256:264, :] = stats[:, core * 128:(core + 1) * 128]
        a1(b).start()

    attend_step(it, n_seq, per_seq, lambda b: 2 * prefix_ref[b] - cp * (per_seq * CHUNK), q_ref, k_buf.at[it % SLOTS],
                v_buf.at[it % SLOTS], k_own, v_own, emit,
                s_a, s_b, m_ref, l_ref, acc_ref, m_own, l_own, acc_own)

    def s1(u):
        b = 2 * u + 1 - y
        a1(b).wait_recv()
        accs, stats = merge([part_ref[b, c], ra1[b]])
        for h in range(2):
            sa2[u, h * 128:(h + 1) * 128, :] = accs[h]
        sa2[u, 256:264, :] = stats
        a2(u).start()

    def s2(u):
        b = 2 * u + y
        a1(b).wait_recv()
        a2(u).wait_recv()
        accs, stats = merge([part_ref[b, c], ra1[b], ra2[u]])
        heads = []
        for h in range(2):
            o = (accs[h] / stats[2 + h:3 + h]).T.astype(BF16)
            heads += [o[g * 32:(g + 1) * 32] for g in range(4)]
        o = jnp.concatenate(heads, axis=1)
        for half in (far, near):
            for p in range(pieces):
                cols = pl.ds(pl.multiple_of((half * pieces + p) * width, width), width)
                proj[u, half, p] = jnp.dot(o, wo[:, cols], preferred_element_type=F32)

        @pl.when(is_end)
        def _():
            for half in (far, near):
                for p in range(pieces):
                    rs_out(u, half, p).start()

    def s3(u):
        @pl.when(is_mid)
        def _():
            for p in range(pieces):
                rs_out(u, far, p).wait_recv()
                fwd[u, p] = proj[u, far, p] + rs_o[u, far, p]
                rs_in(u, p).start()

    def s4(u):
        for p in range(pieces):
            @pl.when(is_mid)
            def _(p=p):
                rs_out(u, near, p).wait_recv()
                rs_in(u, p).wait_recv()
                total = (proj[u, near, p] + rs_o[u, near, p]) + rs_i[u, p]
                x = x_buf[u, :, pl.ds(pl.multiple_of((near * pieces + p) * width, width), width)].astype(F32)
                og[me, u, near, p] = (x + total).astype(BF16).astype(F32)
                gather(me, u, near, p, 2, {"tp": inner}).start()
                gather(me, u, near, p, 3, {"tp": outer}).start()

            @pl.when(is_end)
            def _(p=p):
                gather(me, u, near, p, 2, {"tp": mid}).wait_recv()

            gather(me, u, near, p, 1, y_peer).start()
            gather(me, u, near, p, 0, core_peer).start()

    def s5(u):
        for p in range(pieces):
            gather(me, u, far, p, 2, {"tp": inner}).wait_recv()

            @pl.when(is_mid)
            def _(p=p):
                gather(me, u, far, p, 3, {"tp": outer}).start()

            gather(me, u, far, p, 1, y_peer).start()
            gather(me, u, far, p, 0, core_peer).start()

    def s6(u):
        for half in (near, far):
            for p in range(pieces):
                gather(yq, u, half, p, 1, y_peer).wait_recv()
                gather(yq, u, half, p, 4, core_peer).start()

    def put(q, u, half, p):
        cols = pl.ds(pl.multiple_of((half * pieces + p) * width, width), width)
        out_ref[2 * u + q // 2, pl.ds(pl.multiple_of(32 * (q % 2), 32), 32), cols] = og[q, u, half, p].astype(BF16)

    def s7(u):
        for half in (near, far):
            for p in range(pieces):
                put(me, u, half, p)
                put(yq, u, half, p)
        for q in (y * 2 + 1 - c, (1 - y) * 2 + 1 - c):
            for half in (near, far):
                for p in range(pieces):
                    gather(q, u, half, p, 0, core_peer).wait_recv()
                    put(q, u, half, p)

    stages = (s1, s2, s3, s4, s5, s6, s7)

    def slot(t, carry):
        for stage, lag in zip(stages, LAGS):
            since = t - (3 * per_seq - 1) - lag
            @pl.when(jnp.logical_and(since >= 0, jnp.logical_and(since < 2 * per_seq * units, since % (2 * per_seq) == 0)))
            def _(stage=stage, since=since):
                stage(since // (2 * per_seq))
        return carry

    last = (2 * units + 1) * per_seq - 1 + LAGS[-1]
    lax.fori_loop(it, jnp.where(it == steps - 1, last + 1, it + 1), slot, 0)

    @pl.when(it == steps - 1)
    def _():
        for b in range(n_seq):
            a1(b).wait_send()
        for u in range(units):
            a2(u).wait_send()
            for half in (near, far):
                for p in range(pieces):
                    gather(me, u, half, p, 0, core_peer).wait_send()
                    gather(me, u, half, p, 1, y_peer).wait_send()
                    gather(yq, u, half, p, 4, core_peer).wait_send()

        @pl.when(is_end)
        def _():
            for u in range(units):
                for half in (near, far):
                    for p in range(pieces):
                        rs_out(u, half, p).wait_send()

        @pl.when(is_mid)
        def _():
            for u in range(units):
                for p in range(pieces):
                    rs_in(u, p).wait_send()
                    gather(me, u, near, p, 2, {"tp": inner}).wait_send()
                    for half in (near, far):
                        gather(me, u, half, p, 3, {"tp": outer}).wait_send()


def attend_and_combine(prefix_len, q, k_cache, v_cache, k_own, v_own, hidden, w_o):
    n_seq, n_new, d_model = hidden.shape
    slots = k_cache.shape[1]
    k_rows = k_cache.reshape(n_seq, slots * 2, HEAD_DIM)
    v_rows = v_cache.reshape(n_seq, slots * 2, HEAD_DIM)
    per_seq = slots * 2 // CHUNK
    units, width = n_seq // 2, d_model // (2 * PIECES)
    vmem = pl.BlockSpec(memory_space=pltpu.VMEM)
    hbm = pl.BlockSpec(memory_space=pl.ANY)
    dma = pltpu.SemaphoreType.DMA
    return pl.pallas_call(
        fused_kernel,
        grid=((n_seq + 1) * per_seq,),
        out_shape=jax.ShapeDtypeStruct((n_seq, n_new, d_model), BF16),
        in_specs=[pl.BlockSpec(memory_space=pltpu.SMEM), vmem, hbm, hbm, vmem, vmem, hbm, hbm],
        out_specs=vmem,
        scratch_shapes=[
            pltpu.VMEM((SLOTS, CHUNK, HEAD_DIM), BF16),
            pltpu.VMEM((SLOTS, CHUNK, HEAD_DIM), BF16), dma((SLOTS,)), dma((SLOTS,)),
            pltpu.VMEM((slots * 2, 256), F32), pltpu.VMEM((slots * 2, 256), F32),
            pltpu.VMEM((2, 8, 256), F32), pltpu.VMEM((2, 8, 256), F32), pltpu.VMEM((256, 256), F32),
            pltpu.VMEM((n_seq, 8, 256), F32), pltpu.VMEM((n_seq, 8, 256), F32), pltpu.VMEM((n_seq, 256, 256), F32),
            pltpu.VMEM((n_seq, 2, 264, 128), F32),
            pltpu.VMEM((units, 32, d_model), BF16), pltpu.VMEM(w_o.shape, BF16),
            pltpu.VMEM((n_seq, 264, 128), F32), pltpu.VMEM((units, 264, 128), F32),
            pltpu.VMEM((units, 264, 128), F32), pltpu.VMEM((units, 2, PIECES, 32, width), F32),
            pltpu.VMEM((units, 2, PIECES, 32, width), F32), pltpu.VMEM((units, PIECES, 32, width), F32),
            pltpu.VMEM((units, PIECES, 32, width), F32), pltpu.VMEM((4, units, 2, PIECES, 32, width), F32),
            dma((1 + units,)), dma((n_seq,)), dma((n_seq,)), dma((units,)), dma((units,)), dma((units, 2, PIECES)),
            dma((units, 2, PIECES)), dma((units, PIECES)), dma((5, units, 2, PIECES)), dma((4, units, 2, PIECES))],
        compiler_params=pltpu.CompilerParams(collective_id=0, has_side_effects=True, vmem_limit_bytes=VMEM_LIMIT),
        cost_estimate=pl.CostEstimate(flops=19 << 30, bytes_accessed=46 << 20, transcendentals=17 << 20),
        name="attend_and_combine",
    )(prefix_len, q, k_rows, v_rows, k_own, v_own, hidden, w_o)


def solution(mesh):
    def per_device(hidden, prefix_len, k_cache, v_cache, attn_norm, w_q, w_k, w_v, w_o, q_norm, k_norm):
        q, k_own, v_own, k_new, v_new = project(hidden, prefix_len, attn_norm, w_q, w_k, w_v, q_norm, k_norm)
        block_out = attend_and_combine(prefix_len, q, k_cache, v_cache, k_own, v_own, hidden, w_o)
        shape = (hidden.shape[0], hidden.shape[1], 2, HEAD_DIM)
        return block_out, k_new.reshape(shape), v_new.reshape(shape)

    cache_spec = P('dp', 'cp', 'tp', None)
    arg_specs = (P('dp', None, None), P('dp'), cache_spec, cache_spec, P(None), P(None, 'tp'), P(None, 'tp'), P(None, 'tp'), P('tp', None), P(None), P(None))
    out_specs = (P('dp', None, None), P('dp', None, 'tp', None), P('dp', None, 'tp', None))
    return jax.shard_map(per_device, mesh=mesh, in_specs=arg_specs, out_specs=out_specs, check_vma=False)
```

```python
import functools

import jax
import jax.numpy as jnp
import numpy as np
from jax import lax
from jax.experimental import pallas as pl
from jax.experimental.pallas import tpu as pltpu
from jax.sharding import PartitionSpec as P

HEAD_DIM = 128
MASKED = -1e30
EPS = 1e-6
LOG2_SCALE = float(HEAD_DIM ** -0.5 / np.log(2.0))
MESH = pl.DeviceIdType.MESH
NT = (((1,), (1,)), ((), ()))
TN = (((0,), (0,)), ((), ()))
F32 = jnp.float32
BF16 = jnp.bfloat16
VMEM_LIMIT = 67043328


def cos_or_sin(x, want_cos):
    quarter = jnp.floor(x * F32(2.0 / np.pi) + F32(0.5))
    r = ((x - quarter * F32(1.5703125)) - quarter * F32(4.8351287841796875e-4)) - quarter * F32(3.13855707645416259765625e-7)
    r = r - quarter * F32(6.077100628276710381e-11)
    n = quarter.astype(jnp.int32) + want_cos.astype(jnp.int32)
    r2 = r * r
    sin_r = r + r * r2 * (F32(-1.6666654611e-1) + r2 * (F32(8.3321608736e-3) + r2 * F32(-1.9515295891e-4)))
    cos_r = 1.0 - 0.5 * r2 + r2 * r2 * (F32(4.166664568298827e-2) + r2 * (F32(-1.388731625493765e-3) + r2 * F32(2.443315711809948e-5)))
    y = jnp.where(n % 2 == 0, sin_r, cos_r)
    return jnp.where(n % 4 >= 2, -y, y)


def project_kernel(prefix_ref, x_ref, an_ref, wq_hbm, wk_hbm, wv_hbm, qn_ref, kn_ref, freq_ref,
                   q_ref, k_ref, v_ref, kn_out, vn_out, wq, wk, wv, normed, cos_ref, sin_ref, sems):
    n_seq, n_new = k_ref.shape[0], k_ref.shape[2]
    rows = n_seq * n_new
    depth = wq.shape[0] // 4
    copies = [pltpu.make_async_copy(wq_hbm.at[pl.ds(depth * j, depth)], wq.at[pl.ds(depth * j, depth)], sems.at[j])
              for j in range(4)]
    copies.append(pltpu.make_async_copy(wk_hbm, wk, sems.at[4]))
    copies.append(pltpu.make_async_copy(wv_hbm, wv, sems.at[5]))
    for c in copies:
        c.start()
    for r in range(0, rows, 64):
        x = x_ref[r:r + 64, :].astype(F32)
        scale = lax.rsqrt(jnp.mean(x * x, axis=-1, keepdims=True) + EPS)
        for j in range(x.shape[1] // 128):
            cols = slice(128 * j, 128 * j + 128)
            normed[r:r + 64, cols] = (x[:, cols] * scale * an_ref[j:j + 1, :].astype(F32)).astype(BF16)
    low = lax.broadcasted_iota(jnp.int32, (n_new, HEAD_DIM), 1) < HEAD_DIM // 2
    step = lax.broadcasted_iota(jnp.int32, (n_new, HEAD_DIM), 0)
    for b in range(n_seq):
        angle = (prefix_ref[b] + step).astype(F32) * freq_ref[...]
        trig = cos_or_sin(angle, low)
        turned = pltpu.roll(trig, HEAD_DIM // 2, 1)
        cos_ref[b * n_new:(b + 1) * n_new, :] = jnp.where(low, trig, turned)
        sin_ref[b * n_new:(b + 1) * n_new, :] = jnp.where(low, -turned, trig)

    def norm_rope(y, gain_ref):
        y = y.astype(BF16).astype(F32)
        y = y * lax.rsqrt(jnp.mean(y * y, axis=-1, keepdims=True) + EPS) * gain_ref[...].astype(F32)
        return (y * cos_ref[...] + pltpu.roll(y, HEAD_DIM // 2, 1) * sin_ref[...]).astype(BF16)

    for j in range(4):
        copies[j].wait()
    for j in range(4):
        y = jnp.dot(normed[...], wq[:, 256 * j:256 * j + 256], preferred_element_type=F32)
        for i in range(2):
            h, g = j // 2, 2 * (j % 2) + i
            head = norm_rope(y[:, i * HEAD_DIM:(i + 1) * HEAD_DIM], qn_ref)
            for b in range(n_seq):
                for part in range(4):
                    q_ref[b, part * 64 + g * 16:part * 64 + g * 16 + 16, h * 128:(h + 1) * 128] = (
                        head[b * 64 + part * 16:b * 64 + part * 16 + 16])
    dst = lax.broadcasted_iota(jnp.int32, (2 * n_new, 2 * n_new), 0)
    src = lax.broadcasted_iota(jnp.int32, (2 * n_new, 2 * n_new), 1)
    perm = (src == (dst % 2) * n_new + dst // 2).astype(F32).astype(BF16)

    def put(heads, own_ref, new_ref):
        for b in range(n_seq):
            both = jnp.concatenate([head[b * n_new:(b + 1) * n_new] for head in heads], axis=0)
            for h in range(2):
                own_ref[b, h] = both[h * n_new:(h + 1) * n_new]
            new_ref[b] = jnp.dot(perm, both, preferred_element_type=F32).astype(BF16)

    copies[4].wait()
    y = jnp.dot(normed[...], wk[...], preferred_element_type=F32)
    put([norm_rope(y[:, h * HEAD_DIM:(h + 1) * HEAD_DIM], kn_ref) for h in range(2)], k_ref, kn_out)
    copies[5].wait()
    y = jnp.dot(normed[...], wv[...], preferred_element_type=F32).astype(BF16)
    put([y[:, h * HEAD_DIM:(h + 1) * HEAD_DIM] for h in range(2)], v_ref, vn_out)


def project(hidden, prefix_len, attn_norm, w_q, w_k, w_v, q_norm, k_norm):
    n_seq, n_new, d_model = hidden.shape
    freq = 1.0 / (1000000.0 ** (np.arange(HEAD_DIM // 2, dtype=np.float64) * 2.0 / HEAD_DIM))
    freq = jnp.asarray(np.concatenate([freq, freq])[None].astype(np.float32))
    vmem = pl.BlockSpec(memory_space=pltpu.VMEM)
    hbm = pl.BlockSpec(memory_space=pl.ANY)
    rows = n_seq * n_new
    return pl.pallas_call(
        project_kernel,
        out_shape=(jax.ShapeDtypeStruct((n_seq, 256, 256), BF16),
                   jax.ShapeDtypeStruct((n_seq, 2, n_new, HEAD_DIM), BF16),
                   jax.ShapeDtypeStruct((n_seq, 2, n_new, HEAD_DIM), BF16),
                   jax.ShapeDtypeStruct((n_seq, 2 * n_new, HEAD_DIM), BF16),
                   jax.ShapeDtypeStruct((n_seq, 2 * n_new, HEAD_DIM), BF16)),
        in_specs=[pl.BlockSpec(memory_space=pltpu.SMEM), vmem, vmem, hbm, hbm, hbm, vmem, vmem, vmem],
        out_specs=(vmem,) * 5,
        scratch_shapes=[pltpu.VMEM(w_q.shape, BF16), pltpu.VMEM((d_model, 256), BF16),
                        pltpu.VMEM((d_model, 256), BF16), pltpu.VMEM((rows, d_model), BF16),
                        pltpu.VMEM((rows, HEAD_DIM), F32), pltpu.VMEM((rows, HEAD_DIM), F32),
                        pltpu.SemaphoreType.DMA((6,))],
        compiler_params=pltpu.CompilerParams(vmem_limit_bytes=VMEM_LIMIT),
        cost_estimate=pl.CostEstimate(flops=2 * rows * d_model * 1536, bytes_accessed=12 << 20, transcendentals=0),
        name="project",
    )(prefix_len, hidden.reshape(rows, d_model), attn_norm.reshape(d_model // 128, 128), w_q, w_k, w_v, q_norm[None], k_norm[None], freq)


CHUNK = 4096
SLOTS = 3


def pair_reduce(op, x):
    x = op(x, pltpu.roll(x, 2, 0))
    return op(x, pltpu.roll(x, 4, 0))


def split_heads(x):
    even = (lax.broadcasted_iota(jnp.int32, (16, HEAD_DIM), 0) % 2 == 0).astype(F32)
    gains = [even.astype(BF16), (1.0 - even).astype(BF16)]
    return jnp.concatenate([x * jnp.concatenate([g] * (x.shape[0] // 16), axis=0) for g in gains], axis=1)


def own_keys(q, k_own_ref, v_own_ref):
    n_new = k_own_ref.shape[-2]
    key = lax.broadcasted_iota(jnp.int32, (n_new, 256), 0)
    col = lax.broadcasted_iota(jnp.int32, (n_new, 256), 1)
    keep = key <= (col // 64) * 16 + col % 16
    maxes, sums, accs = [], [], []
    for h in range(2):
        s = lax.dot_general(k_own_ref[h], q[:, h * 128:(h + 1) * 128], NT, preferred_element_type=F32)
        s = jnp.where(keep, s * LOG2_SCALE, MASKED)
        m = jnp.max(s, axis=0, keepdims=True)
        p = jnp.exp2(s - m)
        maxes.append(m)
        sums.append(jnp.sum(p, axis=0, keepdims=True))
        accs.append(lax.dot_general(v_own_ref[h], p.astype(BF16), TN, preferred_element_type=F32))
    even = lax.broadcasted_iota(jnp.int32, (8, 256), 0) % 2 == 0
    return (jnp.where(even, maxes[0], maxes[1]), jnp.where(even, sums[0], sums[1]), accs)


def attend_step(it, n_seq, per_seq, limit_of, q_all, k_ref, v_ref, k_own, v_own, emit,
                s_a, s_b, m_ref, l_ref, acc_ref, m_own, l_own, acc_own):
    cp = lax.axis_index("cp")
    s_refs = (s_a, s_b)

    @pl.when(it == 0)
    def _():
        acc_ref[...] = jnp.zeros_like(acc_ref)
        l_ref[...] = jnp.zeros_like(l_ref)

        @pl.when(cp == 0)
        def _():
            for b in range(n_seq):
                m8, l8, accs = own_keys(q_all[b], k_own.at[b], v_own.at[b])
                m_own[b] = m8
                l_own[b] = l8
                for h in range(2):
                    acc_own[b, h * 128:(h + 1) * 128, :] = accs[h]

        @pl.when(cp != 0)
        def _():
            m_own[...] = jnp.full_like(m_own, MASKED)
            l_own[...] = jnp.zeros_like(l_own)
            acc_own[...] = jnp.zeros_like(acc_own)

    b_new, i = it // per_seq, it % per_seq
    b_old = b_new - 1
    rows = pl.ds(pl.multiple_of(i * CHUNK, CHUNK), CHUNK)

    def score_dot():
        both = split_heads(k_ref[...])
        return lax.dot_general(both, q_all[b_new], NT, preferred_element_type=F32)

    def score_post(s, par):
        left = limit_of(b_new) - i * CHUNK - lax.broadcasted_iota(jnp.int32, (8, 128), 0)
        keep = (lax.broadcasted_iota(jnp.int32, (CHUNK // 8, 8, 128), 0) * 8 < left[None]).reshape(CHUNK, 128)
        s = jnp.concatenate([jnp.where(keep, s[:, 0:128], MASKED), jnp.where(keep, s[:, 128:256], MASKED)], axis=1)
        s_refs[par][rows, :] = s
        top = pair_reduce(jnp.maximum, jnp.max(s.reshape(CHUNK // 8, 8, 256), axis=0)) * LOG2_SCALE
        m_ref[par] = jnp.maximum(jnp.where(i == 0, m_own[b_new], m_ref[par]), top)

    def expo(par):
        s = s_refs[par][rows, :]
        p = jnp.exp2(s.reshape(CHUNK // 8, 8, 256) * LOG2_SCALE - m_ref[par][None])
        l_ref[par] = jnp.where(i == 0, 0.0, l_ref[par]) + jnp.sum(p, axis=0)
        return p.reshape(CHUNK, 256).astype(BF16)

    def value(p):
        both = split_heads(v_ref[...])
        part = lax.dot_general(both, p, TN, preferred_element_type=F32)
        acc_ref[...] = jnp.where(i == 0, 0.0, acc_ref[...]) + part

    total = n_seq * per_seq
    scoring, adding = it < total, jnp.logical_and(it >= per_seq, it < total + per_seq)
    for par in range(2):
        @pl.when(b_new % 2 == par)
        def _(par=par):
            main = jnp.logical_and(scoring, adding)

            @pl.when(main)
            def _():
                s = score_dot()
                p = expo(1 - par)
                value(p)
                score_post(s, par)

            @pl.when(jnp.logical_and(scoring, jnp.logical_not(adding)))
            def _():
                score_post(score_dot(), par)

            @pl.when(jnp.logical_and(adding, jnp.logical_not(scoring)))
            def _():
                value(expo(1 - par))

    @pl.when(jnp.logical_and(adding, i == per_seq - 1))
    def _():
        b = b_old
        m8 = m_ref[b % 2]
        w = jnp.exp2(m_own[b] - m8)
        l8 = pair_reduce(jnp.add, l_ref[b % 2]) + w * l_own[b]
        sub = lax.broadcasted_iota(jnp.int32, (8, 256), 0)
        stats = jnp.where(sub < 2, m8, l8)
        accs = [acc_ref[h * 128:(h + 1) * 128, :] + w[h:h + 1] * acc_own[b, h * 128:(h + 1) * 128, :] for h in range(2)]
        emit(b, accs, stats)


def fetch(it, total, per_seq, k_hbm, v_hbm, k_buf, v_buf, k_sem, v_sem):
    def copy(hbm, buf, sem, lag, step):
        j = step - lag
        src = hbm.at[j // per_seq, pl.ds(pl.multiple_of((j % per_seq) * CHUNK, CHUNK), CHUNK), :]
        return pltpu.make_async_copy(src, buf.at[step % SLOTS], sem.at[step % SLOTS])

    for hbm, buf, sem, lag in ((k_hbm, k_buf, k_sem, 0), (v_hbm, v_buf, v_sem, per_seq)):
        if lag == 0:
            @pl.when(it == 0)
            def _():
                for step in range(SLOTS - 1):
                    copy(hbm, buf, sem, lag, step).start()
        ahead = it + SLOTS - 1

        @pl.when(jnp.logical_and(ahead >= lag, ahead < total + lag))
        def _():
            copy(hbm, buf, sem, lag, ahead).start()

        @pl.when(jnp.logical_and(it >= lag, it < total + lag))
        def _():
            copy(hbm, buf, sem, lag, it).wait()


def merge(parts):
    sub = lax.broadcasted_iota(jnp.int32, (8, 128), 0)
    stats = [p[256:264, :] for p in parts]
    maxes = [jnp.where(sub % 4 < 2, s, pltpu.roll(s, 2, 0)) for s in stats]
    top = functools.reduce(jnp.maximum, maxes)
    weights = [jnp.exp2(m - top) for m in maxes]
    total = sum(w * s for w, s in zip(weights, stats))
    accs = [sum(w[h:h + 1] * p[h * 128:(h + 1) * 128, :] for w, p in zip(weights, parts)) for h in range(2)]
    return accs, [top[h:h + 1] for h in range(2)], [total[2 + h:3 + h] for h in range(2)]


def pack_half(pair, want):
    first, second = pair
    low = lax.broadcasted_iota(jnp.int32, first.shape, 1) < 64
    at_zero = jnp.where(low, first, pltpu.roll(second, 64, 1))
    at_one = jnp.where(low, pltpu.roll(first, 64, 1), second)
    return jnp.where(want == 0, at_zero, at_one)


PIECES = 2
LAGS = (1, 3, 5, 6, 7, 9, 10)


def fused_kernel(prefix_ref, q_ref, k_hbm, v_hbm, k_own, v_own, x_hbm, wo_hbm, out_ref,
                 k_buf, v_buf, k_sem, v_sem, s_a, s_b, m_ref, l_ref, acc_ref, m_own, l_own, acc_own,
                 part_ref, x_buf, wo, ra1, sa2, oa2, ra2, proj, rs_o, rs_i, fwd, og,
                 loc_sem, a1_s, a1_r, a2_s, a2_r, rs_s, rso_r, rsi_r, og_s, og_r):
    it = pl.program_id(0)
    steps = pl.num_programs(0)
    per_seq = steps // (q_ref.shape[0] + 1)
    n_seq = q_ref.shape[0]
    units = n_seq
    pieces, width = proj.shape[2], proj.shape[-1]
    cp, z = lax.axis_index("cp"), lax.axis_index("tp")
    y, c = cp // 2, cp % 2
    is_mid = jnp.logical_and(z >= 1, z <= 2)
    is_end = jnp.logical_not(is_mid)
    near, far = z // 2, 1 - z // 2
    outer = jnp.where(z == 1, 0, 3)
    inner = jnp.where(z == 1, 2, 1)
    mid = jnp.where(z == 0, 1, 2)
    core_peer = {"cp": y * 2 + 1 - c}
    y_peer = {"cp": (1 - y) * 2 + c}
    me, yq = y * 2 + c, (1 - y) * 2 + c

    def remote(src, dst, send_sem, recv_sem, peer):
        return pltpu.make_async_remote_copy(src_ref=src, dst_ref=dst, send_sem=send_sem, recv_sem=recv_sem,
                                            device_id=peer, device_id_type=MESH)

    wo_copy = pltpu.make_async_copy(wo_hbm, wo, loc_sem.at[0])
    x_copies = [pltpu.make_async_copy(x_hbm.at[u, pl.ds(pl.multiple_of(32 * c + 16 * y, 16), 16), :], x_buf.at[u], loc_sem.at[1 + u])
                for u in range(units)]

    @pl.when(it == 0)
    def _():
        barrier = pltpu.get_barrier_semaphore()
        pl.semaphore_signal(barrier, inc=1, device_id=core_peer, device_id_type=MESH)
        pl.semaphore_signal(barrier, inc=1, device_id=y_peer, device_id_type=MESH)

        @pl.when(is_mid)
        def _():
            pl.semaphore_signal(barrier, inc=1, device_id={"tp": outer}, device_id_type=MESH)
            pl.semaphore_signal(barrier, inc=1, device_id={"tp": inner}, device_id_type=MESH)
            pl.semaphore_wait(barrier, 4)

        @pl.when(is_end)
        def _():
            pl.semaphore_signal(barrier, inc=1, device_id={"tp": mid}, device_id_type=MESH)
            pl.semaphore_wait(barrier, 3)

    fetch(it, n_seq * per_seq, per_seq, k_hbm, v_hbm, k_buf, v_buf, k_sem, v_sem)

    @pl.when(it == 1)
    def _():
        wo_copy.start()
        for x_copy in x_copies:
            x_copy.start()

    @pl.when(it == 2 * per_seq)
    def _():
        wo_copy.wait()
        for x_copy in x_copies:
            x_copy.wait()

    def a1(b):
        return remote(part_ref.at[b, 1 - c], ra1.at[b], a1_s.at[b], a1_r.at[b], core_peer)

    def a2(u):
        return remote(sa2.at[u], ra2.at[u], a2_s.at[u], a2_r.at[u], y_peer)

    def rs_out(u, half, p):
        return remote(proj.at[u, half, p], rs_o.at[u, half, p], rs_s.at[u, half, p], rso_r.at[u, half, p], {"tp": mid})

    def rs_in(u, p):
        return remote(fwd.at[u, p], rs_i.at[u, p], rs_s.at[u, 0, p], rsi_r.at[u, p], {"tp": inner})

    def gather(q, u, half, p, lane, peer):
        return remote(og.at[q, u, half, p], og.at[q, u, half, p], og_s.at[lane, u, half, p], og_r.at[q, u, half, p], peer)

    def emit(b, accs, stats):
        for core in range(2):
            for h in range(2):
                part_ref[b, core, h * 128:(h + 1) * 128, :] = accs[h][:, core * 128:(core + 1) * 128]
            part_ref[b, core, 256:264, :] = stats[:, core * 128:(core + 1) * 128]
        a1(b).start()

    attend_step(it, n_seq, per_seq, lambda b: 2 * prefix_ref[b] - cp * (per_seq * CHUNK), q_ref, k_buf.at[it % SLOTS],
                v_buf.at[it % SLOTS], k_own, v_own, emit,
                s_a, s_b, m_ref, l_ref, acc_ref, m_own, l_own, acc_own)

    def s1(u):
        a1(u).wait_recv()
        accs, tops, totals = merge([part_ref[u, c], ra1[u]])
        for ref, want in ((sa2, 1 - y), (oa2, y)):
            ref[u, 0:128, :] = pack_half(accs, want)
            ref[u, 128:136, :] = jnp.broadcast_to(pack_half([jnp.broadcast_to(t, (8, 128)) for t in tops], want), (8, 128))
            ref[u, 136:144, :] = jnp.broadcast_to(pack_half([jnp.broadcast_to(t, (8, 128)) for t in totals], want), (8, 128))
        a2(u).start()

    def s2(u):
        a2(u).wait_recv()
        top = jnp.maximum(oa2[u, 128:136, :], ra2[u, 128:136, :])
        weights = [jnp.exp2(ref[u, 128:136, :] - top) for ref in (oa2, ra2)]
        total = weights[0] * oa2[u, 136:144, :] + weights[1] * ra2[u, 136:144, :]
        o = weights[0][0:1] * oa2[u, 0:128, :] + weights[1][0:1] * ra2[u, 0:128, :]
        o = (o / total[0:1]).T
        o = jnp.concatenate([o[16 * i:16 * i + 16].astype(BF16) for i in range(8)], axis=1)
        for half in (far, near):
            for p in range(pieces):
                cols = pl.ds(pl.multiple_of((half * pieces + p) * width, width), width)
                proj[u, half, p] = jnp.dot(o, wo[:, cols], preferred_element_type=F32)

        @pl.when(is_end)
        def _():
            for half in (far, near):
                for p in range(pieces):
                    rs_out(u, half, p).start()

    def s3(u):
        @pl.when(is_mid)
        def _():
            for p in range(pieces):
                rs_out(u, far, p).wait_recv()
                fwd[u, p] = proj[u, far, p] + rs_o[u, far, p]
                rs_in(u, p).start()

    def s4(u):
        for p in range(pieces):
            @pl.when(is_mid)
            def _(p=p):
                rs_out(u, near, p).wait_recv()
                rs_in(u, p).wait_recv()
                total = (proj[u, near, p] + rs_o[u, near, p]) + rs_i[u, p]
                x = x_buf[u, :, pl.ds(pl.multiple_of((near * pieces + p) * width, width), width)].astype(F32)
                og[me, u, near, p] = (x + total).astype(BF16).astype(F32)
                gather(me, u, near, p, 2, {"tp": inner}).start()
                gather(me, u, near, p, 3, {"tp": outer}).start()

            @pl.when(is_end)
            def _(p=p):
                gather(me, u, near, p, 2, {"tp": mid}).wait_recv()

            gather(me, u, near, p, 1, y_peer).start()
            gather(me, u, near, p, 0, core_peer).start()

    def s5(u):
        for p in range(pieces):
            gather(me, u, far, p, 2, {"tp": inner}).wait_recv()

            @pl.when(is_mid)
            def _(p=p):
                gather(me, u, far, p, 3, {"tp": outer}).start()

            gather(me, u, far, p, 1, y_peer).start()
            gather(me, u, far, p, 0, core_peer).start()

    def s6(u):
        for half in (near, far):
            for p in range(pieces):
                gather(yq, u, half, p, 1, y_peer).wait_recv()
                gather(yq, u, half, p, 4, core_peer).start()

    def put(q, u, half, p):
        cols = pl.ds(pl.multiple_of((half * pieces + p) * width, width), width)
        rows = pl.ds(pl.multiple_of(32 * (q % 2) + 16 * (q // 2), 16), 16)
        out_ref[u, rows, cols] = og[q, u, half, p].astype(BF16)

    def s7(u):
        for half in (near, far):
            for p in range(pieces):
                put(me, u, half, p)
                put(yq, u, half, p)
        for q in (y * 2 + 1 - c, (1 - y) * 2 + 1 - c):
            for half in (near, far):
                for p in range(pieces):
                    gather(q, u, half, p, 0, core_peer).wait_recv()
                    put(q, u, half, p)

    stages = (s1, s2, s3, s4, s5, s6, s7)

    def slot(t, carry):
        for stage, lag in zip(stages, LAGS):
            since = t - (2 * per_seq - 1) - lag
            @pl.when(jnp.logical_and(since >= 0, jnp.logical_and(since < per_seq * units, since % per_seq == 0)))
            def _(stage=stage, since=since):
                stage(since // per_seq)
        return carry

    last = (units + 1) * per_seq - 1 + LAGS[-1]
    lax.fori_loop(it, jnp.where(it == steps - 1, last + 1, it + 1), slot, 0)

    @pl.when(it == steps - 1)
    def _():
        for b in range(n_seq):
            a1(b).wait_send()
        for u in range(units):
            a2(u).wait_send()
            for half in (near, far):
                for p in range(pieces):
                    gather(me, u, half, p, 0, core_peer).wait_send()
                    gather(me, u, half, p, 1, y_peer).wait_send()
                    gather(yq, u, half, p, 4, core_peer).wait_send()

        @pl.when(is_end)
        def _():
            for u in range(units):
                for half in (near, far):
                    for p in range(pieces):
                        rs_out(u, half, p).wait_send()

        @pl.when(is_mid)
        def _():
            for u in range(units):
                for p in range(pieces):
                    rs_in(u, p).wait_send()
                    gather(me, u, near, p, 2, {"tp": inner}).wait_send()
                    for half in (near, far):
                        gather(me, u, half, p, 3, {"tp": outer}).wait_send()


def attend_and_combine(prefix_len, q, k_cache, v_cache, k_own, v_own, hidden, w_o):
    n_seq, n_new, d_model = hidden.shape
    slots = k_cache.shape[1]
    k_rows = k_cache.reshape(n_seq, slots * 2, HEAD_DIM)
    v_rows = v_cache.reshape(n_seq, slots * 2, HEAD_DIM)
    per_seq = slots * 2 // CHUNK
    units, width = n_seq, d_model // (2 * PIECES)
    vmem = pl.BlockSpec(memory_space=pltpu.VMEM)
    hbm = pl.BlockSpec(memory_space=pl.ANY)
    dma = pltpu.SemaphoreType.DMA
    return pl.pallas_call(
        fused_kernel,
        grid=((n_seq + 1) * per_seq,),
        out_shape=jax.ShapeDtypeStruct((n_seq, n_new, d_model), BF16),
        in_specs=[pl.BlockSpec(memory_space=pltpu.SMEM), vmem, hbm, hbm, vmem, vmem, hbm, hbm],
        out_specs=vmem,
        scratch_shapes=[
            pltpu.VMEM((SLOTS, CHUNK, HEAD_DIM), BF16),
            pltpu.VMEM((SLOTS, CHUNK, HEAD_DIM), BF16), dma((SLOTS,)), dma((SLOTS,)),
            pltpu.VMEM((slots * 2, 256), F32), pltpu.VMEM((slots * 2, 256), F32),
            pltpu.VMEM((2, 8, 256), F32), pltpu.VMEM((2, 8, 256), F32), pltpu.VMEM((256, 256), F32),
            pltpu.VMEM((n_seq, 8, 256), F32), pltpu.VMEM((n_seq, 8, 256), F32), pltpu.VMEM((n_seq, 256, 256), F32),
            pltpu.VMEM((n_seq, 2, 264, 128), F32),
            pltpu.VMEM((units, 16, d_model), BF16), pltpu.VMEM(w_o.shape, BF16),
            pltpu.VMEM((n_seq, 264, 128), F32), pltpu.VMEM((units, 144, 128), F32),
            pltpu.VMEM((units, 144, 128), F32), pltpu.VMEM((units, 144, 128), F32), pltpu.VMEM((units, 2, PIECES, 16, width), F32),
            pltpu.VMEM((units, 2, PIECES, 16, width), F32), pltpu.VMEM((units, PIECES, 16, width), F32),
            pltpu.VMEM((units, PIECES, 16, width), F32), pltpu.VMEM((4, units, 2, PIECES, 16, width), F32),
            dma((1 + units,)), dma((n_seq,)), dma((n_seq,)), dma((units,)), dma((units,)), dma((units, 2, PIECES)),
            dma((units, 2, PIECES)), dma((units, PIECES)), dma((5, units, 2, PIECES)), dma((4, units, 2, PIECES))],
        compiler_params=pltpu.CompilerParams(collective_id=0, has_side_effects=True, vmem_limit_bytes=VMEM_LIMIT),
        cost_estimate=pl.CostEstimate(flops=19 << 30, bytes_accessed=46 << 20, transcendentals=17 << 20),
        name="attend_and_combine",
    )(prefix_len, q, k_rows, v_rows, k_own, v_own, hidden, w_o)


def solution(mesh):
    def per_device(hidden, prefix_len, k_cache, v_cache, attn_norm, w_q, w_k, w_v, w_o, q_norm, k_norm):
        q, k_own, v_own, k_new, v_new = project(hidden, prefix_len, attn_norm, w_q, w_k, w_v, q_norm, k_norm)
        block_out = attend_and_combine(prefix_len, q, k_cache, v_cache, k_own, v_own, hidden, w_o)
        shape = (hidden.shape[0], hidden.shape[1], 2, HEAD_DIM)
        return block_out, k_new.reshape(shape), v_new.reshape(shape)

    cache_spec = P('dp', 'cp', 'tp', None)
    arg_specs = (P('dp', None, None), P('dp'), cache_spec, cache_spec, P(None), P(None, 'tp'), P(None, 'tp'), P(None, 'tp'), P('tp', None), P(None), P(None))
    out_specs = (P('dp', None, None), P('dp', None, 'tp', None), P('dp', None, 'tp', None))
    return jax.shard_map(per_device, mesh=mesh, in_specs=arg_specs, out_specs=out_specs, check_vma=False)
```

```python
import functools

import jax
import jax.numpy as jnp
import numpy as np
from jax import lax
from jax.experimental import pallas as pl
from jax.experimental.pallas import tpu as pltpu
from jax.sharding import PartitionSpec as P

HEAD_DIM = 128
MASKED = -1e30
EPS = 1e-6
LOG2_SCALE = float(HEAD_DIM ** -0.5 / np.log(2.0))
MESH = pl.DeviceIdType.MESH
NT = (((1,), (1,)), ((), ()))
TN = (((0,), (0,)), ((), ()))
F32 = jnp.float32
BF16 = jnp.bfloat16
VMEM_LIMIT = 67043328


def cos_or_sin(x, want_cos):
    quarter = jnp.floor(x * F32(2.0 / np.pi) + F32(0.5))
    r = ((x - quarter * F32(1.5703125)) - quarter * F32(4.8351287841796875e-4)) - quarter * F32(3.13855707645416259765625e-7)
    r = r - quarter * F32(6.077100628276710381e-11)
    n = quarter.astype(jnp.int32) + want_cos.astype(jnp.int32)
    r2 = r * r
    sin_r = r + r * r2 * (F32(-1.6666654611e-1) + r2 * (F32(8.3321608736e-3) + r2 * F32(-1.9515295891e-4)))
    cos_r = 1.0 - 0.5 * r2 + r2 * r2 * (F32(4.166664568298827e-2) + r2 * (F32(-1.388731625493765e-3) + r2 * F32(2.443315711809948e-5)))
    y = jnp.where(n % 2 == 0, sin_r, cos_r)
    return jnp.where(n % 4 >= 2, -y, y)


def project_kernel(prefix_ref, x_ref, an_ref, wq_hbm, wk_hbm, wv_hbm, qn_ref, kn_ref, freq_ref,
                   q_ref, k_ref, v_ref, kn_out, vn_out, wq, wk, wv, normed, cos_ref, sin_ref, sems):
    n_seq, n_new = k_ref.shape[0], k_ref.shape[2]
    rows = n_seq * n_new
    depth = wq.shape[0] // 4
    copies = [pltpu.make_async_copy(wq_hbm.at[pl.ds(depth * j, depth)], wq.at[pl.ds(depth * j, depth)], sems.at[j])
              for j in range(4)]
    copies.append(pltpu.make_async_copy(wk_hbm, wk, sems.at[4]))
    copies.append(pltpu.make_async_copy(wv_hbm, wv, sems.at[5]))
    for c in copies:
        c.start()
    for r in range(0, rows, 64):
        x = x_ref[r:r + 64, :].astype(F32)
        scale = lax.rsqrt(jnp.mean(x * x, axis=-1, keepdims=True) + EPS)
        for j in range(x.shape[1] // 128):
            cols = slice(128 * j, 128 * j + 128)
            normed[r:r + 64, cols] = (x[:, cols] * scale * an_ref[j:j + 1, :].astype(F32)).astype(BF16)
    low = lax.broadcasted_iota(jnp.int32, (n_new, HEAD_DIM), 1) < HEAD_DIM // 2
    step = lax.broadcasted_iota(jnp.int32, (n_new, HEAD_DIM), 0)
    for b in range(n_seq):
        angle = (prefix_ref[b] + step).astype(F32) * freq_ref[...]
        trig = cos_or_sin(angle, low)
        turned = pltpu.roll(trig, HEAD_DIM // 2, 1)
        cos_ref[b * n_new:(b + 1) * n_new, :] = jnp.where(low, trig, turned)
        sin_ref[b * n_new:(b + 1) * n_new, :] = jnp.where(low, -turned, trig)

    def norm_rope(y, gain_ref):
        y = y.astype(BF16).astype(F32)
        y = y * lax.rsqrt(jnp.mean(y * y, axis=-1, keepdims=True) + EPS) * gain_ref[...].astype(F32)
        return (y * cos_ref[...] + pltpu.roll(y, HEAD_DIM // 2, 1) * sin_ref[...]).astype(BF16)

    for j in range(4):
        copies[j].wait()
    for j in range(4):
        y = jnp.dot(normed[...], wq[:, 256 * j:256 * j + 256], preferred_element_type=F32)
        for i in range(2):
            h, g = j // 2, 2 * (j % 2) + i
            head = norm_rope(y[:, i * HEAD_DIM:(i + 1) * HEAD_DIM], qn_ref)
            for b in range(n_seq):
                for part in range(4):
                    q_ref[b, part * 64 + g * 16:part * 64 + g * 16 + 16, h * 128:(h + 1) * 128] = (
                        head[b * 64 + part * 16:b * 64 + part * 16 + 16])
    dst = lax.broadcasted_iota(jnp.int32, (2 * n_new, 2 * n_new), 0)
    src = lax.broadcasted_iota(jnp.int32, (2 * n_new, 2 * n_new), 1)
    perm = (src == (dst % 2) * n_new + dst // 2).astype(F32).astype(BF16)

    def put(heads, own_ref, new_ref):
        for b in range(n_seq):
            both = jnp.concatenate([head[b * n_new:(b + 1) * n_new] for head in heads], axis=0)
            for h in range(2):
                own_ref[b, h] = both[h * n_new:(h + 1) * n_new]
            new_ref[b] = jnp.dot(perm, both, preferred_element_type=F32).astype(BF16)

    copies[4].wait()
    y = jnp.dot(normed[...], wk[...], preferred_element_type=F32)
    put([norm_rope(y[:, h * HEAD_DIM:(h + 1) * HEAD_DIM], kn_ref) for h in range(2)], k_ref, kn_out)
    copies[5].wait()
    y = jnp.dot(normed[...], wv[...], preferred_element_type=F32).astype(BF16)
    put([y[:, h * HEAD_DIM:(h + 1) * HEAD_DIM] for h in range(2)], v_ref, vn_out)


def project(hidden, prefix_len, attn_norm, w_q, w_k, w_v, q_norm, k_norm):
    n_seq, n_new, d_model = hidden.shape
    freq = 1.0 / (1000000.0 ** (np.arange(HEAD_DIM // 2, dtype=np.float64) * 2.0 / HEAD_DIM))
    freq = jnp.asarray(np.concatenate([freq, freq])[None].astype(np.float32))
    vmem = pl.BlockSpec(memory_space=pltpu.VMEM)
    hbm = pl.BlockSpec(memory_space=pl.ANY)
    rows = n_seq * n_new
    return pl.pallas_call(
        project_kernel,
        out_shape=(jax.ShapeDtypeStruct((n_seq, 256, 256), BF16),
                   jax.ShapeDtypeStruct((n_seq, 2, n_new, HEAD_DIM), BF16),
                   jax.ShapeDtypeStruct((n_seq, 2, n_new, HEAD_DIM), BF16),
                   jax.ShapeDtypeStruct((n_seq, 2 * n_new, HEAD_DIM), BF16),
                   jax.ShapeDtypeStruct((n_seq, 2 * n_new, HEAD_DIM), BF16)),
        in_specs=[pl.BlockSpec(memory_space=pltpu.SMEM), vmem, vmem, hbm, hbm, hbm, vmem, vmem, vmem],
        out_specs=(vmem,) * 5,
        scratch_shapes=[pltpu.VMEM(w_q.shape, BF16), pltpu.VMEM((d_model, 256), BF16),
                        pltpu.VMEM((d_model, 256), BF16), pltpu.VMEM((rows, d_model), BF16),
                        pltpu.VMEM((rows, HEAD_DIM), F32), pltpu.VMEM((rows, HEAD_DIM), F32),
                        pltpu.SemaphoreType.DMA((6,))],
        compiler_params=pltpu.CompilerParams(vmem_limit_bytes=VMEM_LIMIT),
        cost_estimate=pl.CostEstimate(flops=2 * rows * d_model * 1536, bytes_accessed=12 << 20, transcendentals=0),
        name="project",
    )(prefix_len, hidden.reshape(rows, d_model), attn_norm.reshape(d_model // 128, 128), w_q, w_k, w_v, q_norm[None], k_norm[None], freq)


CHUNK = 4096
SLOTS = 3


def pair_reduce(op, x):
    x = op(x, pltpu.roll(x, 2, 0))
    return op(x, pltpu.roll(x, 4, 0))


def split_heads(x):
    even = (lax.broadcasted_iota(jnp.int32, (16, HEAD_DIM), 0) % 2 == 0).astype(F32)
    gains = [even.astype(BF16), (1.0 - even).astype(BF16)]
    return jnp.concatenate([x * jnp.concatenate([g] * (x.shape[0] // 16), axis=0) for g in gains], axis=1)


def own_keys(q, k_own_ref, v_own_ref):
    n_new = k_own_ref.shape[-2]
    key = lax.broadcasted_iota(jnp.int32, (n_new, 256), 0)
    col = lax.broadcasted_iota(jnp.int32, (n_new, 256), 1)
    keep = key <= (col // 64) * 16 + col % 16
    maxes, sums, accs = [], [], []
    for h in range(2):
        s = lax.dot_general(k_own_ref[h], q[:, h * 128:(h + 1) * 128], NT, preferred_element_type=F32)
        s = jnp.where(keep, s * LOG2_SCALE, MASKED)
        m = jnp.max(s, axis=0, keepdims=True)
        p = jnp.exp2(s - m)
        maxes.append(m)
        sums.append(jnp.sum(p, axis=0, keepdims=True))
        accs.append(lax.dot_general(v_own_ref[h], p.astype(BF16), TN, preferred_element_type=F32))
    even = lax.broadcasted_iota(jnp.int32, (8, 256), 0) % 2 == 0
    return (jnp.where(even, maxes[0], maxes[1]), jnp.where(even, sums[0], sums[1]), accs)


def attend_step(it, n_seq, per_seq, limit_of, q_all, k_ref, v_ref, k_own, v_own, emit,
                s_a, s_b, m_ref, l_ref, acc_ref, m_own, l_own, acc_own):
    cp = lax.axis_index("cp")
    s_refs = (s_a, s_b)

    @pl.when(it == 0)
    def _():
        acc_ref[...] = jnp.zeros_like(acc_ref)
        l_ref[...] = jnp.zeros_like(l_ref)

        @pl.when(cp == 0)
        def _():
            for b in range(n_seq):
                m8, l8, accs = own_keys(q_all[b], k_own.at[b], v_own.at[b])
                m_own[b] = m8
                l_own[b] = l8
                for h in range(2):
                    acc_own[b, h * 128:(h + 1) * 128, :] = accs[h]

        @pl.when(cp != 0)
        def _():
            m_own[...] = jnp.full_like(m_own, MASKED)
            l_own[...] = jnp.zeros_like(l_own)
            acc_own[...] = jnp.zeros_like(acc_own)

    b_new, i = it // per_seq, it % per_seq
    b_old = b_new - 1
    rows = pl.ds(pl.multiple_of(i * CHUNK, CHUNK), CHUNK)

    def score_dot():
        both = split_heads(k_ref[...])
        return lax.dot_general(both, q_all[b_new], NT, preferred_element_type=F32)

    def score_post(s, par):
        left = limit_of(b_new) - i * CHUNK - lax.broadcasted_iota(jnp.int32, (8, 128), 0)
        keep = (lax.broadcasted_iota(jnp.int32, (CHUNK // 8, 8, 128), 0) * 8 < left[None]).reshape(CHUNK, 128)
        s = jnp.concatenate([jnp.where(keep, s[:, 0:128], MASKED), jnp.where(keep, s[:, 128:256], MASKED)], axis=1)
        s_refs[par][rows, :] = s
        top = pair_reduce(jnp.maximum, jnp.max(s.reshape(CHUNK // 8, 8, 256), axis=0)) * LOG2_SCALE
        m_ref[par] = jnp.maximum(jnp.where(i == 0, m_own[b_new], m_ref[par]), top)

    def expo(par):
        s = s_refs[par][rows, :]
        p = jnp.exp2(s.reshape(CHUNK // 8, 8, 256) * LOG2_SCALE - m_ref[par][None])
        l_ref[par] = jnp.where(i == 0, 0.0, l_ref[par]) + jnp.sum(p, axis=0)
        return p.reshape(CHUNK, 256).astype(BF16)

    def value(p):
        both = split_heads(v_ref[...])
        part = lax.dot_general(both, p, TN, preferred_element_type=F32)
        acc_ref[...] = jnp.where(i == 0, 0.0, acc_ref[...]) + part

    total = n_seq * per_seq
    scoring, adding = it < total, jnp.logical_and(it >= per_seq, it < total + per_seq)
    for par in range(2):
        @pl.when(b_new % 2 == par)
        def _(par=par):
            main = jnp.logical_and(scoring, adding)

            @pl.when(main)
            def _():
                s = score_dot()
                p = expo(1 - par)
                value(p)
                score_post(s, par)

            @pl.when(jnp.logical_and(scoring, jnp.logical_not(adding)))
            def _():
                score_post(score_dot(), par)

            @pl.when(jnp.logical_and(adding, jnp.logical_not(scoring)))
            def _():
                value(expo(1 - par))

    @pl.when(jnp.logical_and(adding, i == per_seq - 1))
    def _():
        b = b_old
        m8 = m_ref[b % 2]
        w = jnp.exp2(m_own[b] - m8)
        l8 = pair_reduce(jnp.add, l_ref[b % 2]) + w * l_own[b]
        sub = lax.broadcasted_iota(jnp.int32, (8, 256), 0)
        stats = jnp.where(sub < 2, m8, l8)
        accs = [acc_ref[h * 128:(h + 1) * 128, :] + w[h:h + 1] * acc_own[b, h * 128:(h + 1) * 128, :] for h in range(2)]
        emit(b, accs, stats)


def fetch(it, total, per_seq, k_hbm, v_hbm, k_buf, v_buf, k_sem, v_sem):
    def copy(hbm, buf, sem, lag, step):
        j = step - lag
        src = hbm.at[j // per_seq, pl.ds(pl.multiple_of((j % per_seq) * CHUNK, CHUNK), CHUNK), :]
        return pltpu.make_async_copy(src, buf.at[step % SLOTS], sem.at[step % SLOTS])

    for hbm, buf, sem, lag in ((k_hbm, k_buf, k_sem, 0), (v_hbm, v_buf, v_sem, per_seq)):
        if lag == 0:
            @pl.when(it == 0)
            def _():
                for step in range(SLOTS - 1):
                    copy(hbm, buf, sem, lag, step).start()
        ahead = it + SLOTS - 1

        @pl.when(jnp.logical_and(ahead >= lag, ahead < total + lag))
        def _():
            copy(hbm, buf, sem, lag, ahead).start()

        @pl.when(jnp.logical_and(it >= lag, it < total + lag))
        def _():
            copy(hbm, buf, sem, lag, it).wait()


def merge(parts):
    sub = lax.broadcasted_iota(jnp.int32, (8, 128), 0)
    stats = [p[256:264, :] for p in parts]
    maxes = [jnp.where(sub % 4 < 2, s, pltpu.roll(s, 2, 0)) for s in stats]
    top = functools.reduce(jnp.maximum, maxes)
    weights = [jnp.exp2(m - top) for m in maxes]
    total = sum(w * s for w, s in zip(weights, stats))
    accs = [sum(w[h:h + 1] * p[h * 128:(h + 1) * 128, :] for w, p in zip(weights, parts)) for h in range(2)]
    return accs, [top[h:h + 1] for h in range(2)], [total[2 + h:3 + h] for h in range(2)]


def pack_half(pair, want):
    first, second = pair
    low = lax.broadcasted_iota(jnp.int32, first.shape, 1) < 64
    at_zero = jnp.where(low, first, pltpu.roll(second, 64, 1))
    at_one = jnp.where(low, pltpu.roll(first, 64, 1), second)
    return jnp.where(want == 0, at_zero, at_one)


PIECES = 2
LAGS = (1, 3, 8, 10, 13, 16, 18)


def fused_kernel(prefix_ref, q_ref, k_hbm, v_hbm, k_own, v_own, x_hbm, wo_hbm, out_ref,
                 k_buf, v_buf, k_sem, v_sem, s_a, s_b, m_ref, l_ref, acc_ref, m_own, l_own, acc_own,
                 part_ref, x_buf, wo, ra1, sa2, oa2, ra2, proj, rs_o, rs_i, fwd, og,
                 loc_sem, a1_s, a1_r, a2_s, a2_r, rs_s, rso_r, rsi_r, og_s, og_r):
    it = pl.program_id(0)
    steps = pl.num_programs(0)
    per_seq = steps // (q_ref.shape[0] + 1)
    n_seq = q_ref.shape[0]
    units = n_seq
    pieces, width = proj.shape[2], proj.shape[-1]
    cp, z = lax.axis_index("cp"), lax.axis_index("tp")
    y, c = cp // 2, cp % 2
    is_mid = jnp.logical_and(z >= 1, z <= 2)
    is_end = jnp.logical_not(is_mid)
    near, far = z // 2, 1 - z // 2
    outer = jnp.where(z == 1, 0, 3)
    inner = jnp.where(z == 1, 2, 1)
    mid = jnp.where(z == 0, 1, 2)
    core_peer = {"cp": y * 2 + 1 - c}
    y_peer = {"cp": (1 - y) * 2 + c}
    me, yq = y * 2 + c, (1 - y) * 2 + c

    def remote(src, dst, send_sem, recv_sem, peer):
        return pltpu.make_async_remote_copy(src_ref=src, dst_ref=dst, send_sem=send_sem, recv_sem=recv_sem,
                                            device_id=peer, device_id_type=MESH)

    wo_copy = pltpu.make_async_copy(wo_hbm, wo, loc_sem.at[0])
    x_copies = [pltpu.make_async_copy(x_hbm.at[u, pl.ds(pl.multiple_of(32 * c + 16 * y, 16), 16), :], x_buf.at[u], loc_sem.at[1 + u])
                for u in range(units)]

    @pl.when(it == 0)
    def _():
        barrier = pltpu.get_barrier_semaphore()
        pl.semaphore_signal(barrier, inc=1, device_id=core_peer, device_id_type=MESH)
        pl.semaphore_signal(barrier, inc=1, device_id=y_peer, device_id_type=MESH)

        @pl.when(is_mid)
        def _():
            pl.semaphore_signal(barrier, inc=1, device_id={"tp": outer}, device_id_type=MESH)
            pl.semaphore_signal(barrier, inc=1, device_id={"tp": inner}, device_id_type=MESH)
            pl.semaphore_wait(barrier, 4)

        @pl.when(is_end)
        def _():
            pl.semaphore_signal(barrier, inc=1, device_id={"tp": mid}, device_id_type=MESH)
            pl.semaphore_wait(barrier, 3)

    fetch(it, n_seq * per_seq, per_seq, k_hbm, v_hbm, k_buf, v_buf, k_sem, v_sem)

    @pl.when(it == 1)
    def _():
        wo_copy.start()
        for x_copy in x_copies:
            x_copy.start()

    @pl.when(it == 2 * per_seq)
    def _():
        wo_copy.wait()
        for x_copy in x_copies:
            x_copy.wait()

    def a1(b):
        return remote(part_ref.at[b, 1 - c], ra1.at[b], a1_s.at[b], a1_r.at[b], core_peer)

    def a2(u):
        return remote(sa2.at[u], ra2.at[u], a2_s.at[u], a2_r.at[u], y_peer)

    def rs_out(u, half, p):
        return remote(proj.at[u, half, p], rs_o.at[u, half, p], rs_s.at[u, half, p], rso_r.at[u, half, p], {"tp": mid})

    def rs_in(u, p):
        return remote(fwd.at[u, p], rs_i.at[u, p], rs_s.at[u, 0, p], rsi_r.at[u, p], {"tp": inner})

    def gather(q, u, half, p, lane, peer):
        return remote(og.at[q, u, half, p], og.at[q, u, half, p], og_s.at[lane, u, half, p], og_r.at[q, u, half, p], peer)

    def emit(b, accs, stats):
        for core in range(2):
            for h in range(2):
                part_ref[b, core, h * 128:(h + 1) * 128, :] = accs[h][:, core * 128:(core + 1) * 128]
            part_ref[b, core, 256:264, :] = stats[:, core * 128:(core + 1) * 128]
        a1(b).start()

    attend_step(it, n_seq, per_seq, lambda b: 2 * prefix_ref[b] - cp * (per_seq * CHUNK), q_ref, k_buf.at[it % SLOTS],
                v_buf.at[it % SLOTS], k_own, v_own, emit,
                s_a, s_b, m_ref, l_ref, acc_ref, m_own, l_own, acc_own)

    def s1(u):
        a1(u).wait_recv()
        accs, tops, totals = merge([part_ref[u, c], ra1[u]])
        for ref, want in ((sa2, 1 - y), (oa2, y)):
            ref[u, 0:128, :] = pack_half(accs, want)
            ref[u, 128:136, :] = jnp.broadcast_to(pack_half([jnp.broadcast_to(t, (8, 128)) for t in tops], want), (8, 128))
            ref[u, 136:144, :] = jnp.broadcast_to(pack_half([jnp.broadcast_to(t, (8, 128)) for t in totals], want), (8, 128))
        a2(u).start()

    def rows_of(u):
        a2(u).wait_recv()
        top = jnp.maximum(oa2[u, 128:136, :], ra2[u, 128:136, :])
        weights = [jnp.exp2(ref[u, 128:136, :] - top) for ref in (oa2, ra2)]
        total = weights[0] * oa2[u, 136:144, :] + weights[1] * ra2[u, 136:144, :]
        o = weights[0][0:1] * oa2[u, 0:128, :] + weights[1][0:1] * ra2[u, 0:128, :]
        o = (o / total[0:1]).T
        return jnp.concatenate([o[16 * i:16 * i + 16].astype(BF16) for i in range(8)], axis=1)

    def s2(u):
        @pl.when(u % 2 == 1)
        def _():
            o = jnp.concatenate([rows_of(u - 1), rows_of(u)], axis=0)
            for half in (far, near):
                for p in range(pieces):
                    cols = pl.ds(pl.multiple_of((half * pieces + p) * width, width), width)
                    out = jnp.dot(o, wo[:, cols], preferred_element_type=F32)
                    proj[u - 1, half, p] = out[0:16]
                    proj[u, half, p] = out[16:32]

            @pl.when(is_end)
            def _():
                for v in (u - 1, u):
                    for half in (far, near):
                        for p in range(pieces):
                            rs_out(v, half, p).start()

    def s3(u):
        @pl.when(is_mid)
        def _():
            for p in range(pieces):
                rs_out(u, far, p).wait_recv()
                fwd[u, p] = proj[u, far, p] + rs_o[u, far, p]
                rs_in(u, p).start()

    def s4(u):
        for p in range(pieces):
            @pl.when(is_mid)
            def _(p=p):
                rs_out(u, near, p).wait_recv()
                rs_in(u, p).wait_recv()
                total = (proj[u, near, p] + rs_o[u, near, p]) + rs_i[u, p]
                x = x_buf[u, :, pl.ds(pl.multiple_of((near * pieces + p) * width, width), width)].astype(F32)
                og[me, u, near, p] = (x + total).astype(BF16).astype(F32)
                gather(me, u, near, p, 2, {"tp": inner}).start()
                gather(me, u, near, p, 3, {"tp": outer}).start()

            @pl.when(is_end)
            def _(p=p):
                gather(me, u, near, p, 2, {"tp": mid}).wait_recv()

            gather(me, u, near, p, 1, y_peer).start()
            gather(me, u, near, p, 0, core_peer).start()

    def s5(u):
        for p in range(pieces):
            gather(me, u, far, p, 2, {"tp": inner}).wait_recv()

            @pl.when(is_mid)
            def _(p=p):
                gather(me, u, far, p, 3, {"tp": outer}).start()

            gather(me, u, far, p, 1, y_peer).start()
            gather(me, u, far, p, 0, core_peer).start()

    def s6(u):
        for half in (near, far):
            for p in range(pieces):
                gather(yq, u, half, p, 1, y_peer).wait_recv()
                gather(yq, u, half, p, 4, core_peer).start()

    def put(q, u, half, p):
        cols = pl.ds(pl.multiple_of((half * pieces + p) * width, width), width)
        rows = pl.ds(pl.multiple_of(32 * (q % 2) + 16 * (q // 2), 16), 16)
        out_ref[u, rows, cols] = og[q, u, half, p].astype(BF16)

    def s7(u):
        for half in (near, far):
            for p in range(pieces):
                put(me, u, half, p)
                put(yq, u, half, p)
        for q in (y * 2 + 1 - c, (1 - y) * 2 + 1 - c):
            for half in (near, far):
                for p in range(pieces):
                    gather(q, u, half, p, 0, core_peer).wait_recv()
                    put(q, u, half, p)

    stages = (s1, s2, s3, s4, s5, s6, s7)

    def slot(t, carry):
        for stage, lag in zip(stages, LAGS):
            since = t - (2 * per_seq - 1) - lag
            @pl.when(jnp.logical_and(since >= 0, jnp.logical_and(since < per_seq * units, since % per_seq == 0)))
            def _(stage=stage, since=since):
                stage(since // per_seq)
        return carry

    last = (units + 1) * per_seq - 1 + LAGS[-1]
    lax.fori_loop(it, jnp.where(it == steps - 1, last + 1, it + 1), slot, 0)

    @pl.when(it == steps - 1)
    def _():
        for b in range(n_seq):
            a1(b).wait_send()
        for u in range(units):
            a2(u).wait_send()
            for half in (near, far):
                for p in range(pieces):
                    gather(me, u, half, p, 0, core_peer).wait_send()
                    gather(me, u, half, p, 1, y_peer).wait_send()
                    gather(yq, u, half, p, 4, core_peer).wait_send()

        @pl.when(is_end)
        def _():
            for u in range(units):
                for half in (near, far):
                    for p in range(pieces):
                        rs_out(u, half, p).wait_send()

        @pl.when(is_mid)
        def _():
            for u in range(units):
                for p in range(pieces):
                    rs_in(u, p).wait_send()
                    gather(me, u, near, p, 2, {"tp": inner}).wait_send()
                    for half in (near, far):
                        gather(me, u, half, p, 3, {"tp": outer}).wait_send()


def attend_and_combine(prefix_len, q, k_cache, v_cache, k_own, v_own, hidden, w_o):
    n_seq, n_new, d_model = hidden.shape
    slots = k_cache.shape[1]
    k_rows = k_cache.reshape(n_seq, slots * 2, HEAD_DIM)
    v_rows = v_cache.reshape(n_seq, slots * 2, HEAD_DIM)
    per_seq = slots * 2 // CHUNK
    units, width = n_seq, d_model // (2 * PIECES)
    vmem = pl.BlockSpec(memory_space=pltpu.VMEM)
    hbm = pl.BlockSpec(memory_space=pl.ANY)
    dma = pltpu.SemaphoreType.DMA
    return pl.pallas_call(
        fused_kernel,
        grid=((n_seq + 1) * per_seq,),
        out_shape=jax.ShapeDtypeStruct((n_seq, n_new, d_model), BF16),
        in_specs=[pl.BlockSpec(memory_space=pltpu.SMEM), vmem, hbm, hbm, vmem, vmem, hbm, hbm],
        out_specs=vmem,
        scratch_shapes=[
            pltpu.VMEM((SLOTS, CHUNK, HEAD_DIM), BF16),
            pltpu.VMEM((SLOTS, CHUNK, HEAD_DIM), BF16), dma((SLOTS,)), dma((SLOTS,)),
            pltpu.VMEM((slots * 2, 256), F32), pltpu.VMEM((slots * 2, 256), F32),
            pltpu.VMEM((2, 8, 256), F32), pltpu.VMEM((2, 8, 256), F32), pltpu.VMEM((256, 256), F32),
            pltpu.VMEM((n_seq, 8, 256), F32), pltpu.VMEM((n_seq, 8, 256), F32), pltpu.VMEM((n_seq, 256, 256), F32),
            pltpu.VMEM((n_seq, 2, 264, 128), F32),
            pltpu.VMEM((units, 16, d_model), BF16), pltpu.VMEM(w_o.shape, BF16),
            pltpu.VMEM((n_seq, 264, 128), F32), pltpu.VMEM((units, 144, 128), F32),
            pltpu.VMEM((units, 144, 128), F32), pltpu.VMEM((units, 144, 128), F32), pltpu.VMEM((units, 2, PIECES, 16, width), F32),
            pltpu.VMEM((units, 2, PIECES, 16, width), F32), pltpu.VMEM((units, PIECES, 16, width), F32),
            pltpu.VMEM((units, PIECES, 16, width), F32), pltpu.VMEM((4, units, 2, PIECES, 16, width), F32),
            dma((1 + units,)), dma((n_seq,)), dma((n_seq,)), dma((units,)), dma((units,)), dma((units, 2, PIECES)),
            dma((units, 2, PIECES)), dma((units, PIECES)), dma((5, units, 2, PIECES)), dma((4, units, 2, PIECES))],
        compiler_params=pltpu.CompilerParams(collective_id=0, has_side_effects=True, vmem_limit_bytes=VMEM_LIMIT),
        cost_estimate=pl.CostEstimate(flops=19 << 30, bytes_accessed=46 << 20, transcendentals=17 << 20),
        name="attend_and_combine",
    )(prefix_len, q, k_rows, v_rows, k_own, v_own, hidden, w_o)


def solution(mesh):
    def per_device(hidden, prefix_len, k_cache, v_cache, attn_norm, w_q, w_k, w_v, w_o, q_norm, k_norm):
        q, k_own, v_own, k_new, v_new = project(hidden, prefix_len, attn_norm, w_q, w_k, w_v, q_norm, k_norm)
        block_out = attend_and_combine(prefix_len, q, k_cache, v_cache, k_own, v_own, hidden, w_o)
        shape = (hidden.shape[0], hidden.shape[1], 2, HEAD_DIM)
        return block_out, k_new.reshape(shape), v_new.reshape(shape)

    cache_spec = P('dp', 'cp', 'tp', None)
    arg_specs = (P('dp', None, None), P('dp'), cache_spec, cache_spec, P(None), P(None, 'tp'), P(None, 'tp'), P(None, 'tp'), P('tp', None), P(None), P(None))
    out_specs = (P('dp', None, None), P('dp', None, 'tp', None), P('dp', None, 'tp', None))
    return jax.shard_map(per_device, mesh=mesh, in_specs=arg_specs, out_specs=out_specs, check_vma=False)
```
